32 devices in a mesh: gx: 4 (over x, core), gy: 4 (over z), gz: 2 (over y).
Axes of the slice: x: 2, y: 2, z: 4, core: 2. Of those that a mesh axis runs over, the one named last changes fastest.
Arguments:
- density: float32 [32, 64, 256], P('gx', 'gy', 'gz'), may hold values from 0.1 to 10
- x_faces: float32 [2, 64, 256], P(None, 'gy', 'gz'), may hold values from -6 to 6
- y_faces: float32 [2, 32, 256], P(None, 'gx', 'gz'), may hold values from -6 to 6
- z_faces: float32 [2, 32, 64], P(None, 'gx', 'gy'), may hold values from -6 to 6
Outputs:
- solution_field: float32 [32, 64, 256], P('gx', 'gy', 'gz')
- residual: float32 [32, 64, 256], P('gx', 'gy', 'gz')
The draws below stay inside these ranges and needn't reach their ends.
All inputs are finite; a program needn't handle non-finite values.
Results may differ from the reference program's by a relative error of at most 0.0003.
Values sent between devices are 32-bit elements; how exact they have to be, the bound alone decides.
A program may use at most 64 MiB of HBM per device.

```python
import jax
import jax.numpy as jnp

ITERS = 2
LEVELS = 3
COARSE_SWEEPS = 3
NX = 32
NY = 64
NZ = 256


def draw_density(key, part):
    rough_key = jax.random.fold_in(key, 11)
    x_frac = jnp.arange(NX, dtype=jnp.float32) / NX
    rough = jnp.exp(jax.random.uniform(rough_key, (NX, NY, NZ), jnp.float32, jnp.log(0.5), jnp.log(2.0)))
    profile = jnp.exp(jnp.log(3.0) * x_frac)[:, None, None]
    return (rough * profile).astype(jnp.float32)


def shard_levels(stream_key, dims, pieces, least, largest):
    def one(axis_at, blocks):
        heights = jax.random.uniform(jax.random.fold_in(jax.random.fold_in(stream_key, 6), axis_at), (blocks,), jnp.float32, least / len(pieces), largest / len(pieces))
        return jnp.repeat(jnp.exp(heights), dims[axis_at] // blocks).reshape((-1,) + (1,) * (len(dims) - axis_at - 1))

    level = one(*pieces[0])
    for cut in pieces[1:]:
        level = level * one(*cut)
    return level


def bell_draw(stream_key, dims, width, most, cuts=(), kind=jnp.bfloat16):
    gain = shard_levels(stream_key, dims, cuts, -0.22, 0.18) if cuts else 1.0
    array = jax.random.normal(stream_key, dims, jnp.float32) * width * gain
    return jnp.minimum(jnp.maximum(array, -most), most).astype(kind)


def setup_inputs(seed: int = 0) -> dict:
    key_list = jax.random.split(jax.random.key(seed), 5)
    density = draw_density(jax.random.fold_in(key_list[4], 71), 0)
    x_faces = bell_draw(key_list[1], (2, NY, NZ), 1.0, 6.0, ((1, 4), (2, 2)), jnp.float32)
    y_faces = bell_draw(key_list[2], (2, NX, NZ), 1.0, 6.0, ((1, 4), (2, 2)), jnp.float32)
    z_faces = bell_draw(key_list[3], (2, NX, NY), 1.0, 6.0, ((1, 4), (2, 4)), jnp.float32)
    return dict(density=density, x_faces=x_faces, y_faces=y_faces, z_faces=z_faces)


relax_rate = 1.0 / 9.0
coupling = 0.5


def beside_sum(padded):
    beside = padded[2:, 1:-1, 1:-1] + padded[:-2, 1:-1, 1:-1]
    beside = beside + padded[1:-1, 2:, 1:-1] + padded[1:-1, :-2, 1:-1]
    beside = beside + padded[1:-1, 1:-1, 2:] + padded[1:-1, 1:-1, :-2]
    return beside


def operate(field):
    return 6.0 * field - beside_sum(jnp.pad(field, 1))


def restrict(field):
    sx, sy, sz = field.shape
    return 0.5 * jnp.sum(field.reshape(sx // 2, 2, sy // 2, 2, sz // 2, 2), axis=(1, 3, 5))


def prolong(field):
    sx, sy, sz = field.shape
    spread = jnp.broadcast_to(field[:, None, :, None, :, None], (sx, 2, sy, 2, sz, 2))
    return spread.reshape(2 * sx, 2 * sy, 2 * sz)


def cycle(right_side, level_idx):
    approx = relax_rate * right_side
    if level_idx == LEVELS - 1:
        for sweep_idx in range(COARSE_SWEEPS - 1):
            approx = approx + relax_rate * (right_side - operate(approx))
        return approx
    defect = right_side - operate(approx)
    approx = approx + prolong(cycle(restrict(defect), level_idx + 1))
    return approx + relax_rate * (right_side - operate(approx))


def reference(density, x_faces, y_faces, z_faces):
    right_side = -coupling * density
    right_side = right_side.at[0].add(x_faces[0])
    right_side = right_side.at[-1].add(x_faces[1])
    right_side = right_side.at[:, 0].add(y_faces[0])
    right_side = right_side.at[:, -1].add(y_faces[1])
    right_side = right_side.at[:, :, 0].add(z_faces[0])
    right_side = right_side.at[:, :, -1].add(z_faces[1])
    solution_field = jnp.zeros_like(right_side)
    residual = right_side
    precond = cycle(residual, 0)
    direction = precond
    gamma_now = jnp.sum(residual * precond)
    for iteration in range(ITERS):
        image = operate(direction)
        step_size = gamma_now / jnp.sum(direction * image)
        solution_field = solution_field + step_size * direction
        residual = residual - step_size * image
        if iteration + 1 < ITERS:
            precond = cycle(residual, 0)
            gamma_next = jnp.sum(residual * precond)
            direction = precond + (gamma_next / gamma_now) * direction
            gamma_now = gamma_next
    return solution_field, residual
```

```python
import functools
import itertools

import jax
import jax.numpy as jnp
from jax import lax
from jax.experimental import pallas as pl
from jax.experimental.pallas import tpu as pltpu
from jax.sharding import PartitionSpec as P

W = 1.0 / 9.0
COUPLING = 0.5
MESH = pl.DeviceIdType.MESH
REACH = 7
CUT = 8
CHUNK = 16
GROUPS = 64


def lane_of(shape):
    return lax.broadcasted_iota(jnp.int32, shape, len(shape) - 1)


def row_of(shape):
    return lax.broadcasted_iota(jnp.int32, shape, len(shape) - 2)


def roll(x, shift, axis):
    shift = shift % x.shape[axis]
    return pltpu.roll(x, shift, axis) if shift else x


def both_of(a, b):
    return b if a is None else a if b is None else a & b


def partners(g, n, reach):
    out = []
    for m in range(1, min(reach, n - 1) + 1):
        if n == 2:
            out.append((1 - 2 * g, None, None, 0, m))
        elif n == 4 and m == 1:
            inner = (g == 1) | (g == 2)
            out.append((1 - 2 * (g % 2), None, None, 0, m))
            out.append((3 - 2 * g, inner, inner, 1, m))
        elif n == 4 and m == 2:
            out.append((2 - 4 * (g // 2), None, None, 0, m))
        else:
            out.append((m, g + m < n, g - m >= 0, 2 * m - 1, m))
            out.append((-m, g - m >= 0, g + m < n, 2 * m, m))
    return out


def knows_all(ns, kx, ky):
    return ns[0] - 1 <= 3 * kx and ns[1] - 1 <= 3 * ky and ns[2] - 1 <= 3


def kernel(
    ns, bx, by, bz, kx, ky,
    den_in, xf_in, yf_in, zf_in, field_out, residual_out,
    fld, ysrc, yrec, zsrc, zrec, xyrec, pk,
    tu, tx, ty, shrink, grow, dsrc, dside, win, wside, prol, sums, blank,
    vfld, vpk, zfld, zpk, den, xf, yf, zf,
    fsend, frecv, dsend, drecv, ssend, srecv, isem,
):
    nx, ny, nz = ns
    gx, gy, gz = (lax.axis_index(a) for a in ("gx", "gy", "gz"))
    hx, hy, hz = bx // 2, by // 2, bz // 2
    q = bz // 4
    me = (gx * ny + gy) * nz + gz
    total = nx * ny * nz
    f32 = jnp.float32
    bf16 = jnp.bfloat16

    loads = [
        pltpu.make_async_copy(a, b, isem.at[i])
        for i, (a, b) in enumerate(((den_in, den), (xf_in, xf), (yf_in, yf), (zf_in, zf)))
    ]
    for load in loads:
        load.start()

    here = [(0, None, None, 0, 0)]
    window = []
    for o in itertools.product(here + partners(gx, nx, kx), here + partners(gy, ny, ky), here + partners(gz, nz, 1)):
        d, send, recv, key, far = zip(*o)
        if any(far):
            window.append((d, functools.reduce(both_of, send), functools.reduce(both_of, recv), key, far))
    window.sort(key=lambda item: -sum(f > 0 for f in item[4]))

    def at(d):
        return (gx + d[0], gy + d[1], gz + d[2])

    def only(cond, do):
        if cond is None:
            do()
        else:
            pl.when(cond)(do)

    def clear(c):
        for ref in (fld, yrec, zrec, xyrec, win, wside):
            ref[c] = jnp.zeros(ref.shape[1:], f32)

    clear(0)
    barrier = pltpu.get_barrier_semaphore()
    if knows_all(ns, kx, ky):
        callers = 0
        for d, send, recv, _, _ in window:
            only(send, lambda d=d: pl.semaphore_signal(barrier, inc=1, device_id=at(d), device_id_type=MESH))
            callers = callers + (1 if recv is None else jnp.where(recv, 1, 0))
    else:
        callers = total - 1

        def greet(step, c):
            o = lax.rem(me + step, total)
            to = (o // (ny * nz), lax.rem(o // nz, ny), lax.rem(o, nz))
            pl.semaphore_signal(barrier, inc=1, device_id=to, device_id_type=MESH)
            return c

        lax.fori_loop(1, total, greet, 0)

    clear(1)
    pk[...] = jnp.zeros_like(pk)
    tx[...] = jnp.zeros_like(tx)

    lj = lane_of((bz, bz))
    li = row_of((bz, bz))
    maps = (
        ((lj - q + hz) % hz, lj >= 0),
        (hz - CUT + lj % CHUNK, lj % CHUNK <= CUT),
        (lj % CHUNK - 1, lj % CHUNK <= CUT),
        (jnp.where(lj < q, -1, hz), (lj < q) | (lj >= q + hz)),
    )
    for i, (col, ok) in enumerate(maps):
        ok = ok & ((col >= 0) | (gz > 0)) & ((col < hz) | (gz < nz - 1))
        cell = (li // 2 == col) & ok
        outer = ((li == 2 * col - 1) | (li == 2 * col + 2)) & ok
        shrink[0:bz, i * bz : (i + 1) * bz] = jnp.where(cell, 0.5, 0.0).astype(bf16)
        shrink[bz : 2 * bz, i * bz : (i + 1) * bz] = jnp.where(outer, 0.5, 0.0).astype(bf16)
    grow[...] = jnp.where(li == q + lj // 2, 1.0, 0.0).astype(bf16)

    for load in loads:
        load.wait()

    lane = lane_of((by, bz))
    eye = row_of((by, by)) == lane_of((by, by))
    row = row_of((by, bz))
    planes = []
    for p in range(bx):
        r = -COUPLING * den[p]
        if p == 0:
            r = r + jnp.where(gx == 0, xf[0], 0.0)
        if p == bx - 1:
            r = r + jnp.where(gx == nx - 1, xf[1], 0.0)
        r = r + jnp.where((row == 0) & (gy == 0), yf[0, p : p + 1, :], 0.0)
        r = r + jnp.where((row == by - 1) & (gy == ny - 1), yf[1, p : p + 1, :], 0.0)
        for side, (a, edge) in enumerate(((0, 0), (bz - 1, nz - 1))):
            col = jnp.sum(jnp.where(eye, zf[side, p : p + 1, :], 0.0), axis=1, keepdims=True)
            r = r + jnp.where((lane == a) & (gz == edge), col, 0.0)
        planes.append(r)
    r0 = jnp.stack(planes)

    lane8 = lane_of((8, bz))
    lanef = lane_of((by + 16, bz))
    halves = by // 8
    own = pl.ds(8, by)

    def start(items, ssem, rsem):
        for d, send, _, key, _, src, dst in items:
            k = group(key)
            only(send, lambda d=d, src=src, dst=dst, k=k: pltpu.make_async_remote_copy(
                src, dst, ssem.at[k], rsem.at[k], device_id=at(d), device_id_type=MESH
            ).start())

    def group(key):
        return (key[0] * (2 * ky + 1) + key[1]) * 3 + key[2]

    def tiles(ref):
        n = 1
        for s in ref.shape:
            n *= s
        return n // (8 * bz)

    def arrive(items, sem, which):
        counts = {}
        for item in items:
            k = group(item[3])
            counts[k] = (counts.get(k, (0, None))[0] + tiles(item[6]), item[which])
        for k, (n, cond) in counts.items():
            room = blank.at[pl.ds(0, n)]
            only(cond, lambda room=room, k=k: pltpu.make_async_copy(room, room, sem.at[k]).wait())

    def halo(c):
        f = fld.at[c]
        out = []
        for d, send, recv, key, far in window:
            if max(far) > 1 or sum(far) > 2:
                continue
            dx, dy, dz = d
            if far == (1, 0, 0):
                src = f.at[pl.ds(2 + (bx - 2) * ((dx + 1) // 2), 2), own]
                dst = f.at[pl.ds((bx + 2) * ((1 - dx) // 2), 2), own]
            elif far == (0, 1, 0):
                src, dst = ysrc.at[c, (dy + 1) // 2], yrec.at[c, (1 - dy) // 2]
            elif far == (1, 1, 0):
                src, dst = ysrc.at[c, (dy + 1) // 2, 0], xyrec.at[c, (1 - dx) + (1 - dy) // 2]
            else:
                slot = 1 + (1 - dx) // 2 if far[0] else 3 + (1 - dy) // 2 if far[1] else 0
                src, dst = zsrc.at[c, (dz + 1) // 2], zrec.at[c, (1 - dz) // 2, slot]
            out.append((d, send, recv, key, far, src, dst))
        return out

    def gathered(c):
        out = []
        for d, send, recv, key, far in window:
            dx, dy, dz = d
            rows = pl.ds(pl.multiple_of((ky - dy) * hy, 8), hy)
            if far[2]:
                src, dst = dside.at[c, (dz + 1) // 2], wside.at[c, (1 - dz) // 2, kx - dx, rows]
            else:
                src, dst = dsrc.at[c], win.at[c, pl.ds((kx - dx) * 4, 4), rows]
            out.append((d, send, recv, key, far, src, dst))
        return out

    def split(x):
        parts = []
        for _ in range(3):
            part = x.astype(bf16)
            x = x - part.astype(f32)
            parts.append(part)
        return parts

    center = (lane8 >= q) & (lane8 < q + hz)

    def send_halo(c, value):
        fld[c, 2 : bx + 2, 8 : 8 + by, :] = value
        for p in range(bx):
            for d in (0, 1):
                ysrc[c, 0, d, p : p + 1, :] = value[p, d : d + 1, :]
                ysrc[c, 1, d, p : p + 1, :] = value[p, by - 1 - d : by - d, :]
        for side, a in ((0, 0), (1, bz - 2)):
            out = jnp.zeros((8, bz), f32)
            for h in range(halves):
                for p in range(bx):
                    to = 2 * (h * bx + p)
                    moved = roll(value[p, 8 * h : 8 * h + 8, :], to - a, 1)
                    out = jnp.where(lane8 // 2 == to // 2, moved, out)
            zsrc[c, side] = out

    def send_coarse(c, v):
        for i in range(hx):
            pair = v[2 * i] + v[2 * i + 1]
            ends = (v[2 * i - 1] if i else 0.0) + (v[2 * i + 2] if i < hx - 1 else 0.0)
            tu[i] = (1.0 - 3.0 * W) * pair + W * ends
            tx[i, 8 : 8 + by, :] = pair
            ty[i : i + 1, :] = jnp.where(gy > 0, W, 0.0) * pair[0:1]
            ty[hx + i : hx + i + 1, :] = jnp.where(gy < ny - 1, W, 0.0) * pair[by - 1 : by]
        tu[hx] = jnp.where(gx > 0, W, 0.0) * v[0]
        tu[hx + 1] = jnp.where(gx < nx - 1, W, 0.0) * v[bx - 1]

        def rows(ref, a):
            return ref[:, pl.ds(a, hy, stride=2), :]

        g = rows(tu, 0) + rows(tu, 1)
        outer = W * (rows(tx, 7) + rows(tx, 10))
        side = W * (rows(tx, 8) + rows(tx, 9))
        n = hx * hy
        left = jnp.concatenate(
            [(g[:hx] + outer).reshape(n, bz), g[hx:].reshape(2 * hy, bz), ty[...], jnp.zeros((8, bz), f32)]
        )
        right = jnp.concatenate([side.reshape(n, bz), jnp.zeros((2 * hy + 16, bz), f32)])
        m = left.shape[0]
        x = jnp.concatenate([left, right], axis=1)
        y = jnp.dot(jnp.concatenate(split(x)), shrink[...], preferred_element_type=f32)
        y = y[:m] + y[m : 2 * m] + y[2 * m :]

        def piece(i, k):
            return y[8 * i : 8 * i + 8, k * bz : (k + 1) * bz]

        for i in range(hx // 2 + 1):
            dsrc[c, i] = jnp.where(center, piece(2 * i, 0), piece(2 * i + 1, 0))
        skin = jnp.where(center, piece(hx + 2, 0), 0.0)
        for i in range(hx):
            skin = jnp.where((lane8 == q - 1 - 2 * i) | (lane8 == q + hz + 2 * i), piece(i, 3), skin)
        dsrc[c, hx // 2 + 1] = skin
        for s, k in ((1, 1), (0, 2)):
            out = jnp.zeros((8, bz), f32)
            for i in range(hx + 3):
                out = jnp.where(lane8 // CHUNK == i, piece(i, k), out)
            dside[c, s] = out
        for i in range(hx // 2 + 2):
            win[c, kx * 4 + i, ky * hy : (ky + 1) * hy, :] = dsrc[c, i]

    def place_halo(c):
        for p in range(bx):
            for d in (0, 1):
                fld[c, p + 2, 7 - d : 8 - d, :] = yrec[c, 0, d, p : p + 1, :]
                fld[c, p + 2, 8 + by + d : 9 + by + d, :] = yrec[c, 1, d, p : p + 1, :]
        for i in range(4):
            plane, p = ((1, bx - 1), (bx + 2, 0))[i // 2]
            a = (7, 8 + by)[i % 2]
            fld[c, plane, a : a + 1, :] = xyrec[c, i, p : p + 1, :]
        for side in (0, 1):
            t = [zrec[c, side, i] for i in range(5)]
            for h in range(halves):
                o = jnp.where((lane8 >= 4) & (lane8 < 4 + 2 * bx), roll(t[0], 4 - 2 * bx * h, 1), 0.0)
                o = jnp.where(lane8 // 2 == 1, roll(t[1], 2 - 2 * (bx * h + bx - 1), 1), o)
                o = jnp.where(lane8 // 2 == bx + 2, roll(t[2], 2 * (bx + 2) - 2 * bx * h, 1), o)
                pk[c, side, 8 + 8 * h : 16 + 8 * h, :] = o
            inner = (lane8 >= 4) & (lane8 < 4 + 2 * bx)
            before = jnp.where(inner, roll(t[3], 4 - 2 * bx * (halves - 1), 1), 0.0)
            after = jnp.where(inner, roll(t[4], 4, 1), 0.0)
            pk[c, side, 7:8, :] = before[7:8]
            pk[c, side, 8 + by : 9 + by, :] = after[0:1]

    def operate(ref, packed, i, a, b):
        c = ref[i, a:b, :]
        ln = lane_of(c.shape)
        s = ref[i - 1, a:b, :] + ref[i + 1, a:b, :]
        s = s + ref[i, a - 1 : b - 1, :] + ref[i, a + 1 : b + 1, :]
        s = s + jnp.where(ln == 0, packed[0, a:b, 2 * i + 1 : 2 * i + 2], roll(c, 1, 1))
        s = s + jnp.where(ln == bz - 1, packed[1, a:b, 2 * i : 2 * i + 1], roll(c, -1, 1))
        return 6.0 * c - s

    wy = (2 * ky + 1) * hy
    ex = kx * hx
    ey = ky * hy

    def dims(n0, n1, half):
        shape = (n1 - n0, wy, bz)
        x = lax.broadcasted_iota(jnp.int32, shape, 0) + n0
        y = lax.broadcasted_iota(jnp.int32, shape, 1)
        z = lax.broadcasted_iota(jnp.int32, shape, 2)
        x = x + (gx * hx - ex) // half
        y = y + gy * hy - ey
        z = z + gz * hz - q
        return (
            (x >= 0) & (x < nx * hx // half) & (y >= 0) & (y < ny * hy) & (z >= 0) & (z < nz * hz)
        )

    def beside(v, step):
        m = v[1:-1]
        s = v[:-2] + v[2:]
        s = s + roll(m, step, 1) + roll(m, -step, 1)
        return s + roll(m, step, 2) + roll(m, -step, 2)

    def twin(v, axis):
        even = lax.broadcasted_iota(jnp.int32, v.shape, axis) % 2 == 0
        return v + jnp.where(even, roll(v, -1, axis), roll(v, 1, axis))

    zi = lane_of((wy, bz))
    yi = row_of((wy, bz))
    mid = (zi >= q) & (zi < q + hz)
    low, high = (zi >= q - CUT) & (zi <= q), (zi >= q + hz - 1) & (zi < q + hz + CUT)

    def assemble(c, a0, a1):
        def spread(i, k):
            l = roll(wside[c, 0, i], q - CUT - CHUNK * k, 1)
            h = roll(wside[c, 1, i], q + hz - 1 - CHUNK * k, 1)
            return jnp.where(low, l, 0.0) + jnp.where(high, h, 0.0)

        def plane(i, k):
            t = roll(win[c, 4 * i + k // 2], hz * (k % 2), 1)
            return jnp.where(mid, t, 0.0) + spread(i, k)

        skins = [win[c, 4 * i + hx // 2 + 1] for i in range(2 * kx + 1)]
        ends = [jnp.where(mid, s, 0.0) + spread(i, hx + 2) for i, s in enumerate(skins)]
        d = []
        for p in range(a0, a1):
            i, k = p // hx, p % hx
            t = plane(i, k)
            if k == 0 and i > 0:
                t = t + plane(i - 1, hx + 1)
            if k == hx - 1 and i < 2 * kx:
                t = t + plane(i + 1, hx)
            t = t + jnp.where(yi % hy == hy - 1, roll(ends[i], -(k + 1), 0), 0.0)
            t = t + jnp.where(yi % hy == 0, roll(ends[i], hx - k, 0), 0.0)
            t = t + jnp.where(zi == q - 1, roll(skins[i], 2 * k, 1), 0.0)
            t = t + jnp.where(zi == q + hz, roll(skins[i], -2 * k, 1), 0.0)
            d.append(t)
        return jnp.stack(d)

    def coarse(c):
        a0, a1 = ex - REACH, ex + hx + REACH
        d = assemble(c, a0, a1)
        v = W * d
        defect = d[1:-1] - (6.0 * v[1:-1] - beside(v, 1))
        n = defect.shape[0] // 2
        defect = defect.reshape(n, 2, wy, bz)
        r = 0.5 * twin(twin(defect[:, 0] + defect[:, 1], 1), 2)
        b0 = (a0 + 1) // 2
        m2 = dims(b0, b0 + n, 2)
        r = jnp.where(m2, r, 0.0)
        e = W * r
        e = jnp.where(m2[1:-1], e[1:-1] + W * (r[1:-1] - (6.0 * e[1:-1] - beside(e, 2))), 0.0)
        r = r[2:-2]
        e = jnp.where(m2[2:-2], e[1:-1] + W * (r - (6.0 * e[1:-1] - beside(e, 2))), 0.0)
        k0 = (b0 + 2) * 2 - a0
        spread = jnp.stack([e, e], axis=1).reshape(2 * e.shape[0], wy, bz)
        d = d[k0 : k0 + spread.shape[0]]
        v = W * d + spread
        out = v[1:-1] + W * (d[1:-1] - (6.0 * v[1:-1] - beside(v, 1)))
        p0 = (b0 + 2) * 2 + 1
        return jnp.where(dims(p0, p0 + out.shape[0], 1), out, 0.0), p0

    def dot(x, m):
        out = None
        for part in split(x):
            y = jnp.dot(part, m, preferred_element_type=f32)
            out = y if out is None else out + y
        return out

    def cycle_and_image(c, r):
        send_halo(c, r)
        if c == 0:
            pl.semaphore_wait(barrier, callers)
        start(halo(c), fsend.at[c], frecv.at[c])
        send_coarse(c, r)
        start(gathered(c), dsend.at[c], drecv.at[c])
        arrive(halo(c), frecv.at[c], 2)
        place_halo(c)
        rref = fld.at[c]
        arrive(gathered(c), drecv.at[c], 2)
        e1, p0 = coarse(c)
        e1 = e1[ex - 1 - p0 : ex + hx + 1 - p0, ey - 4 : ey + hy + 4]
        n = hy + 8
        prol[:, pl.ds(0, n, stride=2), :] = e1
        prol[:, pl.ds(1, n, stride=2), :] = e1
        for side, a in ((0, q - 1), (1, q + hz)):
            o = W * pk[c, side]
            for j in range(hx + 2):
                o = o + jnp.where(lanef // 4 == j, prol[j, :, a : a + 1], 0.0)
            vpk[side] = o
        fine = dot(prol[...].reshape((hx + 2) * 2 * n, bz), grow[...]).reshape(hx + 2, 2 * n, bz)
        for i in range(bx + 4):
            vfld[i] = W * rref[i] + fine[i // 2]
        for i in range(1, bx + 3):
            a, b = 7, 9 + by
            z = vfld[i, a:b, :] + W * (rref[i, a:b, :] - operate(vfld, vpk, i, a, b))
            zrow = lax.broadcasted_iota(jnp.int32, z.shape, 0)
            inside = ((zrow > 0) | (gy > 0)) & ((zrow < by + 1) | (gy < ny - 1))
            if i == 1:
                inside = inside & (gx > 0)
            if i == bx + 2:
                inside = inside & (gx < nx - 1)
            zfld[i, a:b, :] = jnp.where(inside, z, 0.0)
        for side, a in ((0, 0), (1, bz - 1)):
            o = vpk[side]
            s = roll(o, 2, 1) + roll(o, -2, 1) + roll(o, 1, 0) + roll(o, -1, 0)
            s = s + roll(o, 1 - 2 * side, 1)
            for i in range(2, bx + 2):
                s = s + jnp.where(lanef == 2 * i + 1 - side, vfld[i, :, a : a + 1], 0.0)
            inside = gz < nz - 1 if side else gz > 0
            zpk[side] = jnp.where(inside, o + W * (pk[c, side] - (6.0 * o - s)), 0.0)
        z = zfld[2 : bx + 2, 8 : 8 + by, :]
        return z, jnp.stack([operate(zfld, zpk, i, 8, 8 + by) for i in range(2, bx + 2)])

    z0, w = cycle_and_image(0, r0)
    u, aw = cycle_and_image(1, w)

    pairs = ((r0, z0), (z0, w), (r0, u), (w, u), (u, aw), (z0, aw))
    l1 = lane_of((1, bz))
    mine = jnp.zeros((1, bz), f32)
    for i, (a, b) in enumerate(pairs):
        s = jnp.sum(jnp.sum(jnp.sum(a * b, axis=0), axis=0, keepdims=True), axis=1, keepdims=True)
        mine = jnp.where(l1 == i, s, mine)
    sums[me] = mine

    def share(to):
        pltpu.make_async_remote_copy(
            sums.at[me], sums.at[me], ssend.at[0], srecv.at[0], device_id=to, device_id_type=MESH
        ).start()

    if total <= GROUPS:
        ways = [[lax.rem(g + j, n) for j in range(n)] for g, n in zip((gx, gy, gz), ns)]
        for j in sorted(itertools.product(*(range(n) for n in ns)), key=lambda j: -sum(min(a, n - a) for a, n in zip(j, ns))):
            if any(j):
                share(tuple(way[a] for way, a in zip(ways, j)))
    else:

        def step(i, carry):
            o = lax.rem(me + i, total)
            share((o // (ny * nz), lax.rem(o // nz, ny), lax.rem(o, nz)))
            return carry

        lax.fori_loop(1, total, step, 0)

    rest = sums.at[pl.ds(0, total - 1)]
    pltpu.make_async_copy(rest, rest, srecv.at[0]).wait()
    tot = jnp.sum(sums[...], axis=0)

    def scalar(i):
        return jnp.sum(jnp.where(l1 == i, tot, 0.0), axis=1, keepdims=True)

    g0, d0, ru, wu, uv, zv = (scalar(i) for i in range(6))
    a = g0 / d0
    g1 = (g0 - a * d0) - a * ru + a * a * wu
    beta = g1 / g0
    zaz = d0 - a * (wu + zv) + a * a * uv
    cross = (d0 - a * wu) + (d0 - a * zv)
    b = g1 / (zaz + beta * cross + beta * beta * d0)
    for p in range(bx):
        d1 = (z0[p] - a * u[p]) + beta * z0[p]
        i1 = (w[p] - a * aw[p]) + beta * w[p]
        field_out[p] = a * z0[p] + b * d1
        residual_out[p] = (r0[p] - a * w[p]) - b * i1
    for c in (0, 1):
        arrive(halo(c), fsend.at[c], 1)
        arrive(gathered(c), dsend.at[c], 1)
    pltpu.make_async_copy(rest, rest, ssend.at[0]).wait()


def solution(mesh):
    ns = tuple(mesh.shape[a] for a in ("gx", "gy", "gz"))

    def local(density, x_faces, y_faces, z_faces):
        bx, by, bz = density.shape
        hx, hy = bx // 2, by // 2
        assert hx == 4 and hy == 8
        kx, ky = -(-REACH // hx), -(-REACH // hy)
        total = ns[0] * ns[1] * ns[2]
        f32 = jnp.float32
        dma = pltpu.SemaphoreType.DMA

        def vmem(*shape, dtype=f32):
            return pltpu.VMEM(shape, dtype)

        wy = (2 * ky + 1) * hy
        return pl.pallas_call(
            functools.partial(kernel, ns, bx, by, bz, kx, ky),
            out_shape=[vmem(bx, by, bz)] * 2,
            in_specs=[pl.BlockSpec(memory_space=pl.ANY)] * 4,
            out_specs=[pl.BlockSpec(memory_space=pltpu.VMEM)] * 2,
            scratch_shapes=[
                vmem(2, bx + 4, by + 16, bz),
                vmem(2, 2, 2, bx, bz),
                vmem(2, 2, 2, bx, bz),
                vmem(2, 2, 8, bz),
                vmem(2, 2, 5, 8, bz),
                vmem(2, 4, bx, bz),
                vmem(2, 2, by + 16, bz),
                vmem(hx + 2, by, bz),
                vmem(hx, by + 16, bz),
                vmem(2 * hx, bz),
                vmem(2 * bz, 4 * bz, dtype=jnp.bfloat16),
                vmem(bz, bz, dtype=jnp.bfloat16),
                vmem(2, 4, hy, bz),
                vmem(2, 2, hy, bz),
                vmem(2, (2 * kx + 1) * 4, wy, bz),
                vmem(2, 2, 2 * kx + 1, wy, bz),
                vmem(hx + 2, by + 16, bz),
                vmem(total, 1, bz),
                vmem(GROUPS, 8, bz),
                vmem(bx + 4, by + 16, bz),
                vmem(2, by + 16, bz),
                vmem(bx + 4, by + 16, bz),
                vmem(2, by + 16, bz),
                vmem(*density.shape),
                vmem(*x_faces.shape),
                vmem(*y_faces.shape),
                vmem(*z_faces.shape),
                dma((2, GROUPS)),
                dma((2, GROUPS)),
                dma((2, GROUPS)),
                dma((2, GROUPS)),
                dma((1,)),
                dma((1,)),
                dma((4,)),
            ],
            compiler_params=pltpu.CompilerParams(collective_id=0, has_side_effects=True),
        )(density, x_faces, y_faces, z_faces)

    return jax.shard_map(
        local,
        mesh=mesh,
        in_specs=(P("gx", "gy", "gz"), P(None, "gy", "gz"), P(None, "gx", "gz"), P(None, "gx", "gy")),
        out_specs=(P("gx", "gy", "gz"), P("gx", "gy", "gz")),
        check_vma=False,
    )
```

```python
import functools
import itertools

import jax
import jax.numpy as jnp
from jax import lax
from jax.experimental import pallas as pl
from jax.experimental.pallas import tpu as pltpu
from jax.sharding import PartitionSpec as P

W = 1.0 / 9.0
COUPLING = 0.5
MESH = pl.DeviceIdType.MESH
REACH = 7
CUT = 8
CHUNK = 16
ROWS = 2048


def lane_of(shape):
    return lax.broadcasted_iota(jnp.int32, shape, len(shape) - 1)


def row_of(shape):
    return lax.broadcasted_iota(jnp.int32, shape, len(shape) - 2)


def roll(x, shift, axis):
    shift = shift % x.shape[axis]
    return pltpu.roll(x, shift, axis) if shift else x


def both_of(a, b):
    return b if a is None else a if b is None else a & b


def partners(g, n, reach):
    out = []
    for m in range(1, min(reach, n - 1) + 1):
        if n == 2:
            out.append((1 - 2 * g, None, None, 0, m))
        elif n == 4 and m == 1:
            inner = (g == 1) | (g == 2)
            out.append((1 - 2 * (g % 2), None, None, 0, m))
            out.append((3 - 2 * g, inner, inner, 1, m))
        elif n == 4 and m == 2:
            out.append((2 - 4 * (g // 2), None, None, 0, m))
        else:
            out.append((m, g + m < n, g - m >= 0, 2 * m - 1, m))
            out.append((-m, g - m >= 0, g + m < n, 2 * m, m))
    return out


def knows_all(ns, kx, ky):
    return ns[0] - 1 <= 3 * kx and ns[1] - 1 <= 3 * ky and ns[2] - 1 <= 3


def kernel(
    ns, bx, by, bz, kx, ky,
    den_in, xf_in, yf_in, zf_in, field_out, residual_out,
    fld, ysrc, yrec, zsrc, zrec, xyrec, pk,
    tu, tx, ty, shrink, grow, dsrc, dside, win, wside, prol, sums, blank,
    vfld, vpk, zfld, zpk, den, xf, yf, zf,
    ssem, rsem, isem,
):
    nx, ny, nz = ns
    gx, gy, gz = (lax.axis_index(a) for a in ("gx", "gy", "gz"))
    hx, hy, hz = bx // 2, by // 2, bz // 2
    q = bz // 4
    me = (gx * ny + gy) * nz + gz
    total = nx * ny * nz
    f32 = jnp.float32
    bf16 = jnp.bfloat16

    loads = [
        pltpu.make_async_copy(a, b, isem.at[i])
        for i, a, b in ((0, den_in, den), (0, xf_in, xf), (0, yf_in, yf), (1, zf_in, zf))
    ]
    for load in loads:
        load.start()

    here = [(0, None, None, 0, 0)]
    window = []
    for o in itertools.product(here + partners(gx, nx, kx), here + partners(gy, ny, ky), here + partners(gz, nz, 1)):
        d, send, recv, key, far = zip(*o)
        if any(far):
            window.append((d, functools.reduce(both_of, send), functools.reduce(both_of, recv), key, far))
    window.sort(key=lambda item: -sum(f > 0 for f in item[4]))

    def at(d):
        return (gx + d[0], gy + d[1], gz + d[2])

    def only(cond, do):
        if cond is None:
            do()
        else:
            pl.when(cond)(do)

    def clear(c):
        for ref in (fld, yrec, zrec, xyrec, win, wside):
            ref[c] = jnp.zeros(ref.shape[1:], f32)

    clear(0)
    paired = all(n in (1, 2, 4) for n in ns)
    inner = [(g == 1) | (g == 2) for g in (gx, gy, gz)]

    def rows_of(ref):
        n = 1
        for size in ref.shape:
            n *= size
        return n // bz

    def wait_rows(n, sem):
        room = blank.at[pl.ds(0, n)]
        pltpu.make_async_copy(room, room, sem).wait()

    barrier = pltpu.get_barrier_semaphore()
    if knows_all(ns, kx, ky):
        callers = 0
        for d, send, recv, _, _ in window:
            only(send, lambda d=d: pl.semaphore_signal(barrier, inc=1, device_id=at(d), device_id_type=MESH))
            callers = callers + (1 if recv is None else jnp.where(recv, 1, 0))
    else:
        callers = total - 1

        def greet(step, c):
            o = lax.rem(me + step, total)
            to = (o // (ny * nz), lax.rem(o // nz, ny), lax.rem(o, nz))
            pl.semaphore_signal(barrier, inc=1, device_id=to, device_id_type=MESH)
            return c

        lax.fori_loop(1, total, greet, 0)

    clear(1)
    pk[...] = jnp.zeros_like(pk)
    tx[...] = jnp.zeros_like(tx)

    lj = lane_of((bz, bz))
    li = row_of((bz, bz))
    maps = (
        ((lj - q + hz) % hz, lj >= 0),
        (hz - CUT + lj % CHUNK, lj % CHUNK <= CUT),
        (lj % CHUNK - 1, lj % CHUNK <= CUT),
        (jnp.where(lj < q, -1, hz), (lj < q) | (lj >= q + hz)),
    )
    for i, (col, ok) in enumerate(maps):
        ok = ok & ((col >= 0) | (gz > 0)) & ((col < hz) | (gz < nz - 1))
        cell = (li // 2 == col) & ok
        outer = ((li == 2 * col - 1) | (li == 2 * col + 2)) & ok
        shrink[0:bz, i * bz : (i + 1) * bz] = jnp.where(cell, 0.5, 0.0).astype(bf16)
        shrink[bz : 2 * bz, i * bz : (i + 1) * bz] = jnp.where(outer, 0.5, 0.0).astype(bf16)
    grow[...] = jnp.where(li == q + lj // 2, 1.0, 0.0).astype(bf16)

    wait_rows(sum(rows_of(a) for a in (den, xf, yf)), isem.at[0])
    loads[-1].wait()

    lane = lane_of((by, bz))
    eye = row_of((by, by)) == lane_of((by, by))
    row = row_of((by, bz))
    planes = []
    for p in range(bx):
        r = -COUPLING * den[p]
        if p == 0:
            r = r + jnp.where(gx == 0, xf[0], 0.0)
        if p == bx - 1:
            r = r + jnp.where(gx == nx - 1, xf[1], 0.0)
        r = r + jnp.where((row == 0) & (gy == 0), yf[0, p : p + 1, :], 0.0)
        r = r + jnp.where((row == by - 1) & (gy == ny - 1), yf[1, p : p + 1, :], 0.0)
        for side, (a, edge) in enumerate(((0, 0), (bz - 1, nz - 1))):
            col = jnp.sum(jnp.where(eye, zf[side, p : p + 1, :], 0.0), axis=1, keepdims=True)
            r = r + jnp.where((lane == a) & (gz == edge), col, 0.0)
        planes.append(r)
    r0 = jnp.stack(planes)

    lane8 = lane_of((8, bz))
    lanef = lane_of((by + 16, bz))
    halves = by // 8
    own = pl.ds(8, by)

    def start(items, sem):
        for d, send, _, _, _, src, dst in items:
            only(send, lambda d=d, src=src, dst=dst: pltpu.make_async_remote_copy(
                src, dst, ssem.at[0], sem, device_id=at(d), device_id_type=MESH
            ).start())

    def arrive(items, sem, which, more=0):
        counts = {}
        for item in items:
            counts[item[3]] = (counts.get(item[3], (0,))[0] + rows_of(item[5]), item[which])
        if not paired:
            for n, cond in counts.values():
                only(cond, lambda n=n: wait_rows(n, sem))
            if more:
                wait_rows(more, sem)
            return
        axes = [i for i in range(3) if ns[i] == 4 and any(key[i] for key in counts)]
        for flags in itertools.product((0, 1), repeat=len(axes)):
            state, cond = dict(zip(axes, flags)), None
            for i, flag in state.items():
                cond = both_of(cond, inner[i] if flag else jnp.logical_not(inner[i]))
            n = sum(rows for key, (rows, _) in counts.items() if all(key[i] <= state.get(i, 0) for i in range(3)))
            only(cond, lambda n=n: wait_rows(n + more, sem))

    def halo(c):
        f = fld.at[c]
        out = []
        for d, send, recv, key, far in window:
            if max(far) > 1 or sum(far) > 2:
                continue
            dx, dy, dz = d
            if far == (1, 0, 0):
                src = f.at[pl.ds(2 + (bx - 2) * ((dx + 1) // 2), 2), own]
                dst = f.at[pl.ds((bx + 2) * ((1 - dx) // 2), 2), own]
            elif far == (0, 1, 0):
                src, dst = ysrc.at[c, (dy + 1) // 2], yrec.at[c, (1 - dy) // 2]
            elif far == (1, 1, 0):
                src, dst = ysrc.at[c, (dy + 1) // 2, 0], xyrec.at[c, (1 - dx) + (1 - dy) // 2]
            else:
                slot = 1 + (1 - dx) // 2 if far[0] else 3 + (1 - dy) // 2 if far[1] else 0
                src, dst = zsrc.at[c, (dz + 1) // 2], zrec.at[c, (1 - dz) // 2, slot]
            out.append((d, send, recv, key, far, src, dst))
        return out

    def gathered(c):
        out = []
        for d, send, recv, key, far in window:
            dx, dy, dz = d
            rows = pl.ds(pl.multiple_of((ky - dy) * hy, 8), hy)
            if far[2]:
                src, dst = dside.at[c, (dz + 1) // 2], wside.at[c, (1 - dz) // 2, kx - dx, rows]
            else:
                src, dst = dsrc.at[c], win.at[c, pl.ds((kx - dx) * 4, 4), rows]
            out.append((d, send, recv, key, far, src, dst))
        return out

    def split(x):
        parts = []
        for _ in range(3):
            part = x.astype(bf16)
            x = x - part.astype(f32)
            parts.append(part)
        return parts

    center = (lane8 >= q) & (lane8 < q + hz)

    def send_halo(c, value):
        fld[c, 2 : bx + 2, 8 : 8 + by, :] = value
        for p in range(bx):
            for d in (0, 1):
                ysrc[c, 0, d, p : p + 1, :] = value[p, d : d + 1, :]
                ysrc[c, 1, d, p : p + 1, :] = value[p, by - 1 - d : by - d, :]
        for side, a in ((0, 0), (1, bz - 2)):
            out = jnp.zeros((8, bz), f32)
            for h in range(halves):
                for p in range(bx):
                    to = 2 * (h * bx + p)
                    moved = roll(value[p, 8 * h : 8 * h + 8, :], to - a, 1)
                    out = jnp.where(lane8 // 2 == to // 2, moved, out)
            zsrc[c, side] = out

    def send_coarse(c, v):
        for i in range(hx):
            pair = v[2 * i] + v[2 * i + 1]
            ends = (v[2 * i - 1] if i else 0.0) + (v[2 * i + 2] if i < hx - 1 else 0.0)
            tu[i] = (1.0 - 3.0 * W) * pair + W * ends
            tx[i, 8 : 8 + by, :] = pair
            ty[i : i + 1, :] = jnp.where(gy > 0, W, 0.0) * pair[0:1]
            ty[hx + i : hx + i + 1, :] = jnp.where(gy < ny - 1, W, 0.0) * pair[by - 1 : by]
        tu[hx] = jnp.where(gx > 0, W, 0.0) * v[0]
        tu[hx + 1] = jnp.where(gx < nx - 1, W, 0.0) * v[bx - 1]

        def rows(ref, a):
            return ref[:, pl.ds(a, hy, stride=2), :]

        g = rows(tu, 0) + rows(tu, 1)
        outer = W * (rows(tx, 7) + rows(tx, 10))
        side = W * (rows(tx, 8) + rows(tx, 9))
        n = hx * hy
        left = jnp.concatenate(
            [(g[:hx] + outer).reshape(n, bz), g[hx:].reshape(2 * hy, bz), ty[...], jnp.zeros((8, bz), f32)]
        )
        right = jnp.concatenate([side.reshape(n, bz), jnp.zeros((2 * hy + 16, bz), f32)])
        m = left.shape[0]
        x = jnp.concatenate([left, right], axis=1)
        y = jnp.dot(jnp.concatenate(split(x)), shrink[...], preferred_element_type=f32)
        y = y[:m] + y[m : 2 * m] + y[2 * m :]

        def piece(i, k):
            return y[8 * i : 8 * i + 8, k * bz : (k + 1) * bz]

        for i in range(hx // 2 + 1):
            dsrc[c, i] = jnp.where(center, piece(2 * i, 0), piece(2 * i + 1, 0))
        skin = jnp.where(center, piece(hx + 2, 0), 0.0)
        for i in range(hx):
            skin = jnp.where((lane8 == q - 1 - 2 * i) | (lane8 == q + hz + 2 * i), piece(i, 3), skin)
        dsrc[c, hx // 2 + 1] = skin
        for s, k in ((1, 1), (0, 2)):
            out = jnp.zeros((8, bz), f32)
            for i in range(hx + 3):
                out = jnp.where(lane8 // CHUNK == i, piece(i, k), out)
            dside[c, s] = out
        for i in range(hx // 2 + 2):
            win[c, kx * 4 + i, ky * hy : (ky + 1) * hy, :] = dsrc[c, i]

    def place_halo(c):
        for p in range(bx):
            for d in (0, 1):
                fld[c, p + 2, 7 - d : 8 - d, :] = yrec[c, 0, d, p : p + 1, :]
                fld[c, p + 2, 8 + by + d : 9 + by + d, :] = yrec[c, 1, d, p : p + 1, :]
        for i in range(4):
            plane, p = ((1, bx - 1), (bx + 2, 0))[i // 2]
            a = (7, 8 + by)[i % 2]
            fld[c, plane, a : a + 1, :] = xyrec[c, i, p : p + 1, :]
        for side in (0, 1):
            t = [zrec[c, side, i] for i in range(5)]
            for h in range(halves):
                o = jnp.where((lane8 >= 4) & (lane8 < 4 + 2 * bx), roll(t[0], 4 - 2 * bx * h, 1), 0.0)
                o = jnp.where(lane8 // 2 == 1, roll(t[1], 2 - 2 * (bx * h + bx - 1), 1), o)
                o = jnp.where(lane8 // 2 == bx + 2, roll(t[2], 2 * (bx + 2) - 2 * bx * h, 1), o)
                pk[c, side, 8 + 8 * h : 16 + 8 * h, :] = o
            inner = (lane8 >= 4) & (lane8 < 4 + 2 * bx)
            before = jnp.where(inner, roll(t[3], 4 - 2 * bx * (halves - 1), 1), 0.0)
            after = jnp.where(inner, roll(t[4], 4, 1), 0.0)
            pk[c, side, 7:8, :] = before[7:8]
            pk[c, side, 8 + by : 9 + by, :] = after[0:1]

    def operate(ref, packed, i, a, b):
        c = ref[i, a:b, :]
        ln = lane_of(c.shape)
        s = ref[i - 1, a:b, :] + ref[i + 1, a:b, :]
        s = s + ref[i, a - 1 : b - 1, :] + ref[i, a + 1 : b + 1, :]
        s = s + jnp.where(ln == 0, packed[0, a:b, 2 * i + 1 : 2 * i + 2], roll(c, 1, 1))
        s = s + jnp.where(ln == bz - 1, packed[1, a:b, 2 * i : 2 * i + 1], roll(c, -1, 1))
        return 6.0 * c - s

    wy = (2 * ky + 1) * hy
    ex = kx * hx
    ey = ky * hy

    def dims(n0, n1, half):
        shape = (n1 - n0, wy, bz)
        x = lax.broadcasted_iota(jnp.int32, shape, 0) + n0
        y = lax.broadcasted_iota(jnp.int32, shape, 1)
        z = lax.broadcasted_iota(jnp.int32, shape, 2)
        x = x + (gx * hx - ex) // half
        y = y + gy * hy - ey
        z = z + gz * hz - q
        return (
            (x >= 0) & (x < nx * hx // half) & (y >= 0) & (y < ny * hy) & (z >= 0) & (z < nz * hz)
        )

    def beside(v, step):
        m = v[1:-1]
        s = v[:-2] + v[2:]
        s = s + roll(m, step, 1) + roll(m, -step, 1)
        return s + roll(m, step, 2) + roll(m, -step, 2)

    def twin(v, axis):
        even = lax.broadcasted_iota(jnp.int32, v.shape, axis) % 2 == 0
        return v + jnp.where(even, roll(v, -1, axis), roll(v, 1, axis))

    zi = lane_of((wy, bz))
    yi = row_of((wy, bz))
    mid = (zi >= q) & (zi < q + hz)
    low, high = (zi >= q - CUT) & (zi <= q), (zi >= q + hz - 1) & (zi < q + hz + CUT)

    def assemble(c, a0, a1):
        def spread(i, k):
            l = roll(wside[c, 0, i], q - CUT - CHUNK * k, 1)
            h = roll(wside[c, 1, i], q + hz - 1 - CHUNK * k, 1)
            return jnp.where(low, l, 0.0) + jnp.where(high, h, 0.0)

        def plane(i, k):
            t = roll(win[c, 4 * i + k // 2], hz * (k % 2), 1)
            return jnp.where(mid, t, 0.0) + spread(i, k)

        skins = [win[c, 4 * i + hx // 2 + 1] for i in range(2 * kx + 1)]
        ends = [jnp.where(mid, s, 0.0) + spread(i, hx + 2) for i, s in enumerate(skins)]
        d = []
        for p in range(a0, a1):
            i, k = p // hx, p % hx
            t = plane(i, k)
            if k == 0 and i > 0:
                t = t + plane(i - 1, hx + 1)
            if k == hx - 1 and i < 2 * kx:
                t = t + plane(i + 1, hx)
            t = t + jnp.where(yi % hy == hy - 1, roll(ends[i], -(k + 1), 0), 0.0)
            t = t + jnp.where(yi % hy == 0, roll(ends[i], hx - k, 0), 0.0)
            t = t + jnp.where(zi == q - 1, roll(skins[i], 2 * k, 1), 0.0)
            t = t + jnp.where(zi == q + hz, roll(skins[i], -2 * k, 1), 0.0)
            d.append(t)
        return jnp.stack(d)

    def coarse(c):
        a0, a1 = ex - REACH, ex + hx + REACH
        d = assemble(c, a0, a1)
        v = W * d
        defect = d[1:-1] - (6.0 * v[1:-1] - beside(v, 1))
        n = defect.shape[0] // 2
        defect = defect.reshape(n, 2, wy, bz)
        r = 0.5 * twin(twin(defect[:, 0] + defect[:, 1], 1), 2)
        b0 = (a0 + 1) // 2
        m2 = dims(b0, b0 + n, 2)
        r = jnp.where(m2, r, 0.0)
        e = W * r
        e = jnp.where(m2[1:-1], e[1:-1] + W * (r[1:-1] - (6.0 * e[1:-1] - beside(e, 2))), 0.0)
        r = r[2:-2]
        e = jnp.where(m2[2:-2], e[1:-1] + W * (r - (6.0 * e[1:-1] - beside(e, 2))), 0.0)
        k0 = (b0 + 2) * 2 - a0
        spread = jnp.stack([e, e], axis=1).reshape(2 * e.shape[0], wy, bz)
        d = d[k0 : k0 + spread.shape[0]]
        v = W * d + spread
        out = v[1:-1] + W * (d[1:-1] - (6.0 * v[1:-1] - beside(v, 1)))
        p0 = (b0 + 2) * 2 + 1
        return jnp.where(dims(p0, p0 + out.shape[0], 1), out, 0.0), p0

    def dot(x, m):
        out = None
        for part in split(x):
            y = jnp.dot(part, m, preferred_element_type=f32)
            out = y if out is None else out + y
        return out

    def cycle_and_image(c, r):
        send_halo(c, r)
        if c == 0:
            pl.semaphore_wait(barrier, callers)
        start(halo(c), rsem.at[2 * c])
        send_coarse(c, r)
        start(gathered(c), rsem.at[2 * c + 1])
        arrive(halo(c), rsem.at[2 * c], 2)
        place_halo(c)
        rref = fld.at[c]
        arrive(gathered(c), rsem.at[2 * c + 1], 2)
        e1, p0 = coarse(c)
        e1 = e1[ex - 1 - p0 : ex + hx + 1 - p0, ey - 4 : ey + hy + 4]
        n = hy + 8
        prol[:, pl.ds(0, n, stride=2), :] = e1
        prol[:, pl.ds(1, n, stride=2), :] = e1
        for side, a in ((0, q - 1), (1, q + hz)):
            o = W * pk[c, side]
            for j in range(hx + 2):
                o = o + jnp.where(lanef // 4 == j, prol[j, :, a : a + 1], 0.0)
            vpk[side] = o
        fine = dot(prol[...].reshape((hx + 2) * 2 * n, bz), grow[...]).reshape(hx + 2, 2 * n, bz)
        for i in range(bx + 4):
            vfld[i] = W * rref[i] + fine[i // 2]
        for i in range(1, bx + 3):
            a, b = 7, 9 + by
            z = vfld[i, a:b, :] + W * (rref[i, a:b, :] - operate(vfld, vpk, i, a, b))
            zrow = lax.broadcasted_iota(jnp.int32, z.shape, 0)
            inside = ((zrow > 0) | (gy > 0)) & ((zrow < by + 1) | (gy < ny - 1))
            if i == 1:
                inside = inside & (gx > 0)
            if i == bx + 2:
                inside = inside & (gx < nx - 1)
            zfld[i, a:b, :] = jnp.where(inside, z, 0.0)
        for side, a in ((0, 0), (1, bz - 1)):
            o = vpk[side]
            s = roll(o, 2, 1) + roll(o, -2, 1) + roll(o, 1, 0) + roll(o, -1, 0)
            s = s + roll(o, 1 - 2 * side, 1)
            for i in range(2, bx + 2):
                s = s + jnp.where(lanef == 2 * i + 1 - side, vfld[i, :, a : a + 1], 0.0)
            inside = gz < nz - 1 if side else gz > 0
            zpk[side] = jnp.where(inside, o + W * (pk[c, side] - (6.0 * o - s)), 0.0)
        z = zfld[2 : bx + 2, 8 : 8 + by, :]
        return z, jnp.stack([operate(zfld, zpk, i, 8, 8 + by) for i in range(2, bx + 2)])

    z0, w = cycle_and_image(0, r0)
    u, aw = cycle_and_image(1, w)

    pairs = ((r0, z0), (z0, w), (r0, u), (w, u), (u, aw), (z0, aw))
    l1 = lane_of((1, bz))
    mine = jnp.zeros((1, bz), f32)
    for i, (a, b) in enumerate(pairs):
        s = jnp.sum(jnp.sum(jnp.sum(a * b, axis=0), axis=0, keepdims=True), axis=1, keepdims=True)
        mine = jnp.where(l1 == i, s, mine)
    sums[me] = mine

    def share(to):
        pltpu.make_async_remote_copy(
            sums.at[me], sums.at[me], ssem.at[0], rsem.at[4], device_id=to, device_id_type=MESH
        ).start()

    if total <= 64:
        ways = [[lax.rem(g + j, n) for j in range(n)] for g, n in zip((gx, gy, gz), ns)]
        for j in sorted(itertools.product(*(range(n) for n in ns)), key=lambda j: -sum(min(a, n - a) for a, n in zip(j, ns))):
            if any(j):
                share(tuple(way[a] for way, a in zip(ways, j)))
    else:

        def step(i, carry):
            o = lax.rem(me + i, total)
            share((o // (ny * nz), lax.rem(o // nz, ny), lax.rem(o, nz)))
            return carry

        lax.fori_loop(1, total, step, 0)

    wait_rows(total - 1, rsem.at[4])
    tot = jnp.sum(sums[...], axis=0)

    def scalar(i):
        return jnp.sum(jnp.where(l1 == i, tot, 0.0), axis=1, keepdims=True)

    g0, d0, ru, wu, uv, zv = (scalar(i) for i in range(6))
    a = g0 / d0
    g1 = (g0 - a * d0) - a * ru + a * a * wu
    beta = g1 / g0
    zaz = d0 - a * (wu + zv) + a * a * uv
    cross = (d0 - a * wu) + (d0 - a * zv)
    b = g1 / (zaz + beta * cross + beta * beta * d0)
    for p in range(bx):
        d1 = (z0[p] - a * u[p]) + beta * z0[p]
        i1 = (w[p] - a * aw[p]) + beta * w[p]
        field_out[p] = a * z0[p] + b * d1
        residual_out[p] = (r0[p] - a * w[p]) - b * i1
    arrive([item for c in (0, 1) for item in halo(c) + gathered(c)], ssem.at[0], 1, total - 1)


def solution(mesh):
    ns = tuple(mesh.shape[a] for a in ("gx", "gy", "gz"))

    def local(density, x_faces, y_faces, z_faces):
        bx, by, bz = density.shape
        hx, hy = bx // 2, by // 2
        assert hx == 4 and hy == 8
        kx, ky = -(-REACH // hx), -(-REACH // hy)
        total = ns[0] * ns[1] * ns[2]
        f32 = jnp.float32
        dma = pltpu.SemaphoreType.DMA

        def vmem(*shape, dtype=f32):
            return pltpu.VMEM(shape, dtype)

        wy = (2 * ky + 1) * hy
        return pl.pallas_call(
            functools.partial(kernel, ns, bx, by, bz, kx, ky),
            out_shape=[vmem(bx, by, bz)] * 2,
            in_specs=[pl.BlockSpec(memory_space=pl.ANY)] * 4,
            out_specs=[pl.BlockSpec(memory_space=pltpu.VMEM)] * 2,
            scratch_shapes=[
                vmem(2, bx + 4, by + 16, bz),
                vmem(2, 2, 2, bx, bz),
                vmem(2, 2, 2, bx, bz),
                vmem(2, 2, 8, bz),
                vmem(2, 2, 5, 8, bz),
                vmem(2, 4, bx, bz),
                vmem(2, 2, by + 16, bz),
                vmem(hx + 2, by, bz),
                vmem(hx, by + 16, bz),
                vmem(2 * hx, bz),
                vmem(2 * bz, 4 * bz, dtype=jnp.bfloat16),
                vmem(bz, bz, dtype=jnp.bfloat16),
                vmem(2, 4, hy, bz),
                vmem(2, 2, hy, bz),
                vmem(2, (2 * kx + 1) * 4, wy, bz),
                vmem(2, 2, 2 * kx + 1, wy, bz),
                vmem(hx + 2, by + 16, bz),
                vmem(total, 1, bz),
                vmem(ROWS, 1, bz),
                vmem(bx + 4, by + 16, bz),
                vmem(2, by + 16, bz),
                vmem(bx + 4, by + 16, bz),
                vmem(2, by + 16, bz),
                vmem(*density.shape),
                vmem(*x_faces.shape),
                vmem(*y_faces.shape),
                vmem(*z_faces.shape),
                dma((1,)),
                dma((5,)),
                dma((2,)),
            ],
            compiler_params=pltpu.CompilerParams(collective_id=0, has_side_effects=True),
        )(density, x_faces, y_faces, z_faces)

    return jax.shard_map(
        local,
        mesh=mesh,
        in_specs=(P("gx", "gy", "gz"), P(None, "gy", "gz"), P(None, "gx", "gz"), P(None, "gx", "gy")),
        out_specs=(P("gx", "gy", "gz"), P("gx", "gy", "gz")),
        check_vma=False,
    )
```

```python
import functools
import itertools

import jax
import jax.numpy as jnp
from jax import lax
from jax.experimental import pallas as pl
from jax.experimental.pallas import tpu as pltpu
from jax.sharding import PartitionSpec as P

W = 1.0 / 9.0
COUPLING = 0.5
MESH = pl.DeviceIdType.MESH
REACH = 7
CUT = 8
CHUNK = 16
ROWS = 2048


def lane_of(shape):
    return lax.broadcasted_iota(jnp.int32, shape, len(shape) - 1)


def row_of(shape):
    return lax.broadcasted_iota(jnp.int32, shape, len(shape) - 2)


def roll(x, shift, axis):
    shift = shift % x.shape[axis]
    return pltpu.roll(x, shift, axis) if shift else x


def both_of(a, b):
    return b if a is None else a if b is None else a & b


def partners(g, n, reach):
    out = []
    for m in range(1, min(reach, n - 1) + 1):
        if n == 2:
            out.append((1 - 2 * g, None, None, 0, m))
        elif n == 4 and m == 1:
            inner = (g == 1) | (g == 2)
            out.append((1 - 2 * (g % 2), None, None, 0, m))
            out.append((3 - 2 * g, inner, inner, 1, m))
        elif n == 4 and m == 2:
            out.append((2 - 4 * (g // 2), None, None, 0, m))
        else:
            out.append((m, g + m < n, g - m >= 0, 2 * m - 1, m))
            out.append((-m, g - m >= 0, g + m < n, 2 * m, m))
    return out


def knows_all(ns, kx, ky):
    return ns[0] - 1 <= 3 * kx and ns[1] - 1 <= 3 * ky and ns[2] - 1 <= 3


def kernel(
    ns, bx, by, bz, kx, ky,
    den_in, xf_in, yf_in, zf_in, both,
    fld, ysrc, yrec, zsrc, zrec, xyrec, pk,
    tu, tx, ty, shrink, grow, dsrc, dside, win, wside, prol, sums, blank,
    wedge, wd, pair, wb, wr, we, wv, vfld, vpk, zfld, zpk, den, xf, yf, zf,
    ssem, rsem, isem,
):
    nx, ny, nz = ns
    gx, gy, gz = (lax.axis_index(a) for a in ("gx", "gy", "gz"))
    hx, hy, hz = bx // 2, by // 2, bz // 2
    q = bz // 4
    me = (gx * ny + gy) * nz + gz
    total = nx * ny * nz
    f32 = jnp.float32
    bf16 = jnp.bfloat16

    loads = [
        pltpu.make_async_copy(a, b, isem.at[i])
        for i, a, b in ((0, den_in, den), (0, xf_in, xf), (0, yf_in, yf), (1, zf_in, zf))
    ]
    for load in loads:
        load.start()

    here = [(0, None, None, 0, 0)]
    window = []
    for o in itertools.product(here + partners(gx, nx, kx), here + partners(gy, ny, ky), here + partners(gz, nz, 1)):
        d, send, recv, key, far = zip(*o)
        if any(far):
            window.append((d, functools.reduce(both_of, send), functools.reduce(both_of, recv), key, far))
    window.sort(key=lambda item: -sum(f > 0 for f in item[4]))

    def at(d):
        return (gx + d[0], gy + d[1], gz + d[2])

    def only(cond, do):
        if cond is None:
            do()
        else:
            pl.when(cond)(do)

    def clear(c):
        for ref in (fld, yrec, zrec, xyrec, win, wside):
            ref[c] = jnp.zeros(ref.shape[1:], f32)

    clear(0)
    paired = all(n in (1, 2, 4) for n in ns)
    inner = [(g == 1) | (g == 2) for g in (gx, gy, gz)]

    def rows_of(ref):
        n = 1
        for size in ref.shape:
            n *= size
        return n // bz

    def wait_rows(n, sem):
        room = blank.at[pl.ds(0, n)]
        pltpu.make_async_copy(room, room, sem).wait()

    barrier = pltpu.get_barrier_semaphore()
    if knows_all(ns, kx, ky):
        callers = 0
        for d, send, recv, _, _ in window:
            only(send, lambda d=d: pl.semaphore_signal(barrier, inc=1, device_id=at(d), device_id_type=MESH))
            callers = callers + (1 if recv is None else jnp.where(recv, 1, 0))
    else:
        callers = total - 1

        def greet(step, c):
            o = lax.rem(me + step, total)
            to = (o // (ny * nz), lax.rem(o // nz, ny), lax.rem(o, nz))
            pl.semaphore_signal(barrier, inc=1, device_id=to, device_id_type=MESH)
            return c

        lax.fori_loop(1, total, greet, 0)

    clear(1)
    pk[...] = jnp.zeros_like(pk)
    tx[...] = jnp.zeros_like(tx)
    for ref in (wedge, wd, pair, wb, wr, we, wv):
        rim = jnp.zeros((ref.shape[0], 8, bz), f32)
        ref[:, 0:8, :] = rim
        ref[:, ref.shape[1] - 8 :, :] = rim

    lj = lane_of((bz, bz))
    li = row_of((bz, bz))
    maps = (
        ((lj - q + hz) % hz, lj >= 0),
        (hz - CUT + lj % CHUNK, lj % CHUNK <= CUT),
        (lj % CHUNK - 1, lj % CHUNK <= CUT),
        (jnp.where(lj < q, -1, hz), (lj < q) | (lj >= q + hz)),
    )
    for i, (col, ok) in enumerate(maps):
        ok = ok & ((col >= 0) | (gz > 0)) & ((col < hz) | (gz < nz - 1))
        cell = (li // 2 == col) & ok
        outer = ((li == 2 * col - 1) | (li == 2 * col + 2)) & ok
        shrink[0:bz, i * bz : (i + 1) * bz] = jnp.where(cell, 0.5, 0.0).astype(bf16)
        shrink[bz : 2 * bz, i * bz : (i + 1) * bz] = jnp.where(outer, 0.5, 0.0).astype(bf16)
    grow[...] = jnp.where(li == q + lj // 2, 1.0, 0.0).astype(bf16)

    wait_rows(sum(rows_of(a) for a in (den, xf, yf)), isem.at[0])
    loads[-1].wait()

    lane = lane_of((by, bz))
    eye = row_of((by, by)) == lane_of((by, by))
    row = row_of((by, bz))
    planes = []
    for p in range(bx):
        r = -COUPLING * den[p]
        if p == 0:
            r = r + jnp.where(gx == 0, xf[0], 0.0)
        if p == bx - 1:
            r = r + jnp.where(gx == nx - 1, xf[1], 0.0)
        r = r + jnp.where((row == 0) & (gy == 0), yf[0, p : p + 1, :], 0.0)
        r = r + jnp.where((row == by - 1) & (gy == ny - 1), yf[1, p : p + 1, :], 0.0)
        for side, (a, edge) in enumerate(((0, 0), (bz - 1, nz - 1))):
            col = jnp.sum(jnp.where(eye, zf[side, p : p + 1, :], 0.0), axis=1, keepdims=True)
            r = r + jnp.where((lane == a) & (gz == edge), col, 0.0)
        planes.append(r)
    r0 = jnp.stack(planes)

    lane8 = lane_of((8, bz))
    lanef = lane_of((by + 16, bz))
    halves = by // 8
    own = pl.ds(8, by)

    def start(items, sem):
        for d, send, _, _, _, src, dst in items:
            only(send, lambda d=d, src=src, dst=dst: pltpu.make_async_remote_copy(
                src, dst, ssem.at[0], sem, device_id=at(d), device_id_type=MESH
            ).start())

    def arrive(items, sem, which, more=0):
        counts = {}
        for item in items:
            counts[item[3]] = (counts.get(item[3], (0,))[0] + rows_of(item[5]), item[which])
        if not paired:
            for n, cond in counts.values():
                only(cond, lambda n=n: wait_rows(n, sem))
            if more:
                wait_rows(more, sem)
            return
        axes = [i for i in range(3) if ns[i] == 4 and any(key[i] for key in counts)]
        for flags in itertools.product((0, 1), repeat=len(axes)):
            state, cond = dict(zip(axes, flags)), None
            for i, flag in state.items():
                cond = both_of(cond, inner[i] if flag else jnp.logical_not(inner[i]))
            n = sum(rows for key, (rows, _) in counts.items() if all(key[i] <= state.get(i, 0) for i in range(3)))
            only(cond, lambda n=n: wait_rows(n + more, sem))

    def halo(c):
        f = fld.at[c]
        out = []
        for d, send, recv, key, far in window:
            if max(far) > 1 or sum(far) > 2:
                continue
            dx, dy, dz = d
            if far == (1, 0, 0):
                src = f.at[pl.ds(2 + (bx - 2) * ((dx + 1) // 2), 2), own]
                dst = f.at[pl.ds((bx + 2) * ((1 - dx) // 2), 2), own]
            elif far == (0, 1, 0):
                src, dst = ysrc.at[c, (dy + 1) // 2], yrec.at[c, (1 - dy) // 2]
            elif far == (1, 1, 0):
                src, dst = ysrc.at[c, (dy + 1) // 2, 0], xyrec.at[c, (1 - dx) + (1 - dy) // 2]
            else:
                slot = 1 + (1 - dx) // 2 if far[0] else 3 + (1 - dy) // 2 if far[1] else 0
                src, dst = zsrc.at[c, (dz + 1) // 2], zrec.at[c, (1 - dz) // 2, slot]
            out.append((d, send, recv, key, far, src, dst))
        return out

    def gathered(c):
        out = []
        for d, send, recv, key, far in window:
            dx, dy, dz = d
            rows = pl.ds(pl.multiple_of((ky - dy) * hy, 8), hy)
            if far[2]:
                src, dst = dside.at[c, (dz + 1) // 2], wside.at[c, (1 - dz) // 2, kx - dx, rows]
            else:
                src, dst = dsrc.at[c], win.at[c, pl.ds((kx - dx) * 4, 4), rows]
            out.append((d, send, recv, key, far, src, dst))
        return out

    def split(x):
        parts = []
        for _ in range(3):
            part = x.astype(bf16)
            x = x - part.astype(f32)
            parts.append(part)
        return parts

    center = (lane8 >= q) & (lane8 < q + hz)

    def send_halo(c, value):
        fld[c, 2 : bx + 2, 8 : 8 + by, :] = value
        for p in range(bx):
            for d in (0, 1):
                ysrc[c, 0, d, p : p + 1, :] = value[p, d : d + 1, :]
                ysrc[c, 1, d, p : p + 1, :] = value[p, by - 1 - d : by - d, :]
        for side, a in ((0, 0), (1, bz - 2)):
            out = jnp.zeros((8, bz), f32)
            for h in range(halves):
                for p in range(bx):
                    to = 2 * (h * bx + p)
                    moved = roll(value[p, 8 * h : 8 * h + 8, :], to - a, 1)
                    out = jnp.where(lane8 // 2 == to // 2, moved, out)
            zsrc[c, side] = out

    def send_coarse(c, v):
        for i in range(hx):
            pair = v[2 * i] + v[2 * i + 1]
            ends = (v[2 * i - 1] if i else 0.0) + (v[2 * i + 2] if i < hx - 1 else 0.0)
            tu[i] = (1.0 - 3.0 * W) * pair + W * ends
            tx[i, 8 : 8 + by, :] = pair
            ty[i : i + 1, :] = jnp.where(gy > 0, W, 0.0) * pair[0:1]
            ty[hx + i : hx + i + 1, :] = jnp.where(gy < ny - 1, W, 0.0) * pair[by - 1 : by]
        tu[hx] = jnp.where(gx > 0, W, 0.0) * v[0]
        tu[hx + 1] = jnp.where(gx < nx - 1, W, 0.0) * v[bx - 1]

        def rows(ref, a):
            return ref[:, pl.ds(a, hy, stride=2), :]

        g = rows(tu, 0) + rows(tu, 1)
        outer = W * (rows(tx, 7) + rows(tx, 10))
        side = W * (rows(tx, 8) + rows(tx, 9))
        n = hx * hy
        left = jnp.concatenate(
            [(g[:hx] + outer).reshape(n, bz), g[hx:].reshape(2 * hy, bz), ty[...], jnp.zeros((8, bz), f32)]
        )
        right = jnp.concatenate([side.reshape(n, bz), jnp.zeros((2 * hy + 16, bz), f32)])
        m = left.shape[0]
        x = jnp.concatenate([left, right], axis=1)
        y = jnp.dot(jnp.concatenate(split(x)), shrink[...], preferred_element_type=f32)
        y = y[:m] + y[m : 2 * m] + y[2 * m :]

        def piece(i, k):
            return y[8 * i : 8 * i + 8, k * bz : (k + 1) * bz]

        for i in range(hx // 2 + 1):
            dsrc[c, i] = jnp.where(center, piece(2 * i, 0), piece(2 * i + 1, 0))
        skin = jnp.where(center, piece(hx + 2, 0), 0.0)
        for i in range(hx):
            skin = jnp.where((lane8 == q - 1 - 2 * i) | (lane8 == q + hz + 2 * i), piece(i, 3), skin)
        dsrc[c, hx // 2 + 1] = skin
        for s, k in ((1, 1), (0, 2)):
            out = jnp.zeros((8, bz), f32)
            for i in range(hx + 3):
                out = jnp.where(lane8 // CHUNK == i, piece(i, k), out)
            dside[c, s] = out
        for i in range(hx // 2 + 2):
            win[c, kx * 4 + i, ky * hy : (ky + 1) * hy, :] = dsrc[c, i]

    def place_halo(c):
        for p in range(bx):
            for d in (0, 1):
                fld[c, p + 2, 7 - d : 8 - d, :] = yrec[c, 0, d, p : p + 1, :]
                fld[c, p + 2, 8 + by + d : 9 + by + d, :] = yrec[c, 1, d, p : p + 1, :]
        for i in range(4):
            plane, p = ((1, bx - 1), (bx + 2, 0))[i // 2]
            a = (7, 8 + by)[i % 2]
            fld[c, plane, a : a + 1, :] = xyrec[c, i, p : p + 1, :]
        for side in (0, 1):
            t = [zrec[c, side, i] for i in range(5)]
            for h in range(halves):
                o = jnp.where((lane8 >= 4) & (lane8 < 4 + 2 * bx), roll(t[0], 4 - 2 * bx * h, 1), 0.0)
                o = jnp.where(lane8 // 2 == 1, roll(t[1], 2 - 2 * (bx * h + bx - 1), 1), o)
                o = jnp.where(lane8 // 2 == bx + 2, roll(t[2], 2 * (bx + 2) - 2 * bx * h, 1), o)
                pk[c, side, 8 + 8 * h : 16 + 8 * h, :] = o
            inner = (lane8 >= 4) & (lane8 < 4 + 2 * bx)
            before = jnp.where(inner, roll(t[3], 4 - 2 * bx * (halves - 1), 1), 0.0)
            after = jnp.where(inner, roll(t[4], 4, 1), 0.0)
            pk[c, side, 7:8, :] = before[7:8]
            pk[c, side, 8 + by : 9 + by, :] = after[0:1]

    def around(ref, packed, i, a, b):
        c = ref[i, a:b, :]
        ln = lane_of(c.shape)
        s = ref[i - 1, a:b, :] + ref[i + 1, a:b, :]
        s = s + ref[i, a - 1 : b - 1, :] + ref[i, a + 1 : b + 1, :]
        s = s + jnp.where(ln == 0, packed[0, a:b, 2 * i + 1 : 2 * i + 2], roll(c, 1, 1))
        return s + jnp.where(ln == bz - 1, packed[1, a:b, 2 * i : 2 * i + 1], roll(c, -1, 1))

    wy = (2 * ky + 1) * hy
    ex = kx * hx
    ey = ky * hy

    zi = lane_of((8, bz))
    yi = row_of((8, bz))
    mid = (zi >= q) & (zi < q + hz)
    low, high = (zi >= q - CUT) & (zi <= q), (zi >= q + hz - 1) & (zi < q + hz + CUT)
    if nz == 2:
        sides = [(1 - gz, jnp.where(gz == 0, q + hz - 1, q - CUT), (high & (gz == 0)) | (low & (gz == 1)))]
    else:
        sides = [(0, q - CUT, low), (1, q + hz - 1, high)] if nz > 1 else []
    strips = [slice(8 + 8 * t, 16 + 8 * t) for t in range(wy // 8)]

    def grid_strip(t):
        y = yi + 8 * t
        ok = (y >= ey - gy * hy) & (y < ey + (ny - gy) * hy) & (zi >= q - gz * hz) & (zi < q + (nz - gz) * hz)
        return jnp.where(ok, 1.0, 0.0)

    def there(p, half):
        x = p + (gx * hx - ex) // half
        return jnp.where((x >= 0) & (x < nx * hx // half), 1.0, 0.0)

    def total_of(terms):
        while len(terms) > 1:
            terms = [a + b for a, b in zip(terms[::2], terms[1::2])] + ([terms[-1]] if len(terms) % 2 else [])
        return terms[0]

    def shifted(ref, p, t, step):
        v = ref[p, strips[t], :]
        r0 = strips[t].start
        return total_of([
            ref[p, r0 - step : r0 - step + 8, :], ref[p, r0 + step : r0 + step + 8, :],
            roll(v, step, 1), roll(v, -step, 1),
        ])

    def assemble(c, a0, a1):
        def side_of(i, k, rows):
            return [
                (m, pltpu.roll(wside[c, s, i, rows, :], (base - CHUNK * k) % bz, 1)) for s, base, m in sides
            ]

        for t, strip in enumerate(strips):
            rows = slice(8 * t, 8 * t + 8)
            for i in range(2 * kx + 1):
                e = jnp.where(mid, win[c, 4 * i + hx // 2 + 1, rows, :], 0.0)
                for m, v in side_of(i, hx + 2, rows):
                    e = e + jnp.where(m, v, 0.0)
                wedge[i, strip, :] = e
        for t, strip in enumerate(strips):
            rows = slice(8 * t, 8 * t + 8)
            for p in range(a0, a1):
                i, k = p // hx, p % hx
                parts = [(i, k)]
                if k == 0 and i > 0:
                    parts.append((i - 1, hx + 1))
                if k == hx - 1 and i < 2 * kx:
                    parts.append((i + 1, hx))
                inner_part = total_of([roll(win[c, 4 * j + f // 2, rows, :], hz * (f % 2), 1) for j, f in parts])
                terms = [jnp.where(mid, inner_part, 0.0)]
                found = [side_of(j, f, rows) for j, f in parts]
                for n, (_, _, m) in enumerate(sides):
                    terms.append(jnp.where(m, total_of([f[n][1] for f in found]), 0.0))
                up = 8 + 8 * t + k + 1
                down = 8 + 8 * t - hx + k
                terms.append(jnp.where(yi == 7, wedge[i, up : up + 8, :], jnp.where(yi == 0, wedge[i, down : down + 8, :], 0.0)))
                skin = win[c, 4 * i + hx // 2 + 1, rows, :]
                terms.append(jnp.where(zi == q - 1, roll(skin, 2 * k, 1), jnp.where(zi == q + hz, roll(skin, -2 * k, 1), 0.0)))
                wd[p - a0, strip, :] = total_of(terms)

    def coarse(c):
        a0, a1 = ex - REACH, ex + hx + REACH
        assemble(c, a0, a1)
        n = (a1 - a0) // 2 - 1
        b0 = (a0 + 1) // 2
        on2 = [there(b0 + j, 2) for j in range(n)]
        grid = [grid_strip(t) for t in range(len(strips))]
        every = list(enumerate(strips))
        for t, strip in every:
            for j in range(n):
                pair[j, strip, :] = wd[2 * j + 1, strip, :] + wd[2 * j + 2, strip, :]
        for t, strip in every:
            for j in range(n):
                ends = wd[2 * j, strip, :] + wd[2 * j + 3, strip, :]
                wb[j, strip, :] = (1.0 - 5.0 * W) * pair[j, strip, :] + W * (ends + shifted(pair, j, t, 1))
        for t, strip in every:
            for j in range(n):
                r0 = strip.start
                v = wb[j, strip, :]
                v = v + jnp.where(yi % 2 == 0, wb[j, r0 + 1 : r0 + 9, :], wb[j, r0 - 1 : r0 + 7, :])
                v = v + jnp.where(zi % 2 == 0, roll(v, -1, 1), roll(v, 1, 1))
                wr[j, strip, :] = (0.5 * on2[j]) * (grid[t] * v)
        for t, strip in every:
            for j in range(1, n - 1):
                v = (2.0 * W - 6.0 * W * W) * wr[j, strip, :]
                v = v + (W * W) * (wr[j - 1, strip, :] + wr[j + 1, strip, :] + shifted(wr, j, t, 2))
                we[j, strip, :] = on2[j] * (grid[t] * v)
        k0 = (b0 + 2) * 2 - a0
        for t, strip in every:
            for j in range(2, n - 2):
                v = wr[j, strip, :] + (we[j - 1, strip, :] + we[j + 1, strip, :] + shifted(we, j, t, 2))
                v = on2[j] * (grid[t] * ((1.0 - 6.0 * W) * we[j, strip, :] + W * v))
                for k in (2 * j - 4, 2 * j - 3):
                    wv[k, strip, :] = W * wd[k0 + k, strip, :] + v
        for t, strip in every:
            for k in range(1, 2 * n - 9):
                v = wd[k0 + k, strip, :] + (wv[k - 1, strip, :] + wv[k + 1, strip, :] + shifted(wv, k, t, 1))
                v = there(a0 + k0 + k, 1) * (grid[t] * ((1.0 - 6.0 * W) * wv[k, strip, :] + W * v))
                prol[k - 1, pl.ds(16 * t, 8, stride=2), :] = v
                prol[k - 1, pl.ds(16 * t + 1, 8, stride=2), :] = v

    def dot(x, m):
        out = None
        for part in split(x):
            y = jnp.dot(part, m, preferred_element_type=f32)
            out = y if out is None else out + y
        return out

    def cycle_and_image(c, r):
        send_halo(c, r)
        if c == 0:
            pl.semaphore_wait(barrier, callers)
        start(halo(c), rsem.at[2 * c])
        send_coarse(c, r)
        start(gathered(c), rsem.at[2 * c + 1])
        arrive(halo(c), rsem.at[2 * c], 2)
        place_halo(c)
        rref = fld.at[c]
        arrive(gathered(c), rsem.at[2 * c + 1], 2)
        coarse(c)
        kept = slice(2 * ey - 8, 2 * ey + by + 8)
        for side, a in ((0, q - 1), (1, q + hz)):
            o = W * pk[c, side]
            for j in range(hx + 2):
                o = o + jnp.where(lanef // 4 == j, prol[j, kept, a : a + 1], 0.0)
            vpk[side] = o
        fine = dot(prol[:, kept, :].reshape((hx + 2) * (by + 16), bz), grow[...]).reshape(hx + 2, by + 16, bz)
        for i in range(bx + 4):
            vfld[i] = W * rref[i] + fine[i // 2]
        for i in range(1, bx + 3):
            a, b = 7, 9 + by
            z = (1.0 - 6.0 * W) * vfld[i, a:b, :] + W * (rref[i, a:b, :] + around(vfld, vpk, i, a, b))
            zrow = lax.broadcasted_iota(jnp.int32, z.shape, 0)
            ok = ((zrow > 0) | (gy > 0)) & ((zrow < by + 1) | (gy < ny - 1))
            if i == 1:
                ok = ok & (gx > 0)
            if i == bx + 2:
                ok = ok & (gx < nx - 1)
            zfld[i, a:b, :] = jnp.where(ok, z, 0.0)
        for side, a in ((0, 0), (1, bz - 1)):
            o = vpk[side]
            s = roll(o, 2, 1) + roll(o, -2, 1) + roll(o, 1, 0) + roll(o, -1, 0)
            s = s + roll(o, 1 - 2 * side, 1)
            for i in range(2, bx + 2):
                s = s + jnp.where(lanef == 2 * i + 1 - side, vfld[i, :, a : a + 1], 0.0)
            ok = gz < nz - 1 if side else gz > 0
            zpk[side] = jnp.where(ok, (1.0 - 6.0 * W) * o + W * (pk[c, side] + s), 0.0)
        z = zfld[2 : bx + 2, 8 : 8 + by, :]
        return z, jnp.stack([6.0 * z[i - 2] - around(zfld, zpk, i, 8, 8 + by) for i in range(2, bx + 2)])

    z0, w = cycle_and_image(0, r0)
    u, aw = cycle_and_image(1, w)

    pairs = ((r0, z0), (z0, w), (r0, u), (w, u), (u, aw), (z0, aw))
    l1 = lane_of((1, bz))
    mine = jnp.zeros((1, bz), f32)
    for i, (a, b) in enumerate(pairs):
        s = jnp.sum(jnp.sum(jnp.sum(a * b, axis=0), axis=0, keepdims=True), axis=1, keepdims=True)
        mine = jnp.where(l1 == i, s, mine)
    sums[me] = mine

    def share(to):
        pltpu.make_async_remote_copy(
            sums.at[me], sums.at[me], ssem.at[0], rsem.at[4], device_id=to, device_id_type=MESH
        ).start()

    if total <= 64:
        def ways(g, n):
            return [g, g + 1 - 2 * (g % 2), lax.rem(g + 2, 4), 3 - g] if n == 4 else [lax.rem(g + j, n) for j in range(n)]

        options = [ways(g, n) for g, n in zip((gx, gy, gz), ns)]
        for j in sorted(itertools.product(*(range(n) for n in ns)), key=lambda j: -sum(j)):
            if any(j):
                share(tuple(way[i] for way, i in zip(options, j)))
    else:

        def step(i, carry):
            o = lax.rem(me + i, total)
            share((o // (ny * nz), lax.rem(o // nz, ny), lax.rem(o, nz)))
            return carry

        lax.fori_loop(1, total, step, 0)

    wait_rows(total - 1, rsem.at[4])
    tot = jnp.sum(sums[...], axis=0)

    def scalar(i):
        return jnp.sum(jnp.where(l1 == i, tot, 0.0), axis=1, keepdims=True)

    g0, d0, ru, wu, uv, zv = (scalar(i) for i in range(6))
    a = g0 / d0
    g1 = (g0 - a * d0) - a * ru + a * a * wu
    beta = g1 / g0
    zaz = d0 - a * (wu + zv) + a * a * uv
    cross = (d0 - a * wu) + (d0 - a * zv)
    b = g1 / (zaz + beta * cross + beta * beta * d0)
    for p in range(bx):
        d1 = (z0[p] - a * u[p]) + beta * z0[p]
        i1 = (w[p] - a * aw[p]) + beta * w[p]
        both[0, p] = a * z0[p] + b * d1
        both[1, p] = (r0[p] - a * w[p]) - b * i1
    arrive([item for c in (0, 1) for item in halo(c) + gathered(c)], ssem.at[0], 1, total - 1)


def solution(mesh):
    ns = tuple(mesh.shape[a] for a in ("gx", "gy", "gz"))

    def local(density, x_faces, y_faces, z_faces):
        bx, by, bz = density.shape
        hx, hy = bx // 2, by // 2
        assert hx == 4 and hy == 8
        kx, ky = -(-REACH // hx), -(-REACH // hy)
        total = ns[0] * ns[1] * ns[2]
        f32 = jnp.float32
        dma = pltpu.SemaphoreType.DMA

        def vmem(*shape, dtype=f32):
            return pltpu.VMEM(shape, dtype)

        wy = (2 * ky + 1) * hy
        pairs = hx // 2 + REACH - 1
        both = pl.pallas_call(
            functools.partial(kernel, ns, bx, by, bz, kx, ky),
            out_shape=vmem(2, bx, by, bz),
            in_specs=[pl.BlockSpec(memory_space=pl.ANY)] * 4,
            out_specs=pl.BlockSpec(memory_space=pltpu.VMEM),
            scratch_shapes=[
                vmem(2, bx + 4, by + 16, bz),
                vmem(2, 2, 2, bx, bz),
                vmem(2, 2, 2, bx, bz),
                vmem(2, 2, 8, bz),
                vmem(2, 2, 5, 8, bz),
                vmem(2, 4, bx, bz),
                vmem(2, 2, by + 16, bz),
                vmem(hx + 2, by, bz),
                vmem(hx, by + 16, bz),
                vmem(2 * hx, bz),
                vmem(2 * bz, 4 * bz, dtype=jnp.bfloat16),
                vmem(bz, bz, dtype=jnp.bfloat16),
                vmem(2, 4, hy, bz),
                vmem(2, 2, hy, bz),
                vmem(2, (2 * kx + 1) * 4, wy, bz),
                vmem(2, 2, 2 * kx + 1, wy, bz),
                vmem(hx + 2, 2 * wy, bz),
                vmem(total, 1, bz),
                vmem(ROWS, 1, bz),
                vmem(2 * kx + 1, wy + 16, bz),
                vmem(hx + 2 * REACH, wy + 16, bz),
                vmem(pairs, wy + 16, bz),
                vmem(pairs, wy + 16, bz),
                vmem(pairs, wy + 16, bz),
                vmem(pairs, wy + 16, bz),
                vmem(2 * (pairs - 4), wy + 16, bz),
                vmem(bx + 4, by + 16, bz),
                vmem(2, by + 16, bz),
                vmem(bx + 4, by + 16, bz),
                vmem(2, by + 16, bz),
                vmem(*density.shape),
                vmem(*x_faces.shape),
                vmem(*y_faces.shape),
                vmem(*z_faces.shape),
                dma((1,)),
                dma((5,)),
                dma((2,)),
            ],
            compiler_params=pltpu.CompilerParams(collective_id=0, has_side_effects=True),
        )(density, x_faces, y_faces, z_faces)
        return both[0], both[1]

    return jax.shard_map(
        local,
        mesh=mesh,
        in_specs=(P("gx", "gy", "gz"), P(None, "gy", "gz"), P(None, "gx", "gz"), P(None, "gx", "gy")),
        out_specs=(P("gx", "gy", "gz"), P("gx", "gy", "gz")),
        check_vma=False,
    )
```

```python
import functools
import itertools

import jax
import jax.numpy as jnp
from jax import lax
from jax.experimental import pallas as pl
from jax.experimental.pallas import tpu as pltpu
from jax.sharding import PartitionSpec as P

W = 1.0 / 9.0
COUPLING = 0.5
MESH = pl.DeviceIdType.MESH
REACH = 7
CUT = 8
CHUNK = 16
DOWN, UP, SKIN, TILES = 4, 5, 6, 5
ROWS = 2048


def lane_of(shape):
    return lax.broadcasted_iota(jnp.int32, shape, len(shape) - 1)


def row_of(shape):
    return lax.broadcasted_iota(jnp.int32, shape, len(shape) - 2)


def roll(x, shift, axis):
    shift = shift % x.shape[axis]
    return pltpu.roll(x, shift, axis) if shift else x


def both_of(a, b):
    return b if a is None else a if b is None else a & b


def partners(g, n, reach):
    out = []
    for m in range(1, min(reach, n - 1) + 1):
        if n == 2:
            out.append((1 - 2 * g, None, None, 0, m))
        elif n == 4 and m == 1:
            inner = (g == 1) | (g == 2)
            out.append((1 - 2 * (g % 2), None, None, 0, m))
            out.append((3 - 2 * g, inner, inner, 1, m))
        elif n == 4 and m == 2:
            out.append((2 - 4 * (g // 2), None, None, 0, m))
        else:
            out.append((m, g + m < n, g - m >= 0, 2 * m - 1, m))
            out.append((-m, g - m >= 0, g + m < n, 2 * m, m))
    return out


def chunk_of(piece):
    return piece + 2 if piece < DOWN else piece - DOWN if piece < SKIN else SKIN


def knows_all(ns, kx, ky):
    return ns[0] - 1 <= 3 * kx and ns[1] - 1 <= 3 * ky and ns[2] - 1 <= 3


def kernel(
    ns, bx, by, bz, kx, ky,
    den_in, xf_in, yf_in, zf_in, both,
    fld, ysrc, yrec, zsrc, zrec, xyrec, pk,
    tu, tx, ty, shrink, grow, dsrc, dside, win, wside, prol, sums, blank,
    wedge, beyond, wd, pair, wb, wr, we, wv, vfld, vpk, zfld, zpk, den, xf, yf, zf,
    ssem, rsem, isem,
):
    nx, ny, nz = ns
    gx, gy, gz = (lax.axis_index(a) for a in ("gx", "gy", "gz"))
    hx, hy, hz = bx // 2, by // 2, bz // 2
    q = bz // 4
    me = (gx * ny + gy) * nz + gz
    total = nx * ny * nz
    f32 = jnp.float32
    bf16 = jnp.bfloat16

    loads = [
        pltpu.make_async_copy(a, b, isem.at[i])
        for i, a, b in ((0, den_in, den), (0, xf_in, xf), (0, yf_in, yf), (1, zf_in, zf))
    ]
    for load in loads:
        load.start()

    here = [(0, None, None, 0, 0)]
    window = []
    for o in itertools.product(here + partners(gx, nx, kx), here + partners(gy, ny, ky), here + partners(gz, nz, 1)):
        d, send, recv, key, far = zip(*o)
        if any(far):
            window.append((d, functools.reduce(both_of, send), functools.reduce(both_of, recv), key, far))
    window.sort(key=lambda item: -sum(f > 0 for f in item[4]))

    def at(d):
        return (gx + d[0], gy + d[1], gz + d[2])

    def only(cond, do):
        if cond is None:
            do()
        else:
            pl.when(cond)(do)

    def clear(c):
        for ref in (fld, yrec, zrec, xyrec, win, wside):
            ref[c] = jnp.zeros(ref.shape[1:], f32)

    clear(0)
    paired = all(n in (1, 2, 4) for n in ns)
    inner = [(g == 1) | (g == 2) for g in (gx, gy, gz)]

    def rows_of(ref):
        n = 1
        for size in ref.shape:
            n *= size
        return n // bz

    def wait_rows(n, sem):
        room = blank.at[pl.ds(0, n)]
        pltpu.make_async_copy(room, room, sem).wait()

    barrier = pltpu.get_barrier_semaphore()
    if knows_all(ns, kx, ky):
        callers = 0
        for d, send, recv, _, _ in window:
            only(send, lambda d=d: pl.semaphore_signal(barrier, inc=1, device_id=at(d), device_id_type=MESH))
            callers = callers + (1 if recv is None else jnp.where(recv, 1, 0))
    else:
        callers = total - 1

        def greet(step, c):
            o = lax.rem(me + step, total)
            to = (o // (ny * nz), lax.rem(o // nz, ny), lax.rem(o, nz))
            pl.semaphore_signal(barrier, inc=1, device_id=to, device_id_type=MESH)
            return c

        lax.fori_loop(1, total, greet, 0)

    clear(1)
    pk[...] = jnp.zeros_like(pk)
    tx[...] = jnp.zeros_like(tx)
    for ref in (wedge, wd, pair, wb, wr, we, wv):
        rim = jnp.zeros((ref.shape[0], 8, bz), f32)
        ref[:, 0:8, :] = rim
        ref[:, ref.shape[1] - 8 :, :] = rim

    lj = lane_of((bz, bz))
    li = row_of((bz, bz))
    maps = (
        ((lj - q + hz) % hz, lj >= 0),
        (hz - CUT + lj % CHUNK, lj % CHUNK <= CUT),
        (lj % CHUNK - 1, lj % CHUNK <= CUT),
        (jnp.where(lj % CHUNK == 1, hz, -1), (lj % CHUNK == 1) | (lj % CHUNK == CUT - 1)),
    )
    for i, (col, ok) in enumerate(maps):
        ok = ok & ((col >= 0) | (gz > 0)) & ((col < hz) | (gz < nz - 1))
        cell = (li // 2 == col) & ok
        outer = ((li == 2 * col - 1) | (li == 2 * col + 2)) & ok
        shrink[0:bz, i * bz : (i + 1) * bz] = jnp.where(cell, 0.5, 0.0).astype(bf16)
        shrink[bz : 2 * bz, i * bz : (i + 1) * bz] = jnp.where(outer, 0.5, 0.0).astype(bf16)
    grow[...] = jnp.where(li == q + lj // 2, 1.0, 0.0).astype(bf16)

    wait_rows(sum(rows_of(a) for a in (den, xf, yf)), isem.at[0])
    loads[-1].wait()

    lane = lane_of((by, bz))
    eye = row_of((by, by)) == lane_of((by, by))
    row = row_of((by, bz))
    planes = []
    for p in range(bx):
        r = -COUPLING * den[p]
        if p == 0:
            r = r + jnp.where(gx == 0, xf[0], 0.0)
        if p == bx - 1:
            r = r + jnp.where(gx == nx - 1, xf[1], 0.0)
        r = r + jnp.where((row == 0) & (gy == 0), yf[0, p : p + 1, :], 0.0)
        r = r + jnp.where((row == by - 1) & (gy == ny - 1), yf[1, p : p + 1, :], 0.0)
        for side, (a, edge) in enumerate(((0, 0), (bz - 1, nz - 1))):
            col = jnp.sum(jnp.where(eye, zf[side, p : p + 1, :], 0.0), axis=1, keepdims=True)
            r = r + jnp.where((lane == a) & (gz == edge), col, 0.0)
        planes.append(r)
    r0 = jnp.stack(planes)

    lane8 = lane_of((8, bz))
    lanef = lane_of((by + 16, bz))
    halves = by // 8
    own = pl.ds(8, by)

    def start(items, sem):
        for d, send, _, _, _, src, dst in items:
            only(send, lambda d=d, src=src, dst=dst: pltpu.make_async_remote_copy(
                src, dst, ssem.at[0], sem, device_id=at(d), device_id_type=MESH
            ).start())

    def arrive(items, sem, which, more=0):
        counts = {}
        for item in items:
            counts[item[3]] = (counts.get(item[3], (0,))[0] + rows_of(item[5]), item[which])
        if not paired:
            for n, cond in counts.values():
                only(cond, lambda n=n: wait_rows(n, sem))
            if more:
                wait_rows(more, sem)
            return
        axes = [i for i in range(3) if ns[i] == 4 and any(key[i] for key in counts)]
        for flags in itertools.product((0, 1), repeat=len(axes)):
            state, cond = dict(zip(axes, flags)), None
            for i, flag in state.items():
                cond = both_of(cond, inner[i] if flag else jnp.logical_not(inner[i]))
            n = sum(rows for key, (rows, _) in counts.items() if all(key[i] <= state.get(i, 0) for i in range(3)))
            only(cond, lambda n=n: wait_rows(n + more, sem))

    def halo(c):
        f = fld.at[c]
        out = []
        for d, send, recv, key, far in window:
            if max(far) > 1 or sum(far) > 2:
                continue
            dx, dy, dz = d
            if far == (1, 0, 0):
                src = f.at[pl.ds(2 + (bx - 2) * ((dx + 1) // 2), 2), own]
                dst = f.at[pl.ds((bx + 2) * ((1 - dx) // 2), 2), own]
            elif far == (0, 1, 0):
                src, dst = ysrc.at[c, (dy + 1) // 2], yrec.at[c, (1 - dy) // 2]
            elif far == (1, 1, 0):
                src, dst = ysrc.at[c, (dy + 1) // 2, 0], xyrec.at[c, (1 - dx) + (1 - dy) // 2]
            else:
                slot = 1 + (1 - dx) // 2 if far[0] else 3 + (1 - dy) // 2 if far[1] else 0
                src, dst = zsrc.at[c, (dz + 1) // 2], zrec.at[c, (1 - dz) // 2, slot]
            out.append((d, send, recv, key, far, src, dst))
        return out

    def gathered(c):
        out = []
        for d, send, recv, key, far in window:
            dx, dy, dz = d
            rows = pl.ds(pl.multiple_of((ky - dy) * hy, 8), hy)
            if far[2]:
                src, dst = dside.at[c, (dz + 1) // 2], wside.at[c, (1 - dz) // 2, kx - dx, rows]
            else:
                a, n = ((dx + 2) // 2, 3) if far[0] == 2 else (0, 4)
                src, dst = dsrc.at[c, pl.ds(a, n)], win.at[c, pl.ds((kx - dx) * TILES + a, n), rows]
            out.append((d, send, recv, key, far, src, dst))
        return out

    def split(x):
        parts = []
        for _ in range(3):
            part = x.astype(bf16)
            x = x - part.astype(f32)
            parts.append(part)
        return parts

    center = (lane8 >= q) & (lane8 < q + hz)

    def send_halo(c, value):
        fld[c, 2 : bx + 2, 8 : 8 + by, :] = value
        for p in range(bx):
            for d in (0, 1):
                ysrc[c, 0, d, p : p + 1, :] = value[p, d : d + 1, :]
                ysrc[c, 1, d, p : p + 1, :] = value[p, by - 1 - d : by - d, :]
        for side, a in ((0, 0), (1, bz - 2)):
            out = jnp.zeros((8, bz), f32)
            for h in range(halves):
                for p in range(bx):
                    to = 2 * (h * bx + p)
                    moved = roll(value[p, 8 * h : 8 * h + 8, :], to - a, 1)
                    out = jnp.where(lane8 // 2 == to // 2, moved, out)
            zsrc[c, side] = out

    def send_coarse(c, v):
        for i in range(hx):
            pair = v[2 * i] + v[2 * i + 1]
            ends = (v[2 * i - 1] if i else 0.0) + (v[2 * i + 2] if i < hx - 1 else 0.0)
            tu[i] = (1.0 - 3.0 * W) * pair + W * ends
            tx[i, 8 : 8 + by, :] = pair
            ty[i : i + 1, :] = jnp.where(gy > 0, W, 0.0) * pair[0:1]
            ty[hx + i : hx + i + 1, :] = jnp.where(gy < ny - 1, W, 0.0) * pair[by - 1 : by]
        tu[hx] = jnp.where(gx > 0, W, 0.0) * v[0]
        tu[hx + 1] = jnp.where(gx < nx - 1, W, 0.0) * v[bx - 1]

        def rows(ref, a):
            return ref[:, pl.ds(a, hy, stride=2), :]

        g = rows(tu, 0) + rows(tu, 1)
        outer = W * (rows(tx, 7) + rows(tx, 10))
        side = W * (rows(tx, 8) + rows(tx, 9))
        n = hx * hy
        left = jnp.concatenate(
            [(g[:hx] + outer).reshape(n, bz), g[hx:].reshape(2 * hy, bz), ty[...], jnp.zeros((8, bz), f32)]
        )
        right = jnp.concatenate([side.reshape(n, bz), jnp.zeros((2 * hy + 16, bz), f32)])
        m = left.shape[0]
        x = jnp.concatenate([left, right], axis=1)
        y = jnp.dot(jnp.concatenate(split(x)), shrink[...], preferred_element_type=f32)
        y = y[:m] + y[m : 2 * m] + y[2 * m :]

        def piece(i, k):
            return y[8 * i : 8 * i + 8, k * bz : (k + 1) * bz]

        skin = piece(SKIN, 0)
        for i in range(hx):
            skin = jnp.where(lane8 // CHUNK == chunk_of(i), piece(i, 3), skin)
        block = [skin] + [
            jnp.where(center, piece(a, 0), piece(b, 0)) for a, b in ((0, DOWN), (2, 1), (UP, 3))
        ]
        for i, tile in enumerate(block + [skin]):
            dsrc[c, i] = tile
            win[c, kx * TILES + i, ky * hy : (ky + 1) * hy, :] = tile
        for s, k in ((1, 1), (0, 2)):
            out = jnp.zeros((8, bz), f32)
            for i in range(hx + 3):
                out = jnp.where(lane8 // CHUNK == chunk_of(i), piece(i, k), out)
            dside[c, s] = out

    def place_halo(c):
        for p in range(bx):
            for d in (0, 1):
                fld[c, p + 2, 7 - d : 8 - d, :] = yrec[c, 0, d, p : p + 1, :]
                fld[c, p + 2, 8 + by + d : 9 + by + d, :] = yrec[c, 1, d, p : p + 1, :]
        for i in range(4):
            plane, p = ((1, bx - 1), (bx + 2, 0))[i // 2]
            a = (7, 8 + by)[i % 2]
            fld[c, plane, a : a + 1, :] = xyrec[c, i, p : p + 1, :]
        for side in (0, 1):
            t = [zrec[c, side, i] for i in range(5)]
            for h in range(halves):
                o = jnp.where((lane8 >= 4) & (lane8 < 4 + 2 * bx), roll(t[0], 4 - 2 * bx * h, 1), 0.0)
                o = jnp.where(lane8 // 2 == 1, roll(t[1], 2 - 2 * (bx * h + bx - 1), 1), o)
                o = jnp.where(lane8 // 2 == bx + 2, roll(t[2], 2 * (bx + 2) - 2 * bx * h, 1), o)
                pk[c, side, 8 + 8 * h : 16 + 8 * h, :] = o
            inner = (lane8 >= 4) & (lane8 < 4 + 2 * bx)
            before = jnp.where(inner, roll(t[3], 4 - 2 * bx * (halves - 1), 1), 0.0)
            after = jnp.where(inner, roll(t[4], 4, 1), 0.0)
            pk[c, side, 7:8, :] = before[7:8]
            pk[c, side, 8 + by : 9 + by, :] = after[0:1]

    def around(ref, packed, i, a, b):
        c = ref[i, a:b, :]
        ln = lane_of(c.shape)
        s = ref[i - 1, a:b, :] + ref[i + 1, a:b, :]
        s = s + ref[i, a - 1 : b - 1, :] + ref[i, a + 1 : b + 1, :]
        s = s + jnp.where(ln == 0, packed[0, a:b, 2 * i + 1 : 2 * i + 2], roll(c, 1, 1))
        return s + jnp.where(ln == bz - 1, packed[1, a:b, 2 * i : 2 * i + 1], roll(c, -1, 1))

    wy = (2 * ky + 1) * hy
    ex = kx * hx
    ey = ky * hy

    zi = lane_of((8, bz))
    yi = row_of((8, bz))
    mid = (zi >= q) & (zi < q + hz)
    low, high = (zi >= q - CUT) & (zi <= q), (zi >= q + hz - 1) & (zi < q + hz + CUT)
    if nz == 2:
        sides = [(
            1 - gz, jnp.where(gz == 0, q + hz - 1, q - CUT), (high & (gz == 0)) | (low & (gz == 1)),
            mid & (zi % CHUNK == jnp.where(gz == 0, 1, CUT - 1)),
        )]
    else:
        sides = [(0, q - CUT, low, mid & (zi % CHUNK == CUT - 1)), (1, q + hz - 1, high, mid & (zi % CHUNK == 1))]
        sides = sides if nz > 1 else []
    strips = [slice(8 + 8 * t, 16 + 8 * t) for t in range(wy // 8)]

    def grid_strip(t):
        y = yi + 8 * t
        ok = (y >= ey - gy * hy) & (y < ey + (ny - gy) * hy) & (zi >= q - gz * hz) & (zi < q + (nz - gz) * hz)
        return jnp.where(ok, 1.0, 0.0)

    def there(p, half):
        x = p + (gx * hx - ex) // half
        return jnp.where((x >= 0) & (x < nx * hx // half), 1.0, 0.0)

    def total_of(terms):
        while len(terms) > 1:
            terms = [a + b for a, b in zip(terms[::2], terms[1::2])] + ([terms[-1]] if len(terms) % 2 else [])
        return terms[0]

    def shifted(ref, p, t, step):
        v = ref[p, strips[t], :]
        r0 = strips[t].start
        return total_of([
            ref[p, r0 - step : r0 - step + 8, :], ref[p, r0 + step : r0 + step + 8, :],
            roll(v, step, 1), roll(v, -step, 1),
        ])

    def helpers(c, rows):
        def tile(i, j):
            return win[c, TILES * i + j, rows, :]

        def along(n, i, piece):
            return pltpu.roll(beyond[n, i, rows, :], (sides[n][1] - CHUNK * chunk_of(piece)) % bz, 1)

        def over(parts):
            return [
                jnp.where(side[2], total_of([along(n, i, f) for i, f in parts]), 0.0)
                for n, side in enumerate(sides)
            ]

        return tile, over

    def assemble(c, a0, a1):
        blocks = range(2 * kx + 1)
        for t, strip in enumerate(strips):
            rows = slice(8 * t, 8 * t + 8)

            tile, over = helpers(c, rows)
            for i in blocks:
                skin = tile(i, 4 if i == 0 else 0)
                for n, (s, _, _, spill) in enumerate(sides):
                    beyond[n, i, rows, :] = wside[c, s, i, rows, :] + jnp.where(spill, skin, 0.0)
                wedge[i, strip, :] = total_of([jnp.where(mid, roll(skin, hz, 1), 0.0)] + over([(i, SKIN)]))
        for t, strip in enumerate(strips):
            rows = slice(8 * t, 8 * t + 8)

            tile, over = helpers(c, rows)
            for p in range(a0, a1):
                i, k = p // hx, p % hx
                body, parts = tile(i, (1, 2, 2, 3)[k]), [(i, k)]
                if k == 0 and i > 0:
                    body = body + tile(i - 1, 3)
                    parts.append((i - 1, UP))
                if k == hx - 1 and i < 2 * kx:
                    body = body + tile(i + 1, 1)
                    parts.append((i + 1, DOWN))
                terms = [jnp.where(mid, roll(body, hz * (k % 2), 1), 0.0)] + over(parts)
                up = 8 + 8 * t + k + 1
                down = 8 + 8 * t - hx + k
                terms.append(jnp.where(yi == 7, wedge[i, up : up + 8, :], jnp.where(yi == 0, wedge[i, down : down + 8, :], 0.0)))
                wd[p - a0, strip, :] = total_of(terms)

    def coarse(c):
        a0, a1 = ex - REACH, ex + hx + REACH
        assemble(c, a0, a1)
        n = (a1 - a0) // 2 - 1
        b0 = (a0 + 1) // 2
        on2 = [there(b0 + j, 2) for j in range(n)]
        grid = [grid_strip(t) for t in range(len(strips))]
        every = list(enumerate(strips))
        for t, strip in every:
            for j in range(n):
                pair[j, strip, :] = wd[2 * j + 1, strip, :] + wd[2 * j + 2, strip, :]
        for t, strip in every:
            for j in range(n):
                ends = wd[2 * j, strip, :] + wd[2 * j + 3, strip, :]
                wb[j, strip, :] = (1.0 - 5.0 * W) * pair[j, strip, :] + W * (ends + shifted(pair, j, t, 1))
        for t, strip in every:
            for j in range(n):
                r0 = strip.start
                v = wb[j, strip, :]
                v = v + jnp.where(yi % 2 == 0, wb[j, r0 + 1 : r0 + 9, :], wb[j, r0 - 1 : r0 + 7, :])
                v = v + jnp.where(zi % 2 == 0, roll(v, -1, 1), roll(v, 1, 1))
                wr[j, strip, :] = (0.5 * on2[j]) * (grid[t] * v)
        for t, strip in every:
            for j in range(1, n - 1):
                v = (2.0 * W - 6.0 * W * W) * wr[j, strip, :]
                v = v + (W * W) * (wr[j - 1, strip, :] + wr[j + 1, strip, :] + shifted(wr, j, t, 2))
                we[j, strip, :] = on2[j] * (grid[t] * v)
        k0 = (b0 + 2) * 2 - a0
        for t, strip in every:
            for j in range(2, n - 2):
                v = wr[j, strip, :] + (we[j - 1, strip, :] + we[j + 1, strip, :] + shifted(we, j, t, 2))
                v = on2[j] * (grid[t] * ((1.0 - 6.0 * W) * we[j, strip, :] + W * v))
                for k in (2 * j - 4, 2 * j - 3):
                    wv[k, strip, :] = W * wd[k0 + k, strip, :] + v
        for t, strip in every:
            for k in range(1, 2 * n - 9):
                v = wd[k0 + k, strip, :] + (wv[k - 1, strip, :] + wv[k + 1, strip, :] + shifted(wv, k, t, 1))
                v = there(a0 + k0 + k, 1) * (grid[t] * ((1.0 - 6.0 * W) * wv[k, strip, :] + W * v))
                prol[k - 1, pl.ds(16 * t, 8, stride=2), :] = v
                prol[k - 1, pl.ds(16 * t + 1, 8, stride=2), :] = v

    def dot(x, m):
        out = None
        for part in split(x):
            y = jnp.dot(part, m, preferred_element_type=f32)
            out = y if out is None else out + y
        return out

    def cycle_and_image(c, r):
        send_halo(c, r)
        if c == 0:
            pl.semaphore_wait(barrier, callers)
        start(halo(c), rsem.at[2 * c])
        send_coarse(c, r)
        start(gathered(c), rsem.at[2 * c + 1])
        arrive(halo(c), rsem.at[2 * c], 2)
        place_halo(c)
        rref = fld.at[c]
        arrive(gathered(c), rsem.at[2 * c + 1], 2)
        coarse(c)
        kept = slice(2 * ey - 8, 2 * ey + by + 8)
        for side, a in ((0, q - 1), (1, q + hz)):
            o = W * pk[c, side]
            for j in range(hx + 2):
                o = o + jnp.where(lanef // 4 == j, prol[j, kept, a : a + 1], 0.0)
            vpk[side] = o
        fine = dot(prol[:, kept, :].reshape((hx + 2) * (by + 16), bz), grow[...]).reshape(hx + 2, by + 16, bz)
        for i in range(bx + 4):
            vfld[i] = W * rref[i] + fine[i // 2]
        for i in range(1, bx + 3):
            a, b = 7, 9 + by
            z = (1.0 - 6.0 * W) * vfld[i, a:b, :] + W * (rref[i, a:b, :] + around(vfld, vpk, i, a, b))
            zrow = lax.broadcasted_iota(jnp.int32, z.shape, 0)
            ok = ((zrow > 0) | (gy > 0)) & ((zrow < by + 1) | (gy < ny - 1))
            if i == 1:
                ok = ok & (gx > 0)
            if i == bx + 2:
                ok = ok & (gx < nx - 1)
            zfld[i, a:b, :] = jnp.where(ok, z, 0.0)
        for side, a in ((0, 0), (1, bz - 1)):
            o = vpk[side]
            s = roll(o, 2, 1) + roll(o, -2, 1) + roll(o, 1, 0) + roll(o, -1, 0)
            s = s + roll(o, 1 - 2 * side, 1)
            for i in range(2, bx + 2):
                s = s + jnp.where(lanef == 2 * i + 1 - side, vfld[i, :, a : a + 1], 0.0)
            ok = gz < nz - 1 if side else gz > 0
            zpk[side] = jnp.where(ok, (1.0 - 6.0 * W) * o + W * (pk[c, side] + s), 0.0)
        z = zfld[2 : bx + 2, 8 : 8 + by, :]
        return z, jnp.stack([6.0 * z[i - 2] - around(zfld, zpk, i, 8, 8 + by) for i in range(2, bx + 2)])

    z0, w = cycle_and_image(0, r0)
    u, aw = cycle_and_image(1, w)

    pairs = ((r0, z0), (z0, w), (r0, u), (w, u), (u, aw), (z0, aw))
    l1 = lane_of((1, bz))
    mine = jnp.zeros((1, bz), f32)
    for i, (a, b) in enumerate(pairs):
        s = jnp.sum(jnp.sum(jnp.sum(a * b, axis=0), axis=0, keepdims=True), axis=1, keepdims=True)
        mine = jnp.where(l1 == i, s, mine)
    sums[me] = mine

    def share(to):
        pltpu.make_async_remote_copy(
            sums.at[me], sums.at[me], ssem.at[0], rsem.at[4], device_id=to, device_id_type=MESH
        ).start()

    if total <= 64:
        def ways(g, n):
            return [g, g + 1 - 2 * (g % 2), lax.rem(g + 2, 4), 3 - g] if n == 4 else [lax.rem(g + j, n) for j in range(n)]

        options = [ways(g, n) for g, n in zip((gx, gy, gz), ns)]
        for j in sorted(itertools.product(*(range(n) for n in ns)), key=lambda j: -sum(j)):
            if any(j):
                share(tuple(way[i] for way, i in zip(options, j)))
    else:

        def step(i, carry):
            o = lax.rem(me + i, total)
            share((o // (ny * nz), lax.rem(o // nz, ny), lax.rem(o, nz)))
            return carry

        lax.fori_loop(1, total, step, 0)

    wait_rows(total - 1, rsem.at[4])
    tot = jnp.sum(sums[...], axis=0)

    def scalar(i):
        return jnp.sum(jnp.where(l1 == i, tot, 0.0), axis=1, keepdims=True)

    g0, d0, ru, wu, uv, zv = (scalar(i) for i in range(6))
    a = g0 / d0
    g1 = (g0 - a * d0) - a * ru + a * a * wu
    beta = g1 / g0
    zaz = d0 - a * (wu + zv) + a * a * uv
    cross = (d0 - a * wu) + (d0 - a * zv)
    b = g1 / (zaz + beta * cross + beta * beta * d0)
    for p in range(bx):
        d1 = (z0[p] - a * u[p]) + beta * z0[p]
        i1 = (w[p] - a * aw[p]) + beta * w[p]
        both[0, p] = a * z0[p] + b * d1
        both[1, p] = (r0[p] - a * w[p]) - b * i1
    arrive([item for c in (0, 1) for item in halo(c) + gathered(c)], ssem.at[0], 1, total - 1)


def solution(mesh):
    ns = tuple(mesh.shape[a] for a in ("gx", "gy", "gz"))

    def local(density, x_faces, y_faces, z_faces):
        bx, by, bz = density.shape
        hx, hy = bx // 2, by // 2
        assert hx == 4 and hy == 8 and REACH == 7
        kx, ky = -(-REACH // hx), -(-REACH // hy)
        total = ns[0] * ns[1] * ns[2]
        f32 = jnp.float32
        dma = pltpu.SemaphoreType.DMA

        def vmem(*shape, dtype=f32):
            return pltpu.VMEM(shape, dtype)

        wy = (2 * ky + 1) * hy
        pairs = hx // 2 + REACH - 1
        both = pl.pallas_call(
            functools.partial(kernel, ns, bx, by, bz, kx, ky),
            out_shape=vmem(2, bx, by, bz),
            in_specs=[pl.BlockSpec(memory_space=pl.ANY)] * 4,
            out_specs=pl.BlockSpec(memory_space=pltpu.VMEM),
            scratch_shapes=[
                vmem(2, bx + 4, by + 16, bz),
                vmem(2, 2, 2, bx, bz),
                vmem(2, 2, 2, bx, bz),
                vmem(2, 2, 8, bz),
                vmem(2, 2, 5, 8, bz),
                vmem(2, 4, bx, bz),
                vmem(2, 2, by + 16, bz),
                vmem(hx + 2, by, bz),
                vmem(hx, by + 16, bz),
                vmem(2 * hx, bz),
                vmem(2 * bz, 4 * bz, dtype=jnp.bfloat16),
                vmem(bz, bz, dtype=jnp.bfloat16),
                vmem(2, TILES, hy, bz),
                vmem(2, 2, hy, bz),
                vmem(2, (2 * kx + 1) * TILES, wy, bz),
                vmem(2, 2, 2 * kx + 1, wy, bz),
                vmem(hx + 2, 2 * wy, bz),
                vmem(total, 1, bz),
                vmem(ROWS, 1, bz),
                vmem(2 * kx + 1, wy + 16, bz),
                vmem(2, 2 * kx + 1, wy, bz),
                vmem(hx + 2 * REACH, wy + 16, bz),
                vmem(pairs, wy + 16, bz),
                vmem(pairs, wy + 16, bz),
                vmem(pairs, wy + 16, bz),
                vmem(pairs, wy + 16, bz),
                vmem(2 * (pairs - 4), wy + 16, bz),
                vmem(bx + 4, by + 16, bz),
                vmem(2, by + 16, bz),
                vmem(bx + 4, by + 16, bz),
                vmem(2, by + 16, bz),
                vmem(*density.shape),
                vmem(*x_faces.shape),
                vmem(*y_faces.shape),
                vmem(*z_faces.shape),
                dma((1,)),
                dma((5,)),
                dma((2,)),
            ],
            compiler_params=pltpu.CompilerParams(collective_id=0, has_side_effects=True),
        )(density, x_faces, y_faces, z_faces)
        return both[0], both[1]

    return jax.shard_map(
        local,
        mesh=mesh,
        in_specs=(P("gx", "gy", "gz"), P(None, "gy", "gz"), P(None, "gx", "gz"), P(None, "gx", "gy")),
        out_specs=(P("gx", "gy", "gz"), P("gx", "gy", "gz")),
        check_vma=False,
    )
```

```python
import functools
import itertools

import jax
import jax.numpy as jnp
from jax import lax
from jax.experimental import pallas as pl
from jax.experimental.pallas import tpu as pltpu
from jax.sharding import PartitionSpec as P

W = 1.0 / 9.0
COUPLING = 0.5
MESH = pl.DeviceIdType.MESH
REACH = 7
CUT = 8
CHUNK = 16
DOWN, UP, SKIN, TILES = 4, 5, 6, 5
ROWS = 2048


def lane_of(shape):
    return lax.broadcasted_iota(jnp.int32, shape, len(shape) - 1)


def row_of(shape):
    return lax.broadcasted_iota(jnp.int32, shape, len(shape) - 2)


def roll(x, shift, axis):
    shift = shift % x.shape[axis]
    return pltpu.roll(x, shift, axis) if shift else x


def both_of(a, b):
    return b if a is None else a if b is None else a & b


def partners(g, n, reach):
    out = []
    for m in range(1, min(reach, n - 1) + 1):
        if n == 2:
            out.append((1 - 2 * g, None, None, 0, m))
        elif n == 4 and m == 1:
            inner = (g == 1) | (g == 2)
            out.append((1 - 2 * (g % 2), None, None, 0, m))
            out.append((3 - 2 * g, inner, inner, 1, m))
        elif n == 4 and m == 2:
            out.append((2 - 4 * (g // 2), None, None, 0, m))
        else:
            out.append((m, g + m < n, g - m >= 0, 2 * m - 1, m))
            out.append((-m, g - m >= 0, g + m < n, 2 * m, m))
    return out


def chunk_of(piece):
    return piece + 2 if piece < DOWN else piece - DOWN if piece < SKIN else SKIN


def knows_all(ns, kx, ky):
    return ns[0] - 1 <= 3 * kx and ns[1] - 1 <= 3 * ky and ns[2] - 1 <= 3


def kernel(
    ns, bx, by, bz, kx, ky,
    den_in, xf_in, yf_in, zf_in, both,
    fld, ysrc, yrec, zsrc, zrec, xyrec, pk,
    tu, tx, ty, shrink, grow, dsrc, dside, win, wside, prol, sums, blank,
    wedge, beyond, wd, pair, wb, wr, we, wv, vfld, vpk, zfld, zpk, den, xf, yf, zf,
    ssem, rsem, isem,
):
    nx, ny, nz = ns
    gx, gy, gz = (lax.axis_index(a) for a in ("gx", "gy", "gz"))
    hx, hy, hz = bx // 2, by // 2, bz // 2
    q = bz // 4
    me = (gx * ny + gy) * nz + gz
    total = nx * ny * nz
    f32 = jnp.float32
    bf16 = jnp.bfloat16

    loads = [
        pltpu.make_async_copy(a, b, isem.at[i])
        for i, a, b in ((0, den_in, den), (0, xf_in, xf), (0, yf_in, yf), (1, zf_in, zf))
    ]
    for load in loads:
        load.start()

    here = [(0, None, None, 0, 0)]
    window = []
    for o in itertools.product(here + partners(gx, nx, kx), here + partners(gy, ny, ky), here + partners(gz, nz, 1)):
        d, send, recv, key, far = zip(*o)
        if any(far):
            window.append((d, functools.reduce(both_of, send), functools.reduce(both_of, recv), key, far))
    window.sort(key=lambda item: -sum(f > 0 for f in item[4]))

    def at(d):
        return (gx + d[0], gy + d[1], gz + d[2])

    def only(cond, do):
        if cond is None:
            do()
        else:
            pl.when(cond)(do)

    def clear(c):
        for ref in (fld, yrec, zrec, xyrec, win, wside):
            ref[c] = jnp.zeros(ref.shape[1:], f32)

    clear(0)
    paired = all(n in (1, 2, 4) for n in ns)
    inner = [(g == 1) | (g == 2) for g in (gx, gy, gz)]

    def rows_of(ref):
        n = 1
        for size in ref.shape:
            n *= size
        return n // bz

    def wait_rows(n, sem):
        room = blank.at[pl.ds(0, n)]
        pltpu.make_async_copy(room, room, sem).wait()

    barrier = pltpu.get_barrier_semaphore()
    if knows_all(ns, kx, ky):
        callers = 0
        for d, send, recv, _, _ in window:
            only(send, lambda d=d: pl.semaphore_signal(barrier, inc=1, device_id=at(d), device_id_type=MESH))
            callers = callers + (1 if recv is None else jnp.where(recv, 1, 0))
    else:
        callers = total - 1

        def greet(step, c):
            o = lax.rem(me + step, total)
            to = (o // (ny * nz), lax.rem(o // nz, ny), lax.rem(o, nz))
            pl.semaphore_signal(barrier, inc=1, device_id=to, device_id_type=MESH)
            return c

        lax.fori_loop(1, total, greet, 0)

    clear(1)
    pk[...] = jnp.zeros_like(pk)
    tx[...] = jnp.zeros_like(tx)
    for ref, edge in ((wedge, 8), (wd, 8), (pair, 8), (wb, 8), (wr, 8), (we, 16), (wv, 16)):
        rim = jnp.zeros((ref.shape[0], edge, bz), f32)
        ref[:, 0:edge, :] = rim
        ref[:, ref.shape[1] - edge :, :] = rim

    lj = lane_of((bz, bz))
    li = row_of((bz, bz))
    maps = (
        ((lj - q + hz) % hz, lj >= 0),
        (hz - CUT + lj % CHUNK, lj % CHUNK <= CUT),
        (lj % CHUNK - 1, lj % CHUNK <= CUT),
        (jnp.where(lj % CHUNK == 1, hz, -1), (lj % CHUNK == 1) | (lj % CHUNK == CUT - 1)),
    )
    for i, (col, ok) in enumerate(maps):
        ok = ok & ((col >= 0) | (gz > 0)) & ((col < hz) | (gz < nz - 1))
        cell = (li // 2 == col) & ok
        outer = ((li == 2 * col - 1) | (li == 2 * col + 2)) & ok
        shrink[0:bz, i * bz : (i + 1) * bz] = jnp.where(cell, 0.5, 0.0).astype(bf16)
        shrink[bz : 2 * bz, i * bz : (i + 1) * bz] = jnp.where(outer, 0.5, 0.0).astype(bf16)
    beyond_at = [jnp.where(gz == 0, q + hz, q - 1)] if nz == 2 else [q - 1, q + hz]
    grow[:, 0:bz] = jnp.where(li == q + lj // 2, 1.0, 0.0).astype(bf16)
    for n, col in enumerate(beyond_at):
        grow[:, (n + 1) * bz : (n + 2) * bz] = jnp.where(li == col, 1.0, 0.0).astype(bf16)

    wait_rows(sum(rows_of(a) for a in (den, xf, yf)), isem.at[0])
    loads[-1].wait()

    lane = lane_of((by, bz))
    eye = row_of((by, by)) == lane_of((by, by))
    row = row_of((by, bz))
    planes = []
    for p in range(bx):
        r = -COUPLING * den[p]
        if p == 0:
            r = r + jnp.where(gx == 0, xf[0], 0.0)
        if p == bx - 1:
            r = r + jnp.where(gx == nx - 1, xf[1], 0.0)
        r = r + jnp.where((row == 0) & (gy == 0), yf[0, p : p + 1, :], 0.0)
        r = r + jnp.where((row == by - 1) & (gy == ny - 1), yf[1, p : p + 1, :], 0.0)
        for side, (a, edge) in enumerate(((0, 0), (bz - 1, nz - 1))):
            col = jnp.sum(jnp.where(eye, zf[side, p : p + 1, :], 0.0), axis=1, keepdims=True)
            r = r + jnp.where((lane == a) & (gz == edge), col, 0.0)
        planes.append(r)
    r0 = jnp.stack(planes)

    lane8 = lane_of((8, bz))
    halves = by // 8
    own = pl.ds(8, by)

    def start(items, sem):
        for d, send, _, _, _, src, dst in items:
            only(send, lambda d=d, src=src, dst=dst: pltpu.make_async_remote_copy(
                src, dst, ssem.at[0], sem, device_id=at(d), device_id_type=MESH
            ).start())

    def arrive(items, sem, which, more=0):
        counts = {}
        for item in items:
            counts[item[3]] = (counts.get(item[3], (0,))[0] + rows_of(item[5]), item[which])
        if not paired:
            for n, cond in counts.values():
                only(cond, lambda n=n: wait_rows(n, sem))
            if more:
                wait_rows(more, sem)
            return
        axes = [i for i in range(3) if ns[i] == 4 and any(key[i] for key in counts)]
        for flags in itertools.product((0, 1), repeat=len(axes)):
            state, cond = dict(zip(axes, flags)), None
            for i, flag in state.items():
                cond = both_of(cond, inner[i] if flag else jnp.logical_not(inner[i]))
            n = sum(rows for key, (rows, _) in counts.items() if all(key[i] <= state.get(i, 0) for i in range(3)))
            only(cond, lambda n=n: wait_rows(n + more, sem))

    def halo(c):
        f = fld.at[c]
        out = []
        for d, send, recv, key, far in window:
            if max(far) > 1 or sum(far) > 2:
                continue
            dx, dy, dz = d
            if far == (1, 0, 0):
                src = f.at[pl.ds(2 + (bx - 2) * ((dx + 1) // 2), 2), own]
                dst = f.at[pl.ds((bx + 2) * ((1 - dx) // 2), 2), own]
            elif far == (0, 1, 0):
                src, dst = ysrc.at[c, (dy + 1) // 2], yrec.at[c, (1 - dy) // 2]
            elif far == (1, 1, 0):
                src, dst = ysrc.at[c, (dy + 1) // 2, 0], xyrec.at[c, (1 - dx) + (1 - dy) // 2]
            else:
                slot = 1 + (1 - dx) // 2 if far[0] else 3 + (1 - dy) // 2 if far[1] else 0
                a, b = (0, 0) if nz == 2 else ((dz + 1) // 2, (1 - dz) // 2)
                src, dst = zsrc.at[c, a], zrec.at[c, b, slot]
            out.append((d, send, recv, key, far, src, dst))
        return out

    def gathered(c):
        out = []
        for d, send, recv, key, far in window:
            dx, dy, dz = d
            rows = pl.ds(pl.multiple_of((ky - dy) * hy, 8), hy)
            if far[2]:
                src, dst = dside.at[c, (dz + 1) // 2], wside.at[c, (1 - dz) // 2, kx - dx, rows]
            else:
                a, n = ((dx + 2) // 2, 3) if far[0] == 2 else (0, 4)
                src, dst = dsrc.at[c, pl.ds(a, n)], win.at[c, pl.ds((kx - dx) * TILES + a, n), rows]
            out.append((d, send, recv, key, far, src, dst))
        return out

    def split(x):
        parts = []
        for _ in range(3):
            part = x.astype(bf16)
            x = x - part.astype(f32)
            parts.append(part)
        return parts

    center = (lane8 >= q) & (lane8 < q + hz)

    def send_halo(c, value):
        fld[c, 2 : bx + 2, 8 : 8 + by, :] = value
        for p in range(bx):
            for d in (0, 1):
                ysrc[c, 0, d, p : p + 1, :] = value[p, d : d + 1, :]
                ysrc[c, 1, d, p : p + 1, :] = value[p, by - 1 - d : by - d, :]
        for n, (a, swap) in enumerate([(jnp.where(gz == 0, bz - 2, 0), gz == 1)] if nz == 2 else [(0, True), (bz - 2, False)]):
            out = jnp.zeros((8, bz), f32)
            for h in range(halves):
                for p in range(bx):
                    to = 2 * (h * bx + p)
                    moved = pltpu.roll(value[p, 8 * h : 8 * h + 8, :], (to + bz - a) % bz, 1)
                    out = jnp.where(lane8 // 2 == to // 2, moved, out)
            turned = jnp.where(lane8 % 2 == 0, roll(out, -1, 1), roll(out, 1, 1))
            zsrc[c, n] = jnp.where(swap, turned, out)

    def send_coarse(c, v):
        for i in range(hx):
            pair = v[2 * i] + v[2 * i + 1]
            ends = (v[2 * i - 1] if i else 0.0) + (v[2 * i + 2] if i < hx - 1 else 0.0)
            tu[i] = (1.0 - 3.0 * W) * pair + W * ends
            tx[i, 8 : 8 + by, :] = pair
            ty[i : i + 1, :] = jnp.where(gy > 0, W, 0.0) * pair[0:1]
            ty[hx + i : hx + i + 1, :] = jnp.where(gy < ny - 1, W, 0.0) * pair[by - 1 : by]
        tu[hx] = jnp.where(gx > 0, W, 0.0) * v[0]
        tu[hx + 1] = jnp.where(gx < nx - 1, W, 0.0) * v[bx - 1]

        def rows(ref, a):
            return ref[:, pl.ds(a, hy, stride=2), :]

        g = rows(tu, 0) + rows(tu, 1)
        outer = W * (rows(tx, 7) + rows(tx, 10))
        side = W * (rows(tx, 8) + rows(tx, 9))
        n = hx * hy
        left = jnp.concatenate(
            [(g[:hx] + outer).reshape(n, bz), g[hx:].reshape(2 * hy, bz), ty[...], jnp.zeros((8, bz), f32)]
        )
        right = jnp.concatenate([side.reshape(n, bz), jnp.zeros((2 * hy + 16, bz), f32)])
        m = left.shape[0]
        x = jnp.concatenate([left, right], axis=1)
        y = jnp.dot(jnp.concatenate(split(x)), shrink[...], preferred_element_type=f32)
        y = y[:m] + y[m : 2 * m] + y[2 * m :]

        def piece(i, k):
            return y[8 * i : 8 * i + 8, k * bz : (k + 1) * bz]

        skin = piece(SKIN, 0)
        for i in range(hx):
            skin = jnp.where(lane8 // CHUNK == chunk_of(i), piece(i, 3), skin)
        block = [skin] + [
            jnp.where(center, piece(a, 0), piece(b, 0)) for a, b in ((0, DOWN), (2, 1), (UP, 3))
        ]
        for i, tile in enumerate(block + [skin]):
            dsrc[c, i] = tile
            win[c, kx * TILES + i, ky * hy : (ky + 1) * hy, :] = tile
        for s, k in ((1, 1), (0, 2)):
            out = jnp.zeros((8, bz), f32)
            for i in range(hx + 3):
                out = jnp.where(lane8 // CHUNK == chunk_of(i), piece(i, k), out)
            dside[c, s] = out

    def place_halo(c):
        for p in range(bx):
            for d in (0, 1):
                fld[c, p + 2, 7 - d : 8 - d, :] = yrec[c, 0, d, p : p + 1, :]
                fld[c, p + 2, 8 + by + d : 9 + by + d, :] = yrec[c, 1, d, p : p + 1, :]
        for i in range(4):
            plane, p = ((1, bx - 1), (bx + 2, 0))[i // 2]
            a = (7, 8 + by)[i % 2]
            fld[c, plane, a : a + 1, :] = xyrec[c, i, p : p + 1, :]
        for side in range(len(beyond_at)):
            t = [zrec[c, side, i] for i in range(5)]
            for h in range(halves):
                o = jnp.where((lane8 >= 4) & (lane8 < 4 + 2 * bx), roll(t[0], 4 - 2 * bx * h, 1), 0.0)
                o = jnp.where(lane8 // 2 == 1, roll(t[1], 2 - 2 * (bx * h + bx - 1), 1), o)
                o = jnp.where(lane8 // 2 == bx + 2, roll(t[2], 2 * (bx + 2) - 2 * bx * h, 1), o)
                pk[c, side, 8 + 8 * h : 16 + 8 * h, :] = o
            inner = (lane8 >= 4) & (lane8 < 4 + 2 * bx)
            before = jnp.where(inner, roll(t[3], 4 - 2 * bx * (halves - 1), 1), 0.0)
            after = jnp.where(inner, roll(t[4], 4, 1), 0.0)
            pk[c, side, 7:8, :] = before[7:8]
            pk[c, side, 8 + by : 9 + by, :] = after[0:1]

    def around(ref, packed, i, a, b):
        c = ref[i, a:b, :]
        ln = lane_of(c.shape)
        s = ref[i - 1, a:b, :] + ref[i + 1, a:b, :]
        s = s + ref[i, a - 1 : b - 1, :] + ref[i, a + 1 : b + 1, :]
        near = slice(2 * i + 1, 2 * i + 2)
        if nz == 2:
            s = s + jnp.where(ln == 0, 0.0, roll(c, 1, 1)) + jnp.where(ln == bz - 1, 0.0, roll(c, -1, 1))
            return s + jnp.where(ln == (1 - gz) * (bz - 1), packed[0, a:b, near], 0.0)
        s = s + jnp.where(ln == 0, packed[0, a:b, near], roll(c, 1, 1))
        return s + jnp.where(ln == bz - 1, packed[1, a:b, near], roll(c, -1, 1))

    wy = (2 * ky + 1) * hy
    ex = kx * hx
    ey = ky * hy

    zi = lane_of((8, bz))
    yi = row_of((8, bz))
    mid = (zi >= q) & (zi < q + hz)
    low, high = (zi >= q - CUT) & (zi <= q), (zi >= q + hz - 1) & (zi < q + hz + CUT)
    if nz == 2:
        sides = [(
            1 - gz, jnp.where(gz == 0, q + hz - 1, q - CUT), (high & (gz == 0)) | (low & (gz == 1)),
            mid & (zi % CHUNK == jnp.where(gz == 0, 1, CUT - 1)),
        )]
    else:
        sides = [(0, q - CUT, low, mid & (zi % CHUNK == CUT - 1)), (1, q + hz - 1, high, mid & (zi % CHUNK == 1))]
        sides = sides if nz > 1 else []
    strips = [slice(8 + 8 * t, 16 + 8 * t) for t in range(wy // 8)]

    late = [slice(8 + ey - 4 + r, 16 + ey - 4 + r) for r in range(0, hy + 8, 8)]

    def grid_strip(strip):
        y = yi + strip.start - 8
        ok = (y >= ey - gy * hy) & (y < ey + (ny - gy) * hy) & (zi >= q - gz * hz) & (zi < q + (nz - gz) * hz)
        return jnp.where(ok, 1.0, 0.0)

    def there(p, half):
        x = p + (gx * hx - ex) // half
        return jnp.where((x >= 0) & (x < nx * hx // half), 1.0, 0.0)

    def total_of(terms):
        while len(terms) > 1:
            terms = [a + b for a, b in zip(terms[::2], terms[1::2])] + ([terms[-1]] if len(terms) % 2 else [])
        return terms[0]

    def shifted(ref, p, strip, step):
        v = ref[p, strip, :]
        r0 = strip.start
        return total_of([
            ref[p, r0 - step : r0 - step + 8, :], ref[p, r0 + step : r0 + step + 8, :],
            roll(v, step, 1), roll(v, -step, 1),
        ])

    def helpers(c, rows):
        def tile(i, j):
            return win[c, TILES * i + j, rows, :]

        def along(n, i, piece):
            return pltpu.roll(beyond[n, i, rows, :], (sides[n][1] - CHUNK * chunk_of(piece)) % bz, 1)

        def over(parts):
            return [
                jnp.where(side[2], total_of([along(n, i, f) for i, f in parts]), 0.0)
                for n, side in enumerate(sides)
            ]

        return tile, over

    def assemble(c, a0, a1):
        blocks = range(2 * kx + 1)
        for t, strip in enumerate(strips):
            rows = slice(8 * t, 8 * t + 8)

            tile, over = helpers(c, rows)
            for i in blocks:
                skin = tile(i, 4 if i == 0 else 0)
                for n, (s, _, _, spill) in enumerate(sides):
                    beyond[n, i, rows, :] = wside[c, s, i, rows, :] + jnp.where(spill, skin, 0.0)
                wedge[i, strip, :] = total_of([jnp.where(mid, roll(skin, hz, 1), 0.0)] + over([(i, SKIN)]))
        for t, strip in enumerate(strips):
            rows = slice(8 * t, 8 * t + 8)

            tile, over = helpers(c, rows)
            for p in range(a0, a1):
                i, k = p // hx, p % hx
                body, parts = tile(i, (1, 2, 2, 3)[k]), [(i, k)]
                if k == 0 and i > 0:
                    body = body + tile(i - 1, 3)
                    parts.append((i - 1, UP))
                if k == hx - 1 and i < 2 * kx:
                    body = body + tile(i + 1, 1)
                    parts.append((i + 1, DOWN))
                terms = [jnp.where(mid, roll(body, hz * (k % 2), 1), 0.0)] + over(parts)
                up = 8 + 8 * t + k + 1
                down = 8 + 8 * t - hx + k
                terms.append(jnp.where(yi == 7, wedge[i, up : up + 8, :], jnp.where(yi == 0, wedge[i, down : down + 8, :], 0.0)))
                wd[p - a0, strip, :] = total_of(terms)

    def coarse(c):
        a0, a1 = ex - REACH, ex + hx + REACH
        assemble(c, a0, a1)
        n = (a1 - a0) // 2 - 1
        b0 = (a0 + 1) // 2
        on2 = [there(b0 + j, 2) for j in range(n)]
        for strip in strips:
            for j in range(n):
                pair[j, strip, :] = wd[2 * j + 1, strip, :] + wd[2 * j + 2, strip, :]
        for strip in strips:
            for j in range(n):
                ends = wd[2 * j, strip, :] + wd[2 * j + 3, strip, :]
                wb[j, strip, :] = (1.0 - 5.0 * W) * pair[j, strip, :] + W * (ends + shifted(pair, j, strip, 1))
        for strip in strips:
            grid = grid_strip(strip)
            for j in range(n):
                r0 = strip.start
                v = wb[j, strip, :]
                v = v + jnp.where(yi % 2 == 0, wb[j, r0 + 1 : r0 + 9, :], wb[j, r0 - 1 : r0 + 7, :])
                v = v + jnp.where(zi % 2 == 0, roll(v, -1, 1), roll(v, 1, 1))
                wr[j, strip, :] = (0.5 * on2[j]) * (grid * v)
        grids = [grid_strip(strip) for strip in late]
        for strip, grid in zip(late, grids):
            for j in range(1, n - 1):
                v = (2.0 * W - 6.0 * W * W) * wr[j, strip, :]
                v = v + (W * W) * (wr[j - 1, strip, :] + wr[j + 1, strip, :] + shifted(wr, j, strip, 2))
                we[j, strip, :] = on2[j] * (grid * v)
        k0 = (b0 + 2) * 2 - a0
        for strip, grid in zip(late, grids):
            for j in range(2, n - 2):
                v = wr[j, strip, :] + (we[j - 1, strip, :] + we[j + 1, strip, :] + shifted(we, j, strip, 2))
                v = on2[j] * (grid * ((1.0 - 6.0 * W) * we[j, strip, :] + W * v))
                for k in (2 * j - 4, 2 * j - 3):
                    wv[k, strip, :] = W * wd[k0 + k, strip, :] + v
        for strip, grid in zip(late, grids):
            for k in range(1, 2 * n - 9):
                v = wd[k0 + k, strip, :] + (wv[k - 1, strip, :] + wv[k + 1, strip, :] + shifted(wv, k, strip, 1))
                v = there(a0 + k0 + k, 1) * (grid * ((1.0 - 6.0 * W) * wv[k, strip, :] + W * v))
                to = 2 * (strip.start - late[0].start)
                prol[k - 1, pl.ds(to, 8, stride=2), :] = v
                prol[k - 1, pl.ds(to + 1, 8, stride=2), :] = v

    def dot(x, m):
        out = None
        for part in split(x):
            y = jnp.dot(part, m, preferred_element_type=f32)
            out = y if out is None else out + y
        return out

    def cycle_and_image(c, r):
        send_halo(c, r)
        if c == 0:
            send_coarse(c, r)
            pl.semaphore_wait(barrier, callers)
            start(halo(c), rsem.at[2 * c])
        else:
            start(halo(c), rsem.at[2 * c])
            send_coarse(c, r)
        start(gathered(c), rsem.at[2 * c + 1])
        arrive(halo(c), rsem.at[2 * c], 2)
        place_halo(c)
        rref = fld.at[c]
        arrive(gathered(c), rsem.at[2 * c + 1], 2)
        coarse(c)
        seen = slice(6, 14 + by)
        tall = 8 + by
        fine = dot(prol[:, seen, :].reshape((hx + 2) * tall, bz), grow[...])
        fine = fine.reshape(hx + 2, tall, (1 + len(beyond_at)) * bz)
        for n in range(len(beyond_at)):
            o = W * pk[c, n, seen, :]
            for j in range(hx + 2):
                o = o + jnp.where(lane_of((tall, bz)) // 4 == j, fine[j, :, (n + 1) * bz : (n + 2) * bz], 0.0)
            vpk[n, seen, :] = o
        for i in range(bx + 4):
            vfld[i, seen, :] = W * rref[i, seen, :] + fine[i // 2, :, 0:bz]
        for i in range(1, bx + 3):
            a, b = (8, 8 + by) if i in (1, bx + 2) else (7, 9 + by)
            z = (1.0 - 6.0 * W) * vfld[i, a:b, :] + W * (rref[i, a:b, :] + around(vfld, vpk, i, a, b))
            zrow = lax.broadcasted_iota(jnp.int32, z.shape, 0)
            if i == 1:
                ok = gx > 0
            elif i == bx + 2:
                ok = gx < nx - 1
            else:
                ok = ((zrow > 0) | (gy > 0)) & ((zrow < by + 1) | (gy < ny - 1))
            zfld[i, a:b, :] = jnp.where(ok, z, 0.0)
        rows = slice(8, 8 + by)
        lane2 = lane_of((by, bz))
        for n in range(len(beyond_at)):
            o = vpk[n, rows, :]
            s = roll(o, 2, 1) + roll(o, -2, 1) + roll(o, 1, 1) + vpk[n, 7 : 7 + by, :] + vpk[n, 9 : 9 + by, :]
            for i in range(2, bx + 2):
                v = vfld[i, rows, :]
                v = jnp.where(gz == 1, v, roll(v, 1, 1)) if nz == 2 else v if n == 0 else roll(v, 1, 1)
                s = s + jnp.where(lane2 == 2 * i + 1, v[:, 0:1], 0.0)
            z = (1.0 - 6.0 * W) * o + W * (pk[c, n, rows, :] + s)
            zpk[n, rows, :] = z if nz == 2 else jnp.where(gz > 0 if n == 0 else gz < nz - 1, z, 0.0)
        z = zfld[2 : bx + 2, 8 : 8 + by, :]
        return z, jnp.stack([6.0 * z[i - 2] - around(zfld, zpk, i, 8, 8 + by) for i in range(2, bx + 2)])

    z0, w = cycle_and_image(0, r0)
    u, aw = cycle_and_image(1, w)

    pairs = ((r0, z0), (z0, w), (r0, u), (w, u), (u, aw), (z0, aw))
    l1 = lane_of((1, bz))
    mine = jnp.zeros((1, bz), f32)
    for i, (a, b) in enumerate(pairs):
        s = jnp.sum(jnp.sum(jnp.sum(a * b, axis=0), axis=0, keepdims=True), axis=1, keepdims=True)
        mine = jnp.where(l1 == i, s, mine)
    sums[me] = mine

    def share(to):
        pltpu.make_async_remote_copy(
            sums.at[me], sums.at[me], ssem.at[0], rsem.at[4], device_id=to, device_id_type=MESH
        ).start()

    if total <= 64:
        def ways(g, n):
            return [g, g + 1 - 2 * (g % 2), lax.rem(g + 2, 4), 3 - g] if n == 4 else [lax.rem(g + j, n) for j in range(n)]

        options = [ways(g, n) for g, n in zip((gx, gy, gz), ns)]
        for j in sorted(itertools.product(*(range(n) for n in ns)), key=lambda j: -sum(j)):
            if any(j):
                share(tuple(way[i] for way, i in zip(options, j)))
    else:

        def step(i, carry):
            o = lax.rem(me + i, total)
            share((o // (ny * nz), lax.rem(o // nz, ny), lax.rem(o, nz)))
            return carry

        lax.fori_loop(1, total, step, 0)

    wait_rows(total - 1, rsem.at[4])
    tot = jnp.sum(sums[...], axis=0)

    def scalar(i):
        return jnp.sum(jnp.where(l1 == i, tot, 0.0), axis=1, keepdims=True)

    g0, d0, ru, wu, uv, zv = (scalar(i) for i in range(6))
    a = g0 / d0
    g1 = (g0 - a * d0) - a * ru + a * a * wu
    beta = g1 / g0
    zaz = d0 - a * (wu + zv) + a * a * uv
    cross = (d0 - a * wu) + (d0 - a * zv)
    b = g1 / (zaz + beta * cross + beta * beta * d0)
    along_z, along_u = a + b * (1.0 + beta), a * b
    for p in range(bx):
        both[0, p] = along_z * z0[p] - along_u * u[p]
        both[1, p] = r0[p] - along_z * w[p] + along_u * aw[p]
    arrive([item for c in (0, 1) for item in halo(c) + gathered(c)], ssem.at[0], 1, total - 1)


def solution(mesh):
    ns = tuple(mesh.shape[a] for a in ("gx", "gy", "gz"))

    def local(density, x_faces, y_faces, z_faces):
        bx, by, bz = density.shape
        hx, hy = bx // 2, by // 2
        assert hx == 4 and hy == 8 and REACH == 7
        kx, ky = -(-REACH // hx), -(-REACH // hy)
        total = ns[0] * ns[1] * ns[2]
        f32 = jnp.float32
        dma = pltpu.SemaphoreType.DMA

        def vmem(*shape, dtype=f32):
            return pltpu.VMEM(shape, dtype)

        wy = (2 * ky + 1) * hy
        pairs = hx // 2 + REACH - 1
        both = pl.pallas_call(
            functools.partial(kernel, ns, bx, by, bz, kx, ky),
            out_shape=vmem(2, bx, by, bz),
            in_specs=[pl.BlockSpec(memory_space=pl.ANY)] * 4,
            out_specs=pl.BlockSpec(memory_space=pltpu.VMEM),
            scratch_shapes=[
                vmem(2, bx + 4, by + 16, bz),
                vmem(2, 2, 2, bx, bz),
                vmem(2, 2, 2, bx, bz),
                vmem(2, 2, 8, bz),
                vmem(2, 2, 5, 8, bz),
                vmem(2, 4, bx, bz),
                vmem(2, 2, by + 16, bz),
                vmem(hx + 2, by, bz),
                vmem(hx, by + 16, bz),
                vmem(2 * hx, bz),
                vmem(2 * bz, 4 * bz, dtype=jnp.bfloat16),
                vmem(bz, (2 if ns[2] == 2 else 3) * bz, dtype=jnp.bfloat16),
                vmem(2, TILES, hy, bz),
                vmem(2, 2, hy, bz),
                vmem(2, (2 * kx + 1) * TILES, wy, bz),
                vmem(2, 2, 2 * kx + 1, wy, bz),
                vmem(hx + 2, by + 16, bz),
                vmem(total, 1, bz),
                vmem(ROWS, 1, bz),
                vmem(2 * kx + 1, wy + 16, bz),
                vmem(2, 2 * kx + 1, wy, bz),
                vmem(hx + 2 * REACH, wy + 16, bz),
                vmem(pairs, wy + 16, bz),
                vmem(pairs, wy + 16, bz),
                vmem(pairs, wy + 16, bz),
                vmem(pairs, wy + 16, bz),
                vmem(2 * (pairs - 4), wy + 16, bz),
                vmem(bx + 4, by + 16, bz),
                vmem(2, by + 16, bz),
                vmem(bx + 4, by + 16, bz),
                vmem(2, by + 16, bz),
                vmem(*density.shape),
                vmem(*x_faces.shape),
                vmem(*y_faces.shape),
                vmem(*z_faces.shape),
                dma((1,)),
                dma((5,)),
                dma((2,)),
            ],
            compiler_params=pltpu.CompilerParams(collective_id=0, has_side_effects=True),
        )(density, x_faces, y_faces, z_faces)
        return both[0], both[1]

    return jax.shard_map(
        local,
        mesh=mesh,
        in_specs=(P("gx", "gy", "gz"), P(None, "gy", "gz"), P(None, "gx", "gz"), P(None, "gx", "gy")),
        out_specs=(P("gx", "gy", "gz"), P("gx", "gy", "gz")),
        check_vma=False,
    )
```

```python
import functools
import itertools

import jax
import jax.numpy as jnp
from jax import lax
from jax.experimental import pallas as pl
from jax.experimental.pallas import tpu as pltpu
from jax.sharding import PartitionSpec as P

W = 1.0 / 9.0
COUPLING = 0.5
MESH = pl.DeviceIdType.MESH
REACH = 7
CUT = 8
CHUNK = 16
DOWN, UP, SKIN, TILES = 4, 5, 6, 6
ROWS = 2048


def lane_of(shape):
    return lax.broadcasted_iota(jnp.int32, shape, len(shape) - 1)


def row_of(shape):
    return lax.broadcasted_iota(jnp.int32, shape, len(shape) - 2)


def roll(x, shift, axis):
    shift = shift % x.shape[axis]
    return pltpu.roll(x, shift, axis) if shift else x


def both_of(a, b):
    return b if a is None else a if b is None else a & b


def partners(g, n, reach):
    out = []
    for m in range(1, min(reach, n - 1) + 1):
        if n == 2:
            out.append((1 - 2 * g, None, None, 0, m))
        elif n == 4 and m == 1:
            inner = (g == 1) | (g == 2)
            out.append((1 - 2 * (g % 2), None, None, 0, m))
            out.append((3 - 2 * g, inner, inner, 1, m))
        elif n == 4 and m == 2:
            out.append((2 - 4 * (g // 2), None, None, 0, m))
        else:
            out.append((m, g + m < n, g - m >= 0, 2 * m - 1, m))
            out.append((-m, g - m >= 0, g + m < n, 2 * m, m))
    return out


def chunk_of(piece):
    return piece + 2 if piece < DOWN else piece - DOWN if piece < SKIN else SKIN


def knows_all(ns, kx, ky):
    return ns[0] - 1 <= 3 * kx and ns[1] - 1 <= 3 * ky and ns[2] - 1 <= 3


def kernel(
    ns, bx, by, bz, kx, ky,
    den_in, xf_in, yf_in, zf_in, both,
    fld, ysrc, yrec, pk,
    tu, tx, ty, shrink, grow, dsrc, dside, win, wside, prol, sums, blank,
    wedge, beyond, wd, pair, wb, wr, we, wv, vfld, vpk, zfld, zpk, den, xf, yf, zf,
    ssem, rsem, isem,
):
    nx, ny, nz = ns
    gx, gy, gz = (lax.axis_index(a) for a in ("gx", "gy", "gz"))
    hx, hy, hz = bx // 2, by // 2, bz // 2
    q = bz // 4
    me = (gx * ny + gy) * nz + gz
    total = nx * ny * nz
    f32 = jnp.float32
    bf16 = jnp.bfloat16

    loads = [
        pltpu.make_async_copy(a, b, isem.at[i])
        for i, a, b in ((0, den_in, den), (0, xf_in, xf), (0, yf_in, yf), (1, zf_in, zf))
    ]
    for load in loads:
        load.start()

    here = [(0, None, None, 0, 0)]
    window = []
    for o in itertools.product(here + partners(gx, nx, kx), here + partners(gy, ny, ky), here + partners(gz, nz, 1)):
        d, send, recv, key, far = zip(*o)
        if any(far):
            window.append((d, functools.reduce(both_of, send), functools.reduce(both_of, recv), key, far))
    window.sort(key=lambda item: (-sum(f > 0 for f in item[4]), item[3][0] + item[3][1]))

    def at(d):
        return (gx + d[0], gy + d[1], gz + d[2])

    def only(cond, do):
        if cond is None:
            do()
        else:
            pl.when(cond)(do)

    def clear(c):
        for ref in (fld, yrec, win, wside):
            ref[c] = jnp.zeros(ref.shape[1:], f32)

    clear(0)
    paired = all(n in (1, 2, 4) for n in ns)
    inner = [(g == 1) | (g == 2) for g in (gx, gy, gz)]

    def rows_of(ref):
        n = 1
        for size in ref.shape:
            n *= size
        return n // bz

    def wait_rows(n, sem):
        room = blank.at[pl.ds(0, n)]
        pltpu.make_async_copy(room, room, sem).wait()

    barrier = pltpu.get_barrier_semaphore()
    if knows_all(ns, kx, ky):
        callers = 0
        for d, send, recv, _, _ in window:
            only(send, lambda d=d: pl.semaphore_signal(barrier, inc=1, device_id=at(d), device_id_type=MESH))
            callers = callers + (1 if recv is None else jnp.where(recv, 1, 0))
    else:
        callers = total - 1

        def greet(step, c):
            o = lax.rem(me + step, total)
            to = (o // (ny * nz), lax.rem(o // nz, ny), lax.rem(o, nz))
            pl.semaphore_signal(barrier, inc=1, device_id=to, device_id_type=MESH)
            return c

        lax.fori_loop(1, total, greet, 0)

    clear(1)
    pk[...] = jnp.zeros_like(pk)
    tx[...] = jnp.zeros_like(tx)
    for ref, edge in ((wedge, 8), (wd, 8), (pair, 8), (wb, 8), (wr, 8), (we, 16), (wv, 16)):
        rim = jnp.zeros((ref.shape[0], edge, bz), f32)
        ref[:, 0:edge, :] = rim
        ref[:, ref.shape[1] - edge :, :] = rim

    lj = lane_of((bz, bz))
    li = row_of((bz, bz))
    maps = (
        ((lj - q + hz) % hz, lj >= 0),
        (hz - CUT + lj % CHUNK, lj % CHUNK <= CUT),
        (lj % CHUNK - 1, lj % CHUNK <= CUT),
        (jnp.where(lj % CHUNK == 1, hz, -1), (lj % CHUNK == 1) | (lj % CHUNK == CUT - 1)),
    )
    for i, (col, ok) in enumerate(maps):
        ok = ok & ((col >= 0) | (gz > 0)) & ((col < hz) | (gz < nz - 1))
        cell = (li // 2 == col) & ok
        outer = ((li == 2 * col - 1) | (li == 2 * col + 2)) & ok
        shrink[0:bz, i * bz : (i + 1) * bz] = jnp.where(cell, 0.5, 0.0).astype(bf16)
        shrink[bz : 2 * bz, i * bz : (i + 1) * bz] = jnp.where(outer, 0.5, 0.0).astype(bf16)
    beyond_at = [jnp.where(gz == 0, q + hz, q - 1)] if nz == 2 else [q - 1, q + hz]
    grow[:, 0:bz] = jnp.where(li == q + lj // 2, 1.0, 0.0).astype(bf16)
    for n, col in enumerate(beyond_at):
        grow[:, (n + 1) * bz : (n + 2) * bz] = jnp.where(li == col, 1.0, 0.0).astype(bf16)

    wait_rows(sum(rows_of(a) for a in (den, xf, yf)), isem.at[0])
    loads[-1].wait()

    lane = lane_of((by, bz))
    eye = row_of((by, by)) == lane_of((by, by))
    row = row_of((by, bz))
    planes = []
    for p in range(bx):
        r = -COUPLING * den[p]
        if p == 0:
            r = r + jnp.where(gx == 0, xf[0], 0.0)
        if p == bx - 1:
            r = r + jnp.where(gx == nx - 1, xf[1], 0.0)
        r = r + jnp.where((row == 0) & (gy == 0), yf[0, p : p + 1, :], 0.0)
        r = r + jnp.where((row == by - 1) & (gy == ny - 1), yf[1, p : p + 1, :], 0.0)
        for side, (a, edge) in enumerate(((0, 0), (bz - 1, nz - 1))):
            col = jnp.sum(jnp.where(eye, zf[side, p : p + 1, :], 0.0), axis=1, keepdims=True)
            r = r + jnp.where((lane == a) & (gz == edge), col, 0.0)
        planes.append(r)
    r0 = jnp.stack(planes)

    lane8 = lane_of((8, bz))
    halves = by // 8
    own = pl.ds(8, by)

    def start(items, sem):
        for d, send, _, _, _, src, dst in items:
            only(send, lambda d=d, src=src, dst=dst: pltpu.make_async_remote_copy(
                src, dst, ssem.at[0], sem, device_id=at(d), device_id_type=MESH
            ).start())

    def arrive(items, sem, which, more=0):
        counts = {}
        for item in items:
            counts[item[3]] = (counts.get(item[3], (0,))[0] + rows_of(item[5]), item[which])
        if not paired:
            for n, cond in counts.values():
                only(cond, lambda n=n: wait_rows(n, sem))
            if more:
                wait_rows(more, sem)
            return
        axes = [i for i in range(3) if ns[i] == 4 and any(key[i] for key in counts)]
        for flags in itertools.product((0, 1), repeat=len(axes)):
            state, cond = dict(zip(axes, flags)), None
            for i, flag in state.items():
                cond = both_of(cond, inner[i] if flag else jnp.logical_not(inner[i]))
            n = sum(rows for key, (rows, _) in counts.items() if all(key[i] <= state.get(i, 0) for i in range(3)))
            only(cond, lambda n=n: wait_rows(n + more, sem))

    def halo(c):
        f = fld.at[c]
        out = []
        for d, send, recv, key, far in window:
            dx, dy, dz = d
            if far == (1, 0, 0):
                src = f.at[pl.ds(2 + (bx - 2) * ((dx + 1) // 2), 2), own]
                dst = f.at[pl.ds((bx + 2) * ((1 - dx) // 2), 2), own]
            elif far == (0, 1, 0):
                src, dst = ysrc.at[c, (dy + 1) // 2], yrec.at[c, (1 - dy) // 2]
            else:
                continue
            out.append((d, send, recv, key, far, src, dst))
        return out

    def gathered(c):
        out = []
        for d, send, recv, key, far in window:
            dx, dy, dz = d
            rows = pl.ds(pl.multiple_of((ky - dy) * hy, 8), hy)
            if far[2]:
                n = 2 if far[0] + far[1] < 2 else 1
                src = dside.at[c, (dz + 1) // 2, pl.ds(0, n)]
                dst = wside.at[c, (1 - dz) // 2, kx - dx, ky - dy, pl.ds(0, n)]
            else:
                a, n = (1 + (dx + 2) // 2, 3) if far[0] == 2 else (0, 5) if far == (1, 1, 0) else (1, 4)
                src, dst = dsrc.at[c, pl.ds(a, n)], win.at[c, pl.ds((kx - dx) * TILES + a, n), rows]
            out.append((d, send, recv, key, far, src, dst))
        return out

    def split(x):
        parts = []
        for _ in range(3):
            part = x.astype(bf16)
            x = x - part.astype(f32)
            parts.append(part)
        return parts

    center = (lane8 >= q) & (lane8 < q + hz)

    corners = ((bx - 1, by - 1), (bx - 1, 0), (0, by - 1), (0, 0))

    def send_halo(c, value):
        fld[c, 2 : bx + 2, 8 : 8 + by, :] = value
        for p in range(bx):
            for d in (0, 1):
                ysrc[c, 0, d, p : p + 1, :] = value[p, d : d + 1, :]
                ysrc[c, 1, d, p : p + 1, :] = value[p, by - 1 - d : by - d, :]
        for n, (a, swap) in enumerate([(jnp.where(gz == 0, bz - 2, 0), gz == 1)] if nz == 2 else [(0, True), (bz - 2, False)]):
            out = jnp.zeros((8, bz), f32)
            for h in range(halves):
                for p in range(bx):
                    to = 2 * (h * bx + p)
                    moved = pltpu.roll(value[p, 8 * h : 8 * h + 8, :], (to + bz - a) % bz, 1)
                    out = jnp.where(lane8 // 2 == to // 2, moved, out)
            turned = jnp.where(lane8 % 2 == 0, roll(out, -1, 1), roll(out, 1, 1))
            out = jnp.where(swap, turned, out)
            for side in (0, 1) if nz == 2 else (n,):
                dside[c, side, 1] = out
        for i, (p, r) in enumerate(corners):
            dsrc[c, 0, i : i + 1, :] = value[p, r : r + 1, :]
        dsrc[c, 0, 4:8, :] = jnp.zeros((4, bz), f32)

    def send_coarse(c, v):
        for i in range(hx):
            pair = v[2 * i] + v[2 * i + 1]
            ends = (v[2 * i - 1] if i else 0.0) + (v[2 * i + 2] if i < hx - 1 else 0.0)
            tu[i] = (1.0 - 3.0 * W) * pair + W * ends
            tx[i, 8 : 8 + by, :] = pair
            ty[i : i + 1, :] = jnp.where(gy > 0, W, 0.0) * pair[0:1]
            ty[hx + i : hx + i + 1, :] = jnp.where(gy < ny - 1, W, 0.0) * pair[by - 1 : by]
        tu[hx] = jnp.where(gx > 0, W, 0.0) * v[0]
        tu[hx + 1] = jnp.where(gx < nx - 1, W, 0.0) * v[bx - 1]

        def rows(ref, a):
            return ref[:, pl.ds(a, hy, stride=2), :]

        g = rows(tu, 0) + rows(tu, 1)
        outer = W * (rows(tx, 7) + rows(tx, 10))
        side = W * (rows(tx, 8) + rows(tx, 9))
        n = hx * hy
        left = jnp.concatenate(
            [(g[:hx] + outer).reshape(n, bz), g[hx:].reshape(2 * hy, bz), ty[...], jnp.zeros((8, bz), f32)]
        )
        right = jnp.concatenate([side.reshape(n, bz), jnp.zeros((2 * hy + 16, bz), f32)])
        m = left.shape[0]
        x = jnp.concatenate([left, right], axis=1)
        y = jnp.dot(jnp.concatenate(split(x)), shrink[...], preferred_element_type=f32)
        y = y[:m] + y[m : 2 * m] + y[2 * m :]

        def piece(i, k):
            return y[8 * i : 8 * i + 8, k * bz : (k + 1) * bz]

        skin = piece(SKIN, 0)
        for i in range(hx):
            skin = jnp.where(lane8 // CHUNK == chunk_of(i), piece(i, 3), skin)
        block = [skin] + [
            jnp.where(center, piece(a, 0), piece(b, 0)) for a, b in ((0, DOWN), (2, 1), (UP, 3))
        ]
        for i, tile in enumerate(block + [skin]):
            dsrc[c, i + 1] = tile
            win[c, kx * TILES + i + 1, ky * hy : (ky + 1) * hy, :] = tile
        for s, k in ((1, 1), (0, 2)):
            out = jnp.zeros((8, bz), f32)
            for i in range(hx + 3):
                out = jnp.where(lane8 // CHUNK == chunk_of(i), piece(i, k), out)
            dside[c, s, 0] = out

    def place_halo(c):
        for p in range(bx):
            for d in (0, 1):
                fld[c, p + 2, 7 - d : 8 - d, :] = yrec[c, 0, d, p : p + 1, :]
                fld[c, p + 2, 8 + by + d : 9 + by + d, :] = yrec[c, 1, d, p : p + 1, :]

    def place_edges(c):
        for i in range(4):
            plane, a = (1, bx + 2)[i // 2], (7, 8 + by)[i % 2]
            x, y = kx + 2 * (i // 2) - 1, ky + 2 * (i % 2) - 1
            fld[c, plane, a : a + 1, :] = win[c, x * TILES, y * hy + i : y * hy + i + 1, :]
        for side in range(len(beyond_at)):
            s = 1 - gz if nz == 2 else side
            t = [wside[c, s, kx + x, ky + y, 1] for x, y in ((0, 0), (-1, 0), (1, 0), (0, -1), (0, 1))]
            for h in range(halves):
                o = jnp.where((lane8 >= 4) & (lane8 < 4 + 2 * bx), roll(t[0], 4 - 2 * bx * h, 1), 0.0)
                o = jnp.where(lane8 // 2 == 1, roll(t[1], 2 - 2 * (bx * h + bx - 1), 1), o)
                o = jnp.where(lane8 // 2 == bx + 2, roll(t[2], 2 * (bx + 2) - 2 * bx * h, 1), o)
                pk[c, side, 8 + 8 * h : 16 + 8 * h, :] = o
            inner = (lane8 >= 4) & (lane8 < 4 + 2 * bx)
            before = jnp.where(inner, roll(t[3], 4 - 2 * bx * (halves - 1), 1), 0.0)
            after = jnp.where(inner, roll(t[4], 4, 1), 0.0)
            pk[c, side, 7:8, :] = before[7:8]
            pk[c, side, 8 + by : 9 + by, :] = after[0:1]

    def around(ref, packed, i, a, b):
        c = ref[i, a:b, :]
        ln = lane_of(c.shape)
        s = ref[i - 1, a:b, :] + ref[i + 1, a:b, :]
        s = s + ref[i, a - 1 : b - 1, :] + ref[i, a + 1 : b + 1, :]
        near = slice(2 * i + 1, 2 * i + 2)
        if nz == 2:
            s = s + jnp.where(ln == 0, 0.0, roll(c, 1, 1)) + jnp.where(ln == bz - 1, 0.0, roll(c, -1, 1))
            return s + jnp.where(ln == (1 - gz) * (bz - 1), packed[0, a:b, near], 0.0)
        s = s + jnp.where(ln == 0, packed[0, a:b, near], roll(c, 1, 1))
        return s + jnp.where(ln == bz - 1, packed[1, a:b, near], roll(c, -1, 1))

    wy = (2 * ky + 1) * hy
    ex = kx * hx
    ey = ky * hy

    zi = lane_of((8, bz))
    yi = row_of((8, bz))
    mid = (zi >= q) & (zi < q + hz)
    low, high = (zi >= q - CUT) & (zi <= q), (zi >= q + hz - 1) & (zi < q + hz + CUT)
    if nz == 2:
        sides = [(
            1 - gz, jnp.where(gz == 0, q + hz - 1, q - CUT), (high & (gz == 0)) | (low & (gz == 1)),
            mid & (zi % CHUNK == jnp.where(gz == 0, 1, CUT - 1)),
        )]
    else:
        sides = [(0, q - CUT, low, mid & (zi % CHUNK == CUT - 1)), (1, q + hz - 1, high, mid & (zi % CHUNK == 1))]
        sides = sides if nz > 1 else []
    strips = [slice(8 + 8 * t, 16 + 8 * t) for t in range(wy // 8)]

    late = [slice(8 + ey - 4 + r, 16 + ey - 4 + r) for r in range(0, hy + 8, 8)]

    def grid_strip(strip):
        y = yi + strip.start - 8
        ok = (y >= ey - gy * hy) & (y < ey + (ny - gy) * hy) & (zi >= q - gz * hz) & (zi < q + (nz - gz) * hz)
        return jnp.where(ok, 1.0, 0.0)

    def there(p, half):
        x = p + (gx * hx - ex) // half
        return jnp.where((x >= 0) & (x < nx * hx // half), 1.0, 0.0)

    def total_of(terms):
        while len(terms) > 1:
            terms = [a + b for a, b in zip(terms[::2], terms[1::2])] + ([terms[-1]] if len(terms) % 2 else [])
        return terms[0]

    def shifted(ref, p, strip, step):
        v = ref[p, strip, :]
        r0 = strip.start
        return total_of([
            ref[p, r0 - step : r0 - step + 8, :], ref[p, r0 + step : r0 + step + 8, :],
            roll(v, step, 1), roll(v, -step, 1),
        ])

    def helpers(c, rows):
        def tile(i, j):
            return win[c, TILES * i + j, rows, :]

        def along(n, i, piece):
            return pltpu.roll(beyond[n, i, rows, :], (sides[n][1] - CHUNK * chunk_of(piece)) % bz, 1)

        def over(parts):
            return [
                jnp.where(side[2], total_of([along(n, i, f) for i, f in parts]), 0.0)
                for n, side in enumerate(sides)
            ]

        return tile, over

    def assemble(c, a0, a1):
        blocks = range(2 * kx + 1)
        for t, strip in enumerate(strips):
            rows = slice(8 * t, 8 * t + 8)

            tile, over = helpers(c, rows)
            for i in blocks:
                skin = tile(i, 5 if i == 0 else 1)
                for n, (s, _, _, spill) in enumerate(sides):
                    beyond[n, i, rows, :] = wside[c, s, i, t, 0] + jnp.where(spill, skin, 0.0)
                wedge[i, strip, :] = total_of([jnp.where(mid, roll(skin, hz, 1), 0.0)] + over([(i, SKIN)]))
        for t, strip in enumerate(strips):
            rows = slice(8 * t, 8 * t + 8)

            tile, over = helpers(c, rows)
            for p in range(a0, a1):
                i, k = p // hx, p % hx
                body, parts = tile(i, (2, 3, 3, 4)[k]), [(i, k)]
                if k == 0 and i > 0:
                    body = body + tile(i - 1, 4)
                    parts.append((i - 1, UP))
                if k == hx - 1 and i < 2 * kx:
                    body = body + tile(i + 1, 2)
                    parts.append((i + 1, DOWN))
                terms = [jnp.where(mid, roll(body, hz * (k % 2), 1), 0.0)] + over(parts)
                up = 8 + 8 * t + k + 1
                down = 8 + 8 * t - hx + k
                terms.append(jnp.where(yi == 7, wedge[i, up : up + 8, :], jnp.where(yi == 0, wedge[i, down : down + 8, :], 0.0)))
                wd[p - a0, strip, :] = total_of(terms)

    def coarse(c):
        a0, a1 = ex - REACH, ex + hx + REACH
        assemble(c, a0, a1)
        n = (a1 - a0) // 2 - 1
        b0 = (a0 + 1) // 2
        on2 = [there(b0 + j, 2) for j in range(n)]
        for strip in strips:
            for j in range(n):
                pair[j, strip, :] = wd[2 * j + 1, strip, :] + wd[2 * j + 2, strip, :]
        for strip in strips:
            for j in range(n):
                ends = wd[2 * j, strip, :] + wd[2 * j + 3, strip, :]
                wb[j, strip, :] = (1.0 - 5.0 * W) * pair[j, strip, :] + W * (ends + shifted(pair, j, strip, 1))
        for strip in strips:
            grid = grid_strip(strip)
            for j in range(n):
                r0 = strip.start
                v = wb[j, strip, :]
                v = v + jnp.where(yi % 2 == 0, wb[j, r0 + 1 : r0 + 9, :], wb[j, r0 - 1 : r0 + 7, :])
                v = v + jnp.where(zi % 2 == 0, roll(v, -1, 1), roll(v, 1, 1))
                wr[j, strip, :] = (0.5 * on2[j]) * (grid * v)
        grids = [grid_strip(strip) for strip in late]
        for strip, grid in zip(late, grids):
            for j in range(1, n - 1):
                v = (2.0 * W - 6.0 * W * W) * wr[j, strip, :]
                v = v + (W * W) * (wr[j - 1, strip, :] + wr[j + 1, strip, :] + shifted(wr, j, strip, 2))
                we[j, strip, :] = on2[j] * (grid * v)
        k0 = (b0 + 2) * 2 - a0
        for strip, grid in zip(late, grids):
            for j in range(2, n - 2):
                v = wr[j, strip, :] + (we[j - 1, strip, :] + we[j + 1, strip, :] + shifted(we, j, strip, 2))
                v = on2[j] * (grid * ((1.0 - 6.0 * W) * we[j, strip, :] + W * v))
                for k in (2 * j - 4, 2 * j - 3):
                    wv[k, strip, :] = W * wd[k0 + k, strip, :] + v
        for strip, grid in zip(late, grids):
            for k in range(1, 2 * n - 9):
                v = wd[k0 + k, strip, :] + (wv[k - 1, strip, :] + wv[k + 1, strip, :] + shifted(wv, k, strip, 1))
                v = there(a0 + k0 + k, 1) * (grid * ((1.0 - 6.0 * W) * wv[k, strip, :] + W * v))
                to = 2 * (strip.start - late[0].start)
                prol[k - 1, pl.ds(to, 8, stride=2), :] = v
                prol[k - 1, pl.ds(to + 1, 8, stride=2), :] = v

    def dot(x, m):
        out = None
        for part in split(x):
            y = jnp.dot(part, m, preferred_element_type=f32)
            out = y if out is None else out + y
        return out

    def cycle_and_image(c, r):
        send_halo(c, r)
        if c == 0:
            send_coarse(c, r)
            pl.semaphore_wait(barrier, callers)
        else:
            send_coarse(c, r)
        items = gathered(c)
        start([m for m in items if all(m[4])], rsem.at[2 * c + 1])
        start(halo(c), rsem.at[2 * c])
        start([m for m in items if not all(m[4])], rsem.at[2 * c + 1])
        arrive(halo(c), rsem.at[2 * c], 2)
        place_halo(c)
        rref = fld.at[c]
        arrive(gathered(c), rsem.at[2 * c + 1], 2)
        place_edges(c)
        coarse(c)
        seen = slice(6, 14 + by)
        tall = 8 + by
        fine = dot(prol[:, seen, :].reshape((hx + 2) * tall, bz), grow[...])
        fine = fine.reshape(hx + 2, tall, (1 + len(beyond_at)) * bz)
        for n in range(len(beyond_at)):
            o = W * pk[c, n, seen, :]
            for j in range(hx + 2):
                o = o + jnp.where(lane_of((tall, bz)) // 4 == j, fine[j, :, (n + 1) * bz : (n + 2) * bz], 0.0)
            vpk[n, seen, :] = o
        for i in range(bx + 4):
            vfld[i, seen, :] = W * rref[i, seen, :] + fine[i // 2, :, 0:bz]
        for i in range(1, bx + 3):
            a, b = (8, 8 + by) if i in (1, bx + 2) else (7, 9 + by)
            z = (1.0 - 6.0 * W) * vfld[i, a:b, :] + W * (rref[i, a:b, :] + around(vfld, vpk, i, a, b))
            zrow = lax.broadcasted_iota(jnp.int32, z.shape, 0)
            if i == 1:
                ok = gx > 0
            elif i == bx + 2:
                ok = gx < nx - 1
            else:
                ok = ((zrow > 0) | (gy > 0)) & ((zrow < by + 1) | (gy < ny - 1))
            zfld[i, a:b, :] = jnp.where(ok, z, 0.0)
        rows = slice(8, 8 + by)
        lane2 = lane_of((by, bz))
        for n in range(len(beyond_at)):
            o = vpk[n, rows, :]
            s = roll(o, 2, 1) + roll(o, -2, 1) + roll(o, 1, 1) + vpk[n, 7 : 7 + by, :] + vpk[n, 9 : 9 + by, :]
            for i in range(2, bx + 2):
                v = vfld[i, rows, :]
                v = jnp.where(gz == 1, v, roll(v, 1, 1)) if nz == 2 else v if n == 0 else roll(v, 1, 1)
                s = s + jnp.where(lane2 == 2 * i + 1, v[:, 0:1], 0.0)
            z = (1.0 - 6.0 * W) * o + W * (pk[c, n, rows, :] + s)
            zpk[n, rows, :] = z if nz == 2 else jnp.where(gz > 0 if n == 0 else gz < nz - 1, z, 0.0)
        z = zfld[2 : bx + 2, 8 : 8 + by, :]
        return z, jnp.stack([6.0 * z[i - 2] - around(zfld, zpk, i, 8, 8 + by) for i in range(2, bx + 2)])

    z0, w = cycle_and_image(0, r0)
    u, aw = cycle_and_image(1, w)

    pairs = ((r0, z0), (z0, w), (r0, u), (w, u), (u, aw), (z0, aw))
    l1 = lane_of((1, bz))
    mine = jnp.zeros((1, bz), f32)
    for i, (a, b) in enumerate(pairs):
        s = jnp.sum(jnp.sum(jnp.sum(a * b, axis=0), axis=0, keepdims=True), axis=1, keepdims=True)
        mine = jnp.where(l1 == i, s, mine)
    sums[me] = mine

    def share(to):
        pltpu.make_async_remote_copy(
            sums.at[me], sums.at[me], ssem.at[0], rsem.at[4], device_id=to, device_id_type=MESH
        ).start()

    if total <= 64:
        def ways(g, n):
            return [g, g + 1 - 2 * (g % 2), lax.rem(g + 2, 4), 3 - g] if n == 4 else [lax.rem(g + j, n) for j in range(n)]

        options = [ways(g, n) for g, n in zip((gx, gy, gz), ns)]
        for j in sorted(itertools.product(*(range(n) for n in ns)), key=lambda j: -sum(j)):
            if any(j):
                share(tuple(way[i] for way, i in zip(options, j)))
    else:

        def step(i, carry):
            o = lax.rem(me + i, total)
            share((o // (ny * nz), lax.rem(o // nz, ny), lax.rem(o, nz)))
            return carry

        lax.fori_loop(1, total, step, 0)

    wait_rows(total - 1, rsem.at[4])
    tot = jnp.sum(sums[...], axis=0)

    def scalar(i):
        return jnp.sum(jnp.where(l1 == i, tot, 0.0), axis=1, keepdims=True)

    g0, d0, ru, wu, uv, zv = (scalar(i) for i in range(6))
    a = g0 / d0
    g1 = (g0 - a * d0) - a * ru + a * a * wu
    beta = g1 / g0
    zaz = d0 - a * (wu + zv) + a * a * uv
    cross = (d0 - a * wu) + (d0 - a * zv)
    b = g1 / (zaz + beta * cross + beta * beta * d0)
    along_z, along_u = a + b * (1.0 + beta), a * b
    for p in range(bx):
        both[0, p] = along_z * z0[p] - along_u * u[p]
        both[1, p] = r0[p] - along_z * w[p] + along_u * aw[p]
    arrive([item for c in (0, 1) for item in halo(c) + gathered(c)], ssem.at[0], 1, total - 1)


def solution(mesh):
    ns = tuple(mesh.shape[a] for a in ("gx", "gy", "gz"))

    def local(density, x_faces, y_faces, z_faces):
        bx, by, bz = density.shape
        hx, hy = bx // 2, by // 2
        assert hx == 4 and hy == 8 and REACH == 7
        kx, ky = -(-REACH // hx), -(-REACH // hy)
        total = ns[0] * ns[1] * ns[2]
        f32 = jnp.float32
        dma = pltpu.SemaphoreType.DMA

        def vmem(*shape, dtype=f32):
            return pltpu.VMEM(shape, dtype)

        wy = (2 * ky + 1) * hy
        pairs = hx // 2 + REACH - 1
        both = pl.pallas_call(
            functools.partial(kernel, ns, bx, by, bz, kx, ky),
            out_shape=vmem(2, bx, by, bz),
            in_specs=[pl.BlockSpec(memory_space=pl.ANY)] * 4,
            out_specs=pl.BlockSpec(memory_space=pltpu.VMEM),
            scratch_shapes=[
                vmem(2, bx + 4, by + 16, bz),
                vmem(2, 2, 2, bx, bz),
                vmem(2, 2, 2, bx, bz),
                vmem(2, 2, by + 16, bz),
                vmem(hx + 2, by, bz),
                vmem(hx, by + 16, bz),
                vmem(2 * hx, bz),
                vmem(2 * bz, 4 * bz, dtype=jnp.bfloat16),
                vmem(bz, (2 if ns[2] == 2 else 3) * bz, dtype=jnp.bfloat16),
                vmem(2, TILES, hy, bz),
                vmem(2, 2, 2, hy, bz),
                vmem(2, (2 * kx + 1) * TILES, wy, bz),
                vmem(2, 2, 2 * kx + 1, 2 * ky + 1, 2, hy, bz),
                vmem(hx + 2, by + 16, bz),
                vmem(total, 1, bz),
                vmem(ROWS, 1, bz),
                vmem(2 * kx + 1, wy + 16, bz),
                vmem(2, 2 * kx + 1, wy, bz),
                vmem(hx + 2 * REACH, wy + 16, bz),
                vmem(pairs, wy + 16, bz),
                vmem(pairs, wy + 16, bz),
                vmem(pairs, wy + 16, bz),
                vmem(pairs, wy + 16, bz),
                vmem(2 * (pairs - 4), wy + 16, bz),
                vmem(bx + 4, by + 16, bz),
                vmem(2, by + 16, bz),
                vmem(bx + 4, by + 16, bz),
                vmem(2, by + 16, bz),
                vmem(*density.shape),
                vmem(*x_faces.shape),
                vmem(*y_faces.shape),
                vmem(*z_faces.shape),
                dma((1,)),
                dma((5,)),
                dma((2,)),
            ],
            compiler_params=pltpu.CompilerParams(collective_id=0, has_side_effects=True),
        )(density, x_faces, y_faces, z_faces)
        return both[0], both[1]

    return jax.shard_map(
        local,
        mesh=mesh,
        in_specs=(P("gx", "gy", "gz"), P(None, "gy", "gz"), P(None, "gx", "gz"), P(None, "gx", "gy")),
        out_specs=(P("gx", "gy", "gz"), P("gx", "gy", "gz")),
        check_vma=False,
    )
```

```python
import functools
import itertools

import jax
import jax.numpy as jnp
from jax import lax
from jax.experimental import pallas as pl
from jax.experimental.pallas import tpu as pltpu
from jax.sharding import PartitionSpec as P

W = 1.0 / 9.0
COUPLING = 0.5
MESH = pl.DeviceIdType.MESH
REACH = 7
CUT = 8
CHUNK = 16
DOWN, UP, SKIN, TILES = 4, 5, 6, 6
ROWS = 2048


def lane_of(shape):
    return lax.broadcasted_iota(jnp.int32, shape, len(shape) - 1)


def row_of(shape):
    return lax.broadcasted_iota(jnp.int32, shape, len(shape) - 2)


def roll(x, shift, axis):
    shift = shift % x.shape[axis]
    return pltpu.roll(x, shift, axis) if shift else x


def both_of(a, b):
    return b if a is None else a if b is None else a & b


def partners(g, n, reach):
    out = []
    for m in range(1, min(reach, n - 1) + 1):
        if n == 2:
            out.append((1 - 2 * g, None, None, 0, m))
        elif n == 4 and m == 1:
            inner = (g == 1) | (g == 2)
            out.append((1 - 2 * (g % 2), None, None, 0, m))
            out.append((3 - 2 * g, inner, inner, 1, m))
        elif n == 4 and m == 2:
            out.append((2 - 4 * (g // 2), None, None, 0, m))
        else:
            out.append((m, g + m < n, g - m >= 0, 2 * m - 1, m))
            out.append((-m, g - m >= 0, g + m < n, 2 * m, m))
    return out


def chunk_of(piece):
    return piece + 2 if piece < DOWN else piece - DOWN if piece < SKIN else SKIN


def knows_all(ns, kx, ky):
    return ns[0] - 1 <= 3 * kx and ns[1] - 1 <= 3 * ky and ns[2] - 1 <= 3


def kernel(
    ns, bx, by, bz, kx, ky,
    den_in, xf_in, yf_in, zf_in, both,
    fld, ysrc, yrec, pk,
    tu, tx, ty, shrink, grow, dsrc, dside, win, wside, prol, sums, blank,
    wedge, beyond, wd, pair, wb, wr, we, wv, vfld, vpk, zfld, zpk, den, xf, yf, zf,
    ssem, rsem, isem,
):
    nx, ny, nz = ns
    gx, gy, gz = (lax.axis_index(a) for a in ("gx", "gy", "gz"))
    hx, hy, hz = bx // 2, by // 2, bz // 2
    q = bz // 4
    me = (gx * ny + gy) * nz + gz
    total = nx * ny * nz
    f32 = jnp.float32
    bf16 = jnp.bfloat16

    loads = [
        pltpu.make_async_copy(a, b, isem.at[i])
        for i, a, b in ((0, den_in, den), (0, xf_in, xf), (0, yf_in, yf), (1, zf_in, zf))
    ]
    for load in loads:
        load.start()

    here = [(0, None, None, 0, 0)]
    window = []
    for o in itertools.product(here + partners(gx, nx, kx), here + partners(gy, ny, ky), here + partners(gz, nz, 1)):
        d, send, recv, key, far = zip(*o)
        if any(far):
            window.append((d, functools.reduce(both_of, send), functools.reduce(both_of, recv), key, far))
    window.sort(key=lambda item: (-sum(f > 0 for f in item[4]), item[3][0] + item[3][1]))

    def at(d):
        return (gx + d[0], gy + d[1], gz + d[2])

    def only(cond, do):
        if cond is None:
            do()
        else:
            pl.when(cond)(do)

    def clear(c):
        for ref in (fld, yrec, win, wside):
            ref[c] = jnp.zeros(ref.shape[1:], f32)

    clear(0)
    paired = all(n in (1, 2, 4) for n in ns)
    inner = [(g == 1) | (g == 2) for g in (gx, gy, gz)]

    def rows_of(ref):
        n = 1
        for size in ref.shape:
            n *= size
        return n // bz

    def wait_rows(n, sem):
        room = blank.at[pl.ds(0, n)]
        pltpu.make_async_copy(room, room, sem).wait()

    barrier = pltpu.get_barrier_semaphore()
    if knows_all(ns, kx, ky):
        callers = 0
        for d, send, recv, _, _ in window:
            only(send, lambda d=d: pl.semaphore_signal(barrier, inc=1, device_id=at(d), device_id_type=MESH))
            callers = callers + (1 if recv is None else jnp.where(recv, 1, 0))
    else:
        callers = total - 1

        def greet(step, c):
            o = lax.rem(me + step, total)
            to = (o // (ny * nz), lax.rem(o // nz, ny), lax.rem(o, nz))
            pl.semaphore_signal(barrier, inc=1, device_id=to, device_id_type=MESH)
            return c

        lax.fori_loop(1, total, greet, 0)

    clear(1)
    pk[...] = jnp.zeros_like(pk)
    tx[...] = jnp.zeros_like(tx)
    for ref, edge in ((wedge, 8), (wd, 8), (pair, 8), (wb, 8), (wr, 8), (we, 16), (wv, 16)):
        rim = jnp.zeros((ref.shape[0], edge, bz), f32)
        ref[:, 0:edge, :] = rim
        ref[:, ref.shape[1] - edge :, :] = rim

    lj = lane_of((bz, bz))
    li = row_of((bz, bz))
    maps = (
        ((lj - q + hz) % hz, lj >= 0),
        (hz - CUT + lj % CHUNK, lj % CHUNK <= CUT),
        (lj % CHUNK - 1, lj % CHUNK <= CUT),
        (jnp.where(lj % CHUNK == 1, hz, -1), (lj % CHUNK == 1) | (lj % CHUNK == CUT - 1)),
    )
    for i, (col, ok) in enumerate(maps):
        ok = ok & ((col >= 0) | (gz > 0)) & ((col < hz) | (gz < nz - 1))
        cell = (li // 2 == col) & ok
        outer = ((li == 2 * col - 1) | (li == 2 * col + 2)) & ok
        shrink[0:bz, i * bz : (i + 1) * bz] = jnp.where(cell, 0.5, 0.0).astype(bf16)
        shrink[bz : 2 * bz, i * bz : (i + 1) * bz] = jnp.where(outer, 0.5, 0.0).astype(bf16)
    beyond_at = [jnp.where(gz == 0, q + hz, q - 1)] if nz == 2 else [q - 1, q + hz]
    grow[:, 0:bz] = jnp.where(li == q + lj // 2, 1.0, 0.0).astype(bf16)
    for n, col in enumerate(beyond_at):
        grow[:, (n + 1) * bz : (n + 2) * bz] = jnp.where(li == col, 1.0, 0.0).astype(bf16)

    wait_rows(sum(rows_of(a) for a in (den, xf, yf)), isem.at[0])
    loads[-1].wait()

    lane = lane_of((by, bz))
    eye = row_of((by, by)) == lane_of((by, by))
    row = row_of((by, bz))
    planes = []
    for p in range(bx):
        r = -COUPLING * den[p]
        if p == 0:
            r = r + jnp.where(gx == 0, xf[0], 0.0)
        if p == bx - 1:
            r = r + jnp.where(gx == nx - 1, xf[1], 0.0)
        r = r + jnp.where((row == 0) & (gy == 0), yf[0, p : p + 1, :], 0.0)
        r = r + jnp.where((row == by - 1) & (gy == ny - 1), yf[1, p : p + 1, :], 0.0)
        for side, (a, edge) in enumerate(((0, 0), (bz - 1, nz - 1))):
            col = jnp.sum(jnp.where(eye, zf[side, p : p + 1, :], 0.0), axis=1, keepdims=True)
            r = r + jnp.where((lane == a) & (gz == edge), col, 0.0)
        planes.append(r)
    r0 = jnp.stack(planes)

    lane8 = lane_of((8, bz))
    halves = by // 8
    own = pl.ds(8, by)

    def start(items, sem):
        for d, send, _, _, _, src, dst in items:
            only(send, lambda d=d, src=src, dst=dst: pltpu.make_async_remote_copy(
                src, dst, ssem.at[0], sem, device_id=at(d), device_id_type=MESH
            ).start())

    def arrive(items, sem, which, more=0):
        counts = {}
        for item in items:
            counts[item[3]] = (counts.get(item[3], (0,))[0] + rows_of(item[5]), item[which])
        if not paired:
            for n, cond in counts.values():
                only(cond, lambda n=n: wait_rows(n, sem))
            if more:
                wait_rows(more, sem)
            return
        axes = [i for i in range(3) if ns[i] == 4 and any(key[i] for key in counts)]
        for flags in itertools.product((0, 1), repeat=len(axes)):
            state, cond = dict(zip(axes, flags)), None
            for i, flag in state.items():
                cond = both_of(cond, inner[i] if flag else jnp.logical_not(inner[i]))
            n = sum(rows for key, (rows, _) in counts.items() if all(key[i] <= state.get(i, 0) for i in range(3)))
            only(cond, lambda n=n: wait_rows(n + more, sem))

    def halo(c):
        f = fld.at[c]
        out = []
        for d, send, recv, key, far in window:
            dx, dy, dz = d
            if far == (1, 0, 0):
                src = f.at[pl.ds(2 + (bx - 2) * ((dx + 1) // 2), 2), own]
                dst = f.at[pl.ds((bx + 2) * ((1 - dx) // 2), 2), own]
            elif far == (0, 1, 0):
                src, dst = ysrc.at[c, (dy + 1) // 2], yrec.at[c, (1 - dy) // 2]
            else:
                continue
            out.append((d, send, recv, key, far, src, dst))
        return out

    def gathered(c):
        out = []
        for d, send, recv, key, far in window:
            dx, dy, dz = d
            rows = pl.ds(pl.multiple_of((ky - dy) * hy, 8), hy)
            if far[2]:
                n = 2 if far[0] + far[1] < 2 else 1
                src = dside.at[c, (dz + 1) // 2, pl.ds(0, n)]
                dst = wside.at[c, (1 - dz) // 2, kx - dx, ky - dy, pl.ds(0, n)]
            else:
                a, n = (1 + (dx + 2) // 2, 3) if far[0] == 2 else (0, 5) if far == (1, 1, 0) else (1, 4)
                src, dst = dsrc.at[c, pl.ds(a, n)], win.at[c, pl.ds((kx - dx) * TILES + a, n), rows]
            out.append((d, send, recv, key, far, src, dst))
        return out

    def split(x):
        parts = []
        for _ in range(3):
            part = x.astype(bf16)
            x = x - part.astype(f32)
            parts.append(part)
        return parts

    center = (lane8 >= q) & (lane8 < q + hz)

    corners = ((bx - 1, by - 1), (bx - 1, 0), (0, by - 1), (0, 0))

    def send_halo(c, value):
        fld[c, 2 : bx + 2, 8 : 8 + by, :] = value
        for p in range(bx):
            for d in (0, 1):
                ysrc[c, 0, d, p : p + 1, :] = value[p, d : d + 1, :]
                ysrc[c, 1, d, p : p + 1, :] = value[p, by - 1 - d : by - d, :]
        for n, (a, swap) in enumerate([(jnp.where(gz == 0, bz - 2, 0), gz == 1)] if nz == 2 else [(0, True), (bz - 2, False)]):
            out = jnp.zeros((8, bz), f32)
            for h in range(halves):
                for p in range(bx):
                    to = 2 * (h * bx + p)
                    moved = pltpu.roll(value[p, 8 * h : 8 * h + 8, :], (to + bz - a) % bz, 1)
                    out = jnp.where(lane8 // 2 == to // 2, moved, out)
            turned = jnp.where(lane8 % 2 == 0, roll(out, -1, 1), roll(out, 1, 1))
            out = jnp.where(swap, turned, out)
            for side in (0, 1) if nz == 2 else (n,):
                dside[c, side, 1] = out
        for i, (p, r) in enumerate(corners):
            dsrc[c, 0, i : i + 1, :] = value[p, r : r + 1, :]
        dsrc[c, 0, 4:8, :] = jnp.zeros((4, bz), f32)

    def send_coarse(c, v):
        for i in range(hx):
            pair = v[2 * i] + v[2 * i + 1]
            ends = (v[2 * i - 1] if i else 0.0) + (v[2 * i + 2] if i < hx - 1 else 0.0)
            tu[i] = (1.0 - 3.0 * W) * pair + W * ends
            tx[i, 8 : 8 + by, :] = pair
            ty[i : i + 1, :] = jnp.where(gy > 0, W, 0.0) * pair[0:1]
            ty[hx + i : hx + i + 1, :] = jnp.where(gy < ny - 1, W, 0.0) * pair[by - 1 : by]
        tu[hx] = jnp.where(gx > 0, W, 0.0) * v[0]
        tu[hx + 1] = jnp.where(gx < nx - 1, W, 0.0) * v[bx - 1]

        def rows(ref, a):
            return ref[:, pl.ds(a, hy, stride=2), :]

        g = rows(tu, 0) + rows(tu, 1)
        outer = W * (rows(tx, 7) + rows(tx, 10))
        side = W * (rows(tx, 8) + rows(tx, 9))
        n = hx * hy
        left = jnp.concatenate(
            [(g[:hx] + outer).reshape(n, bz), g[hx:].reshape(2 * hy, bz), ty[...], jnp.zeros((8, bz), f32)]
        )
        right = jnp.concatenate([side.reshape(n, bz), jnp.zeros((2 * hy + 16, bz), f32)])
        m = left.shape[0]
        x = jnp.concatenate([left, right], axis=1)
        y = jnp.dot(jnp.concatenate(split(x)), shrink[...], preferred_element_type=f32)
        y = y[:m] + y[m : 2 * m] + y[2 * m :]

        def piece(i, k):
            return y[8 * i : 8 * i + 8, k * bz : (k + 1) * bz]

        skin = piece(SKIN, 0)
        for i in range(hx):
            skin = jnp.where(lane8 // CHUNK == chunk_of(i), piece(i, 3), skin)
        block = [skin] + [
            jnp.where(center, piece(a, 0), piece(b, 0)) for a, b in ((0, DOWN), (2, 1), (UP, 3))
        ]
        for i, tile in enumerate(block + [skin]):
            dsrc[c, i + 1] = tile
            win[c, kx * TILES + i + 1, ky * hy : (ky + 1) * hy, :] = tile
        for s, k in ((1, 1), (0, 2)):
            out = jnp.zeros((8, bz), f32)
            for i in range(hx + 3):
                out = jnp.where(lane8 // CHUNK == chunk_of(i), piece(i, k), out)
            dside[c, s, 0] = out

    def place_halo(c):
        for p in range(bx):
            for d in (0, 1):
                fld[c, p + 2, 7 - d : 8 - d, :] = yrec[c, 0, d, p : p + 1, :]
                fld[c, p + 2, 8 + by + d : 9 + by + d, :] = yrec[c, 1, d, p : p + 1, :]

    def place_edges(c):
        for i in range(4):
            plane, a = (1, bx + 2)[i // 2], (7, 8 + by)[i % 2]
            x, y = kx + 2 * (i // 2) - 1, ky + 2 * (i % 2) - 1
            fld[c, plane, a : a + 1, :] = win[c, x * TILES, y * hy + i : y * hy + i + 1, :]
        for side in range(len(beyond_at)):
            s = 1 - gz if nz == 2 else side
            t = [wside[c, s, kx + x, ky + y, 1] for x, y in ((0, 0), (-1, 0), (1, 0), (0, -1), (0, 1))]
            for h in range(halves):
                o = jnp.where((lane8 >= 4) & (lane8 < 4 + 2 * bx), roll(t[0], 4 - 2 * bx * h, 1), 0.0)
                o = jnp.where(lane8 // 2 == 1, roll(t[1], 2 - 2 * (bx * h + bx - 1), 1), o)
                o = jnp.where(lane8 // 2 == bx + 2, roll(t[2], 2 * (bx + 2) - 2 * bx * h, 1), o)
                pk[c, side, 8 + 8 * h : 16 + 8 * h, :] = o
            inner = (lane8 >= 4) & (lane8 < 4 + 2 * bx)
            before = jnp.where(inner, roll(t[3], 4 - 2 * bx * (halves - 1), 1), 0.0)
            after = jnp.where(inner, roll(t[4], 4, 1), 0.0)
            pk[c, side, 7:8, :] = before[7:8]
            pk[c, side, 8 + by : 9 + by, :] = after[0:1]

    def around(ref, packed, i, a, b):
        c = ref[i, a:b, :]
        ln = lane_of(c.shape)
        s = ref[i - 1, a:b, :] + ref[i + 1, a:b, :]
        s = s + ref[i, a - 1 : b - 1, :] + ref[i, a + 1 : b + 1, :]
        near = slice(2 * i + 1, 2 * i + 2)
        if nz == 2:
            s = s + jnp.where(ln == 0, 0.0, roll(c, 1, 1)) + jnp.where(ln == bz - 1, 0.0, roll(c, -1, 1))
            return s + jnp.where(ln == (1 - gz) * (bz - 1), packed[0, a:b, near], 0.0)
        s = s + jnp.where(ln == 0, packed[0, a:b, near], roll(c, 1, 1))
        return s + jnp.where(ln == bz - 1, packed[1, a:b, near], roll(c, -1, 1))

    wy = (2 * ky + 1) * hy
    ex = kx * hx
    ey = ky * hy

    zi = lane_of((8, bz))
    yi = row_of((8, bz))
    mid = (zi >= q) & (zi < q + hz)
    low, high = (zi >= q - CUT) & (zi <= q), (zi >= q + hz - 1) & (zi < q + hz + CUT)
    if nz == 2:
        sides = [(
            1 - gz, jnp.where(gz == 0, q + hz - 1, q - CUT), (high & (gz == 0)) | (low & (gz == 1)),
            mid & (zi % CHUNK == jnp.where(gz == 0, 1, CUT - 1)),
        )]
    else:
        sides = [(0, q - CUT, low, mid & (zi % CHUNK == CUT - 1)), (1, q + hz - 1, high, mid & (zi % CHUNK == 1))]
        sides = sides if nz > 1 else []
    strips = [slice(8 + 8 * t, 16 + 8 * t) for t in range(wy // 8)]

    late = [slice(8 + ey - 4 + r, 16 + ey - 4 + r) for r in range(0, hy + 8, 8)]

    def grid_strip(strip):
        y = yi + strip.start - 8
        ok = (y >= ey - gy * hy) & (y < ey + (ny - gy) * hy) & (zi >= q - gz * hz) & (zi < q + (nz - gz) * hz)
        return jnp.where(ok, 1.0, 0.0)

    def there(p, half):
        x = p + (gx * hx - ex) // half
        return jnp.where((x >= 0) & (x < nx * hx // half), 1.0, 0.0)

    def total_of(terms):
        while len(terms) > 1:
            terms = [a + b for a, b in zip(terms[::2], terms[1::2])] + ([terms[-1]] if len(terms) % 2 else [])
        return terms[0]

    def shifted(ref, p, strip, step):
        v = ref[p, strip, :]
        r0 = strip.start
        return total_of([
            ref[p, r0 - step : r0 - step + 8, :], ref[p, r0 + step : r0 + step + 8, :],
            roll(v, step, 1), roll(v, -step, 1),
        ])

    def helpers(c, rows):
        def tile(i, j):
            return win[c, TILES * i + j, rows, :]

        def along(n, i, piece):
            return pltpu.roll(beyond[n, i, rows, :], (sides[n][1] - CHUNK * chunk_of(piece)) % bz, 1)

        def over(parts):
            return [
                jnp.where(side[2], total_of([along(n, i, f) for i, f in parts]), 0.0)
                for n, side in enumerate(sides)
            ]

        return tile, over

    def assemble(c, a0, a1):
        blocks = range(2 * kx + 1)
        for t, strip in enumerate(strips):
            rows = slice(8 * t, 8 * t + 8)

            tile, over = helpers(c, rows)
            for i in blocks:
                skin = tile(i, 5 if i == 0 else 1)
                for n, (s, _, _, spill) in enumerate(sides):
                    beyond[n, i, rows, :] = wside[c, s, i, t, 0] + jnp.where(spill, skin, 0.0)
                wedge[i, strip, :] = total_of([jnp.where(mid, roll(skin, hz, 1), 0.0)] + over([(i, SKIN)]))
        for t, strip in enumerate(strips):
            rows = slice(8 * t, 8 * t + 8)

            tile, over = helpers(c, rows)
            for p in range(a0, a1):
                i, k = p // hx, p % hx
                body, parts = tile(i, (2, 3, 3, 4)[k]), [(i, k)]
                if k == 0 and i > 0:
                    body = body + tile(i - 1, 4)
                    parts.append((i - 1, UP))
                if k == hx - 1 and i < 2 * kx:
                    body = body + tile(i + 1, 2)
                    parts.append((i + 1, DOWN))
                terms = [jnp.where(mid, roll(body, hz * (k % 2), 1), 0.0)] + over(parts)
                up = 8 + 8 * t + k + 1
                down = 8 + 8 * t - hx + k
                terms.append(jnp.where(yi == 7, wedge[i, up : up + 8, :], jnp.where(yi == 0, wedge[i, down : down + 8, :], 0.0)))
                wd[p - a0, strip, :] = total_of(terms)

    def coarse(c):
        a0, a1 = ex - REACH, ex + hx + REACH
        assemble(c, a0, a1)
        n = (a1 - a0) // 2 - 1
        b0 = (a0 + 1) // 2
        on2 = [there(b0 + j, 2) for j in range(n)]
        for strip in strips:
            for j in range(n):
                pair[j, strip, :] = wd[2 * j + 1, strip, :] + wd[2 * j + 2, strip, :]
        for strip in strips:
            for j in range(n):
                ends = wd[2 * j, strip, :] + wd[2 * j + 3, strip, :]
                wb[j, strip, :] = (1.0 - 5.0 * W) * pair[j, strip, :] + W * (ends + shifted(pair, j, strip, 1))
        for strip in strips:
            grid = grid_strip(strip)
            for j in range(n):
                r0 = strip.start
                v = wb[j, strip, :]
                v = v + jnp.where(yi % 2 == 0, wb[j, r0 + 1 : r0 + 9, :], wb[j, r0 - 1 : r0 + 7, :])
                v = v + jnp.where(zi % 2 == 0, roll(v, -1, 1), roll(v, 1, 1))
                wr[j, strip, :] = (0.5 * on2[j]) * (grid * v)
        grids = [grid_strip(strip) for strip in late]
        for strip, grid in zip(late, grids):
            for j in range(1, n - 1):
                v = (2.0 * W - 6.0 * W * W) * wr[j, strip, :]
                v = v + (W * W) * (wr[j - 1, strip, :] + wr[j + 1, strip, :] + shifted(wr, j, strip, 2))
                we[j, strip, :] = on2[j] * (grid * v)
        k0 = (b0 + 2) * 2 - a0
        for strip, grid in zip(late, grids):
            for j in range(2, n - 2):
                v = wr[j, strip, :] + (we[j - 1, strip, :] + we[j + 1, strip, :] + shifted(we, j, strip, 2))
                v = on2[j] * (grid * ((1.0 - 6.0 * W) * we[j, strip, :] + W * v))
                for k in (2 * j - 4, 2 * j - 3):
                    wv[k, strip, :] = W * wd[k0 + k, strip, :] + v
        for strip, grid in zip(late, grids):
            for k in range(1, 2 * n - 9):
                v = wd[k0 + k, strip, :] + (wv[k - 1, strip, :] + wv[k + 1, strip, :] + shifted(wv, k, strip, 1))
                v = there(a0 + k0 + k, 1) * (grid * ((1.0 - 6.0 * W) * wv[k, strip, :] + W * v))
                to = 2 * (strip.start - late[0].start)
                prol[k - 1, pl.ds(to, 8, stride=2), :] = v
                prol[k - 1, pl.ds(to + 1, 8, stride=2), :] = v

    def dot(x, m):
        out = None
        for part in split(x):
            y = jnp.dot(part, m, preferred_element_type=f32)
            out = y if out is None else out + y
        return out

    def cycle_and_image(c, r):
        send_halo(c, r)
        if c == 0:
            send_coarse(c, r)
            pl.semaphore_wait(barrier, callers)
        else:
            send_coarse(c, r)
        items = gathered(c)
        start([m for m in items if all(m[4])], rsem.at[c])
        start(halo(c), rsem.at[c])
        start([m for m in items if not all(m[4])], rsem.at[c])
        rref = fld.at[c]
        arrive(halo(c) + gathered(c), rsem.at[c], 2)
        place_halo(c)
        place_edges(c)
        coarse(c)
        seen = slice(6, 14 + by)
        tall = 8 + by
        fine = dot(prol[:, seen, :].reshape((hx + 2) * tall, bz), grow[...])
        fine = fine.reshape(hx + 2, tall, (1 + len(beyond_at)) * bz)
        for n in range(len(beyond_at)):
            o = W * pk[c, n, seen, :]
            for j in range(hx + 2):
                o = o + jnp.where(lane_of((tall, bz)) // 4 == j, fine[j, :, (n + 1) * bz : (n + 2) * bz], 0.0)
            vpk[n, seen, :] = o
        for i in range(bx + 4):
            vfld[i, seen, :] = W * rref[i, seen, :] + fine[i // 2, :, 0:bz]
        for i in range(1, bx + 3):
            a, b = (8, 8 + by) if i in (1, bx + 2) else (7, 9 + by)
            z = (1.0 - 6.0 * W) * vfld[i, a:b, :] + W * (rref[i, a:b, :] + around(vfld, vpk, i, a, b))
            zrow = lax.broadcasted_iota(jnp.int32, z.shape, 0)
            if i == 1:
                ok = gx > 0
            elif i == bx + 2:
                ok = gx < nx - 1
            else:
                ok = ((zrow > 0) | (gy > 0)) & ((zrow < by + 1) | (gy < ny - 1))
            zfld[i, a:b, :] = jnp.where(ok, z, 0.0)
        rows = slice(8, 8 + by)
        lane2 = lane_of((by, bz))
        for n in range(len(beyond_at)):
            o = vpk[n, rows, :]
            s = roll(o, 2, 1) + roll(o, -2, 1) + roll(o, 1, 1) + vpk[n, 7 : 7 + by, :] + vpk[n, 9 : 9 + by, :]
            for i in range(2, bx + 2):
                v = vfld[i, rows, :]
                v = jnp.where(gz == 1, v, roll(v, 1, 1)) if nz == 2 else v if n == 0 else roll(v, 1, 1)
                s = s + jnp.where(lane2 == 2 * i + 1, v[:, 0:1], 0.0)
            z = (1.0 - 6.0 * W) * o + W * (pk[c, n, rows, :] + s)
            zpk[n, rows, :] = z if nz == 2 else jnp.where(gz > 0 if n == 0 else gz < nz - 1, z, 0.0)
        z = zfld[2 : bx + 2, 8 : 8 + by, :]
        return z, jnp.stack([6.0 * z[i - 2] - around(zfld, zpk, i, 8, 8 + by) for i in range(2, bx + 2)])

    z0, w = cycle_and_image(0, r0)
    u, aw = cycle_and_image(1, w)

    pairs = ((r0, z0), (z0, w), (w, u), (u, aw))
    l1 = lane_of((1, bz))
    mine = jnp.zeros((1, bz), f32)
    for i, (a, b) in enumerate(pairs):
        s = jnp.sum(jnp.sum(jnp.sum(a * b, axis=0), axis=0, keepdims=True), axis=1, keepdims=True)
        mine = jnp.where(l1 == i, s, mine)
    sums[me] = mine

    def share(to):
        pltpu.make_async_remote_copy(
            sums.at[me], sums.at[me], ssem.at[0], rsem.at[2], device_id=to, device_id_type=MESH
        ).start()

    if total <= 64:
        def ways(g, n):
            return [g, g + 1 - 2 * (g % 2), lax.rem(g + 2, 4), 3 - g] if n == 4 else [lax.rem(g + j, n) for j in range(n)]

        options = [ways(g, n) for g, n in zip((gx, gy, gz), ns)]
        for j in sorted(itertools.product(*(range(n) for n in ns)), key=lambda j: -sum(j)):
            if any(j):
                share(tuple(way[i] for way, i in zip(options, j)))
    else:

        def step(i, carry):
            o = lax.rem(me + i, total)
            share((o // (ny * nz), lax.rem(o // nz, ny), lax.rem(o, nz)))
            return carry

        lax.fori_loop(1, total, step, 0)

    wait_rows(total - 1, rsem.at[2])
    tot = jnp.sum(sums[...], axis=0)

    def scalar(i):
        return jnp.sum(jnp.where(l1 == i, tot, 0.0), axis=1, keepdims=True)

    g0, d0, wu, uv = (scalar(i) for i in range(4))
    a = g0 / d0
    g1 = (g0 - a * d0) - a * d0 + a * a * wu
    beta = g1 / g0
    zaz = d0 - 2.0 * a * wu + a * a * uv
    cross = 2.0 * (d0 - a * wu)
    b = g1 / (zaz + beta * cross + beta * beta * d0)
    along_z, along_u = a + b * (1.0 + beta), a * b
    for p in range(bx):
        both[0, p] = along_z * z0[p] - along_u * u[p]
        both[1, p] = r0[p] - along_z * w[p] + along_u * aw[p]
    arrive([item for c in (0, 1) for item in halo(c) + gathered(c)], ssem.at[0], 1, total - 1)


def solution(mesh):
    ns = tuple(mesh.shape[a] for a in ("gx", "gy", "gz"))

    def local(density, x_faces, y_faces, z_faces):
        bx, by, bz = density.shape
        hx, hy = bx // 2, by // 2
        assert hx == 4 and hy == 8 and REACH == 7
        kx, ky = -(-REACH // hx), -(-REACH // hy)
        total = ns[0] * ns[1] * ns[2]
        f32 = jnp.float32
        dma = pltpu.SemaphoreType.DMA

        def vmem(*shape, dtype=f32):
            return pltpu.VMEM(shape, dtype)

        wy = (2 * ky + 1) * hy
        pairs = hx // 2 + REACH - 1
        both = pl.pallas_call(
            functools.partial(kernel, ns, bx, by, bz, kx, ky),
            out_shape=vmem(2, bx, by, bz),
            in_specs=[pl.BlockSpec(memory_space=pl.ANY)] * 4,
            out_specs=pl.BlockSpec(memory_space=pltpu.VMEM),
            scratch_shapes=[
                vmem(2, bx + 4, by + 16, bz),
                vmem(2, 2, 2, bx, bz),
                vmem(2, 2, 2, bx, bz),
                vmem(2, 2, by + 16, bz),
                vmem(hx + 2, by, bz),
                vmem(hx, by + 16, bz),
                vmem(2 * hx, bz),
                vmem(2 * bz, 4 * bz, dtype=jnp.bfloat16),
                vmem(bz, (2 if ns[2] == 2 else 3) * bz, dtype=jnp.bfloat16),
                vmem(2, TILES, hy, bz),
                vmem(2, 2, 2, hy, bz),
                vmem(2, (2 * kx + 1) * TILES, wy, bz),
                vmem(2, 2, 2 * kx + 1, 2 * ky + 1, 2, hy, bz),
                vmem(hx + 2, by + 16, bz),
                vmem(total, 1, bz),
                vmem(ROWS, 1, bz),
                vmem(2 * kx + 1, wy + 16, bz),
                vmem(2, 2 * kx + 1, wy, bz),
                vmem(hx + 2 * REACH, wy + 16, bz),
                vmem(pairs, wy + 16, bz),
                vmem(pairs, wy + 16, bz),
                vmem(pairs, wy + 16, bz),
                vmem(pairs, wy + 16, bz),
                vmem(2 * (pairs - 4), wy + 16, bz),
                vmem(bx + 4, by + 16, bz),
                vmem(2, by + 16, bz),
                vmem(bx + 4, by + 16, bz),
                vmem(2, by + 16, bz),
                vmem(*density.shape),
                vmem(*x_faces.shape),
                vmem(*y_faces.shape),
                vmem(*z_faces.shape),
                dma((1,)),
                dma((3,)),
                dma((2,)),
            ],
            compiler_params=pltpu.CompilerParams(collective_id=0, has_side_effects=True),
        )(density, x_faces, y_faces, z_faces)
        return both[0], both[1]

    return jax.shard_map(
        local,
        mesh=mesh,
        in_specs=(P("gx", "gy", "gz"), P(None, "gy", "gz"), P(None, "gx", "gz"), P(None, "gx", "gy")),
        out_specs=(P("gx", "gy", "gz"), P("gx", "gy", "gz")),
        check_vma=False,
    )
```
